16 devices in a mesh: data: 16 (over z, y, x, core).
Axes of the slice: x: 2, y: 2, z: 2, core: 2. Of those that a mesh axis runs over, the one named last changes fastest.
Arguments:
- h_a: bfloat16 [8192, 2048], P('data')
- h_b: bfloat16 [8192, 2048], P('data')
- w_one: bfloat16 [2048, 2048], replicated
- w_two: bfloat16 [2048, 2048], replicated
- w_three: bfloat16 [2048, 2048], replicated
- gain_one: float32 [2048], replicated
- shift_one: float32 [2048], replicated
- gain_two: float32 [2048], replicated
- shift_two: float32 [2048], replicated
- lam_off: float32 [], replicated
Outputs:
- output 1: float32 [], replicated
- output 2: float32 [2048, 2048], P('data')
- output 3: float32 [2048, 2048], P('data')
- output 4: float32 [2048, 2048], P('data')
- output 5: float32 [2048], replicated
- output 6: float32 [2048], replicated
- output 7: float32 [2048], replicated
- output 8: float32 [2048], replicated
All inputs are finite; a program needn't handle non-finite values.
Results may differ from the reference program's by a relative error of at most 0.00507078.
Values are sent between devices in bfloat16 or wider.
A program may use at most 1 GiB of HBM per device.

```python
import jax
import jax.numpy as jnp
from jax import lax

FEAT_DIM = 2048
PROJ_DIM = 2048
ROWS_DEV = 512
SHARDS = 16
TOTAL_ROWS = ROWS_DEV * SHARDS
NORM_EPS = 1e-5


def setup_inputs(seed: int = 0) -> dict:
    key_list = jax.random.split(jax.random.key(seed), 14)
    common = jax.random.normal(key_list[0], (TOTAL_ROWS, FEAT_DIM), jnp.float32)
    shard_shift = 0.6 * jax.random.normal(key_list[1], (SHARDS, 1, FEAT_DIM), jnp.float32)
    shard_scale = jnp.exp(0.3 * jax.random.normal(key_list[2], (SHARDS, 1, FEAT_DIM), jnp.float32))

    def make_view(view_key):
        noise_vals = jax.random.normal(view_key, (TOTAL_ROWS, FEAT_DIM), jnp.float32)
        mixed_rows = (0.77 * common + 0.64 * noise_vals).reshape(SHARDS, ROWS_DEV, FEAT_DIM)
        return (mixed_rows * shard_scale + shard_shift).reshape(TOTAL_ROWS, FEAT_DIM).astype(jnp.bfloat16)

    def make_weight(weight_key, fan_in, fan_out):
        weight_scale = fan_in ** -0.5
        return (jax.random.normal(weight_key, (fan_in, fan_out), jnp.float32) * weight_scale).astype(jnp.bfloat16)

    def make_vector(vec_key, center):
        return center + 0.25 * jax.random.normal(vec_key, (PROJ_DIM,), jnp.float32)

    lam_off = (0.1 + 0.2 * jax.random.uniform(key_list[12], (), jnp.float32)) * TOTAL_ROWS / PROJ_DIM
    return {
        "h_a": make_view(key_list[3]),
        "h_b": make_view(key_list[4]),
        "w_one": make_weight(key_list[5], FEAT_DIM, PROJ_DIM),
        "w_two": make_weight(key_list[6], PROJ_DIM, PROJ_DIM),
        "w_three": make_weight(key_list[7], PROJ_DIM, PROJ_DIM),
        "gain_one": make_vector(key_list[8], 1.0),
        "shift_one": make_vector(key_list[9], 0.0),
        "gain_two": make_vector(key_list[10], 1.0),
        "shift_two": make_vector(key_list[11], 0.0),
        "lam_off": lam_off,
    }


def batch_norm(values):
    col_mean = jnp.sum(values, axis=0) / TOTAL_ROWS
    col_var = jnp.sum(values * values, axis=0) / TOTAL_ROWS - col_mean * col_mean
    return (values - col_mean) * lax.rsqrt(col_var + NORM_EPS)


def project(feat_rows, params):
    w_one, w_two, w_three, gain_one, shift_one, gain_two, shift_two = params
    hidden_one = jnp.dot(feat_rows.astype(jnp.float32), w_one, preferred_element_type=jnp.float32)
    act_one = jax.nn.relu(gain_one * batch_norm(hidden_one) + shift_one).astype(jnp.bfloat16)
    hidden_two = jnp.dot(act_one.astype(jnp.float32), w_two, preferred_element_type=jnp.float32)
    act_two = jax.nn.relu(gain_two * batch_norm(hidden_two) + shift_two).astype(jnp.bfloat16)
    proj_out = jnp.dot(act_two.astype(jnp.float32), w_three, preferred_element_type=jnp.float32)
    return batch_norm(proj_out).astype(jnp.bfloat16)


def barlow_loss(params, h_a, h_b, lam_off):
    embed_a = project(h_a, params).astype(jnp.float32)
    embed_b = project(h_b, params).astype(jnp.float32)
    corr_mat = jnp.dot(embed_a.T, embed_b, preferred_element_type=jnp.float32) / TOTAL_ROWS
    feat_index = jnp.arange(PROJ_DIM)
    diag_mask = feat_index[:, None] == feat_index[None, :]
    diag_gap = 1.0 - jnp.diagonal(corr_mat)
    off_square = jnp.sum(jnp.where(diag_mask, 0.0, corr_mat * corr_mat))
    return jnp.sum(diag_gap * diag_gap) + lam_off * off_square


def reference(h_a, h_b, w_one, w_two, w_three, gain_one, shift_one, gain_two, shift_two, lam_off):
    params = (w_one.astype(jnp.float32), w_two.astype(jnp.float32), w_three.astype(jnp.float32),
              gain_one, shift_one, gain_two, shift_two)
    loss_total, grad_list = jax.value_and_grad(barlow_loss)(params, h_a, h_b, lam_off)
    return (loss_total, grad_list[0], grad_list[1], grad_list[2],
            grad_list[3], grad_list[4], grad_list[5], grad_list[6])
```

```python
import functools

import jax
import jax.numpy as jnp
from jax import lax
from jax.experimental import pallas as pl
from jax.experimental.pallas import tpu as pltpu
from jax.sharding import PartitionSpec as P

NORM_EPS = 1e-5
LAST_DIMS = (((2,), (1,)), ((), ()))
MESH = pl.DeviceIdType.MESH
RING = 4
COLS = 256
BLOCK = 128
F32_SPLIT = ((48, 40, 40), (40, 48, 40), (40, 40, 48))
BF16_SPLIT = ((48, 48, 32), (32, 48, 48), (48, 32, 48))


class Place:
    def __init__(self):
        self.me = lax.axis_index("data")
        self.core = lax.rem(self.me, 2)
        self.chip = self.me // 2
        self.coord = (self.chip // 4, lax.rem(self.chip // 2, 2), lax.rem(self.chip, 2))
        self.partner = self.me + 1 - 2 * self.core
        self.near = tuple(self.me + (1 - 2 * c) * w for c, w in zip(self.coord, (8, 4, 2)))


def greet(peers):
    barrier = pltpu.get_barrier_semaphore()
    for peer in peers:
        pl.semaphore_signal(barrier, inc=1, device_id=(peer,), device_id_type=MESH)
    pl.semaphore_wait(barrier, len(peers))


def remote(src, dst, send, recv, peer):
    return pltpu.make_async_remote_copy(src_ref=src, dst_ref=dst, send_sem=send, recv_sem=recv,
                                        device_id=(peer,), device_id_type=MESH)


def row_parts(split, phase):
    sizes = split[phase % 3]
    return tuple((sum(sizes[:r]), sizes[r]) for r in range(3))


class HalvingReduce:
    def __init__(self, place, acc, bufs, ssem, rsem):
        self.place, self.acc, self.bufs, self.ssem, self.rsem = place, acc, bufs, ssem, rsem

    def at(self, t, picks):
        return (lax.rem(t, RING),) + tuple(picks)

    def copy(self, step, t, phase, r):
        slot = lax.rem(t, RING)
        off, size = row_parts(F32_SPLIT, phase)[r]
        rows = pl.ds(off, size)
        picks = [slice(None)] * 3
        for k in range(step):
            axis = (r + k) % 3
            picks[axis] = self.place.coord[axis]
        axis = (r + step) % 3
        picks[axis] = 1 - self.place.coord[axis]
        src = self.acc.at[(slot, *picks, rows, slice(None))]
        dst = self.bufs[step].at[(slot,) + (slice(None),) * (2 - step) + (rows, slice(None))]
        return remote(src, dst, self.ssem.at[slot, 3 * step + r], self.rsem.at[slot, 3 * step + r],
                      self.place.near[axis])

    def send(self, step, t, phase):
        for r in range(3):
            self.copy(step, t, phase, r).start()

    def wait_sends(self, t, phase):
        for step in range(3):
            for r in range(3):
                self.copy(step, t, phase, r).wait_send()

    def add(self, step, t, phase):
        slot = lax.rem(t, RING)
        for r in range(3):
            self.copy(step, t, phase, r).wait_recv()
            off, size = row_parts(F32_SPLIT, phase)[r]
            rows = pl.ds(off, size)
            fixed = {(r + k) % 3 for k in range(step + 1)}
            free = [a for a in range(3) if a not in fixed]
            for n in range(2 ** len(free)):
                picks = list(self.place.coord)
                sub = []
                for pos, a in enumerate(free):
                    bit = (n >> (len(free) - 1 - pos)) & 1
                    picks[a] = bit
                    sub.append(bit)
                where = (slot, *picks, rows, slice(None))
                self.acc[where] = self.acc[where] + self.bufs[step][(slot, *sub, rows, slice(None))]

    def result(self, t, phase, r):
        slot = lax.rem(t, RING)
        self.copy(2, t, phase, r).wait_recv()
        off, size = row_parts(F32_SPLIT, phase)[r]
        rows = pl.ds(off, size)
        return off, size, (self.acc[(slot, *self.place.coord, rows, slice(None))]
                           + self.bufs[2][(slot, rows, slice(None))])


def columns(t, width=COLS):
    return pl.ds(pl.multiple_of(t * width, width), width)


def product_reduce(place, chunks, x_ref, d_ref, xt, xsend, dpart, acc, bufs, sems, finish, extra_slots, extra):
    ssem, rsem, psend, precv = sems
    rows = x_ref.shape[0]
    partner = place.partner
    greet((partner,) + place.near)

    def swap(t):
        cols = columns(t)
        return remote(d_ref.at[:, cols], dpart.at[:, cols], psend.at[t], precv.at[t], partner)

    @pl.loop(0, chunks)
    def _(t):
        swap(t).start()

    @pl.loop(0, 8)
    def _(b):
        to = pl.ds(pl.multiple_of(b * BLOCK, BLOCK), BLOCK)
        other = pl.ds(pl.multiple_of((2 * b + 1 - place.core) * BLOCK, BLOCK), BLOCK)
        xsend[to, :] = x_ref[:, other].T

    x_swap = remote(xsend, xt.at[:, pl.ds(rows, rows)], psend.at[chunks], precv.at[chunks], partner)
    x_swap.start()

    @pl.loop(0, 8)
    def _(b):
        to = pl.ds(pl.multiple_of(b * BLOCK, BLOCK), BLOCK)
        own = pl.ds(pl.multiple_of((2 * b + place.core) * BLOCK, BLOCK), BLOCK)
        xt[to, pl.ds(0, rows)] = x_ref[:, own].T

    x_swap.wait_recv()
    ring = HalvingReduce(place, acc, bufs, ssem, rsem)

    def slot_step(t, s):
        @pl.when(t < chunks)
        def _():
            @pl.when(t >= RING)
            def _():
                ring.wait_sends(t - RING, s - RING)
            swap(t).wait_recv()
            cols = columns(t)
            slot = lax.rem(t, RING)
            for half in range(2):
                feats = pl.ds(512 * half, 512)
                part = jnp.dot(xt[feats, pl.ds(0, rows)], d_ref[:, cols], preferred_element_type=jnp.float32)
                part += jnp.dot(xt[feats, pl.ds(rows, rows)], dpart[:, cols], preferred_element_type=jnp.float32)
                acc[slot, half] = part.reshape(2, 2, BLOCK, COLS)
            ring.send(0, t, s)

        for step in range(2):
            u = t - 1 - step

            @pl.when((u >= 0) & (u < chunks))
            def _():
                ring.add(step, u, s - 1 - step)
                ring.send(step + 1, u, s - 1 - step)

        @pl.when((t >= 3) & (t - 3 < chunks))
        def _():
            finish(ring, t - 3, s - 3)

        extra(t, s)

    @pl.loop(0, (chunks + 3 + extra_slots + 2) // 3)
    def _(q):
        for s in range(3):
            slot_step(3 * q + s, s)

    for t in range(chunks - RING, chunks):
        ring.wait_sends(t, t)

    @pl.loop(0, chunks)
    def _(t):
        swap(t).wait_send()
    x_swap.wait_send()


def weight_kernel(x_ref, d_ref, out_ref, xt, xsend, dpart, acc, b0, b1, b2, ssem, rsem, psend, precv):
    place = Place()
    chunks = d_ref.shape[1] // COLS

    def finish(ring, t, phase):
        for r in range(3):
            off, size, val = ring.result(t, phase, r)
            out_ref[pl.ds(off, size), columns(t)] = val

    product_reduce(place, chunks, x_ref, d_ref, xt, xsend, dpart, acc, (b0, b1, b2),
                   (ssem, rsem, psend, precv), finish, 0, lambda t, s: None)


def corr_kernel(inv_rows, lam_ref, x_ref, d_ref, g_ref, loss_ref,
                xt, xsend, dpart, acc, b0, b1, b2, ssem, rsem, psend, precv, gsend, grecv, stage):
    place = Place()
    chunks = d_ref.shape[1] // COLS
    lam = lam_ref[0, 0]
    loss_ref[...] = jnp.zeros_like(loss_ref)

    def gather(step, t, phase, r):
        off, size = row_parts(BF16_SPLIT, phase)[r]
        picks = list(place.coord)
        for k in range(step):
            picks[(r + 2 - k) % 3] = slice(None)
        axis = (r + 2 - step) % 3
        ref = g_ref.at[(*picks, place.core, pl.ds(off, size), columns(t))]
        return remote(ref, ref, gsend.at[t, 3 * step + r], grecv.at[t, 3 * step + r], place.near[axis])

    def across(t):
        ref = g_ref.at[:, :, :, place.core, :, columns(t)]
        return remote(ref, ref, gsend.at[t, 9], grecv.at[t, 9], place.partner)

    def finish(ring, t, phase):
        for r in range(3):
            off, size, val = ring.result(t, phase, r)
            corr = val * inv_rows
            row_id = place.me * BLOCK + off + lax.broadcasted_iota(jnp.int32, corr.shape, 0)
            col_id = t * COLS + lax.broadcasted_iota(jnp.int32, corr.shape, 1)
            diag = row_id == col_id
            gap = 1.0 - corr
            terms = jnp.where(diag, gap * gap, lam * corr * corr)
            loss_ref[...] += jnp.sum(terms, axis=0, keepdims=True)
            grad = jnp.where(diag, -2.0 * gap, 2.0 * lam * corr) * inv_rows
            stage[pl.ds(off, size), :] = grad
        g_ref[(*place.coord, place.core, slice(None), columns(t))] = stage[...].astype(jnp.bfloat16)
        for r in range(3):
            gather(0, t, phase, r).start()

    def extra(t, s):
        for step in range(2):
            u = t - 4 - step

            @pl.when((u >= 0) & (u < chunks))
            def _():
                for r in range(3):
                    gather(step, u, s - 4 - step, r).wait_recv()
                    gather(step + 1, u, s - 4 - step, r).start()

        @pl.when((t >= 6) & (t - 6 < chunks))
        def _():
            for r in range(3):
                gather(2, t - 6, s - 6, r).wait_recv()
            across(t - 6).start()

    product_reduce(place, chunks, x_ref, d_ref, xt, xsend, dpart, acc, (b0, b1, b2),
                   (ssem, rsem, psend, precv), finish, 3, extra)
    for t in range(chunks):
        across(t).wait()
        for step in range(3):
            for r in range(3):
                gather(step, t, t, r).wait_send()


def product_scratch(rows, width):
    chunks = width // COLS
    return [
        pltpu.VMEM((width // 2, 2 * rows), jnp.bfloat16),
        pltpu.VMEM((width // 2, rows), jnp.bfloat16),
        pltpu.VMEM((rows, width), jnp.bfloat16),
        pltpu.VMEM((RING, 2, 2, 2, BLOCK, COLS), jnp.float32),
        pltpu.VMEM((RING, 2, 2, BLOCK, COLS), jnp.float32),
        pltpu.VMEM((RING, 2, BLOCK, COLS), jnp.float32),
        pltpu.VMEM((RING, BLOCK, COLS), jnp.float32),
        pltpu.SemaphoreType.DMA((RING, 9)),
        pltpu.SemaphoreType.DMA((RING, 9)),
        pltpu.SemaphoreType.DMA((chunks + 1,)),
        pltpu.SemaphoreType.DMA((chunks + 1,)),
    ]


VM = pl.BlockSpec(memory_space=pltpu.VMEM)


def weight_grad(x, d):
    rows, width = x.shape
    return pl.pallas_call(
        weight_kernel,
        out_shape=jax.ShapeDtypeStruct((BLOCK, width), jnp.float32),
        in_specs=[VM, VM], out_specs=VM,
        scratch_shapes=product_scratch(rows, width),
        compiler_params=pltpu.CompilerParams(collective_id=1, has_side_effects=True, vmem_limit_bytes=56 << 20),
        name="weight_grad",
    )(x, d)


def corr_grad(x, d, lam, total_rows):
    rows, width = x.shape
    chunks = width // COLS
    g, loss = pl.pallas_call(
        functools.partial(corr_kernel, 1.0 / total_rows),
        out_shape=(jax.ShapeDtypeStruct((2, 2, 2, 2, BLOCK, width), jnp.bfloat16),
                   jax.ShapeDtypeStruct((1, COLS), jnp.float32)),
        in_specs=[pl.BlockSpec(memory_space=pltpu.SMEM), VM, VM], out_specs=(VM, VM),
        scratch_shapes=product_scratch(rows, width) + [pltpu.SemaphoreType.DMA((chunks, 10))] * 2
        + [pltpu.VMEM((BLOCK, COLS), jnp.float32)],
        compiler_params=pltpu.CompilerParams(collective_id=2, has_side_effects=True, vmem_limit_bytes=56 << 20),
        name="corr_grad",
    )(lam.reshape(1, 1), x, d)
    return g.reshape(width, width), loss


def stats_kernel(p_ref, out_ref, land, parts, psend, precv, csend, crecv, fsend, frecv):
    place = Place()
    peers = []
    for dist in range(1, 8):
        peers.append(lax.rem(place.chip + dist, 8) * 2 + place.core)
    greet([place.partner] + peers)
    first = remote(p_ref.at[1 - place.core], land, psend, precv, place.partner)
    first.start()
    first.wait_recv()
    parts[place.chip] = p_ref[place.core] + land[...]
    copies = []
    for n, peer in enumerate(peers):
        copies.append(remote(parts.at[place.chip], parts.at[place.chip], csend.at[n], crecv.at[n], peer))
        copies[-1].start()
    for copy in copies:
        copy.wait_recv()
    total = parts[0]
    for c in range(1, 8):
        total = total + parts[c]
    out_ref[place.core] = total
    last = remote(out_ref.at[place.core], out_ref.at[place.core], fsend, frecv, place.partner)
    last.start()
    first.wait_send()
    for copy in copies:
        copy.wait_send()
    last.wait()


def all_sum(payload, cid):
    shape = payload.shape
    return pl.pallas_call(
        stats_kernel,
        out_shape=jax.ShapeDtypeStruct(shape, jnp.float32),
        in_specs=[VM], out_specs=VM,
        scratch_shapes=[pltpu.VMEM(shape[1:], jnp.float32), pltpu.VMEM((8,) + shape[1:], jnp.float32),
                        pltpu.SemaphoreType.DMA, pltpu.SemaphoreType.DMA,
                        pltpu.SemaphoreType.DMA((7,)), pltpu.SemaphoreType.DMA((7,)),
                        pltpu.SemaphoreType.DMA, pltpu.SemaphoreType.DMA],
        compiler_params=pltpu.CompilerParams(collective_id=cid, has_side_effects=True),
        name="all_sum",
    )(payload)


def reduce_sums(first, second):
    width = first.shape[1]
    payload = jnp.stack([first, second], axis=1).reshape(2, 8, width // 4)
    total = all_sum(payload, 3).reshape(2, 2, width)
    return total[:, 0], total[:, 1]


def norm_forward(values, total_rows):
    sums, squares = reduce_sums(jnp.sum(values, axis=1), jnp.sum(values * values, axis=1))
    col_mean = sums / total_rows
    inv_std = lax.rsqrt(squares / total_rows - col_mean * col_mean + NORM_EPS)
    return (values - col_mean[:, None, :]) * inv_std[:, None, :], inv_std


def norm_backward(grad_out, normed, inv_std, total_rows):
    sums = reduce_sums(jnp.sum(grad_out, axis=1), jnp.sum(grad_out * normed, axis=1))
    grad_in = inv_std[:, None, :] * (grad_out - (sums[0][:, None, :] + normed * sums[1][:, None, :]) / total_rows)
    return grad_in, sums


def solution(mesh):
    shards = mesh.shape["data"]

    def local_step(h_a, h_b, w_one, w_two, w_three, gain_one, shift_one, gain_two, shift_two, lam_off):
        rows_dev, width = h_a.shape
        total_rows = rows_dev * shards
        feat_rows = jnp.concatenate([h_a, h_b], axis=0)
        hidden_one = jnp.dot(feat_rows, w_one, preferred_element_type=jnp.float32).reshape(2, rows_dev, -1)
        normed_one, inv_one = norm_forward(hidden_one, total_rows)
        pre_one = gain_one * normed_one + shift_one
        act_one = jax.nn.relu(pre_one).astype(jnp.bfloat16)
        hidden_two = jnp.dot(act_one, w_two, preferred_element_type=jnp.float32)
        normed_two, inv_two = norm_forward(hidden_two, total_rows)
        pre_two = gain_two * normed_two + shift_two
        act_two = jax.nn.relu(pre_two).astype(jnp.bfloat16)
        proj_out = jnp.dot(act_two, w_three, preferred_element_type=jnp.float32)
        normed_out, inv_out = norm_forward(proj_out, total_rows)
        embed_pair = normed_out.astype(jnp.bfloat16)
        grad_scaled, loss_part = corr_grad(embed_pair[0], embed_pair[1], lam_off, total_rows)
        grad_embed_a = lax.dot_general(embed_pair[1], grad_scaled, (((1,), (1,)), ((), ())),
                                       preferred_element_type=jnp.float32)
        grad_embed_b = jnp.dot(embed_pair[0], grad_scaled, preferred_element_type=jnp.float32)
        grad_embed = jnp.stack([grad_embed_a, grad_embed_b])
        grad_proj = norm_backward(grad_embed, normed_out, inv_out, total_rows)[0].astype(jnp.bfloat16)
        flat = lambda a: a.reshape(2 * rows_dev, -1)
        grad_w_three = weight_grad(flat(act_two), flat(grad_proj))
        grad_act_two = lax.dot_general(grad_proj, w_three, LAST_DIMS, preferred_element_type=jnp.float32)
        grad_pre_two = jnp.where(pre_two > 0, grad_act_two, 0.0)
        grad_hidden_two, sums_two = norm_backward(grad_pre_two, normed_two, inv_two, total_rows)
        grad_hidden_two = (gain_two * grad_hidden_two).astype(jnp.bfloat16)
        grad_w_two = weight_grad(flat(act_one), flat(grad_hidden_two))
        grad_act_one = lax.dot_general(grad_hidden_two, w_two, LAST_DIMS, preferred_element_type=jnp.float32)
        grad_pre_one = jnp.where(pre_one > 0, grad_act_one, 0.0)
        grad_hidden_one, sums_one = norm_backward(grad_pre_one, normed_one, inv_one, total_rows)
        grad_hidden_one = (gain_one * grad_hidden_one).astype(jnp.bfloat16)
        grad_w_one = weight_grad(feat_rows, flat(grad_hidden_one))
        loss_block = jnp.pad(loss_part.reshape(1, 2, 128), ((0, 1), (0, 6), (0, 0)))
        loss_total = jnp.sum(all_sum(loss_block, 4)[0])
        return (loss_total, grad_w_one, grad_w_two, grad_w_three,
                jnp.sum(sums_one[1], axis=0), jnp.sum(sums_one[0], axis=0),
                jnp.sum(sums_two[1], axis=0), jnp.sum(sums_two[0], axis=0))

    row_spec = P("data", None)
    whole_mat = P(None, None)
    whole_vec = P(None)
    return jax.shard_map(
        local_step, mesh=mesh,
        in_specs=(row_spec, row_spec, whole_mat, whole_mat, whole_mat,
                  whole_vec, whole_vec, whole_vec, whole_vec, P()),
        out_specs=(P(), row_spec, row_spec, row_spec, whole_vec, whole_vec, whole_vec, whole_vec),
        check_vma=False)
```

```python
import functools

import jax
import jax.numpy as jnp
from jax import lax
from jax.experimental import pallas as pl
from jax.experimental.pallas import tpu as pltpu
from jax.sharding import PartitionSpec as P

NORM_EPS = 1e-5
MESH = pl.DeviceIdType.MESH
RING = 4
COLS = 256
BLOCK = 128
F32_SPLIT = ((48, 40, 40), (40, 48, 40), (40, 40, 48))
BF16_SPLIT = ((48, 48, 32), (32, 48, 48), (48, 32, 48))


class Place:
    def __init__(self):
        self.me = lax.axis_index("data")
        self.core = lax.rem(self.me, 2)
        self.chip = self.me // 2
        self.coord = (self.chip // 4, lax.rem(self.chip // 2, 2), lax.rem(self.chip, 2))
        self.partner = self.me + 1 - 2 * self.core
        self.near = tuple(self.me + (1 - 2 * c) * w for c, w in zip(self.coord, (8, 4, 2)))


def greet(peers):
    barrier = pltpu.get_barrier_semaphore()
    for peer in peers:
        pl.semaphore_signal(barrier, inc=1, device_id=(peer,), device_id_type=MESH)
    pl.semaphore_wait(barrier, len(peers))


def remote(src, dst, send, recv, peer):
    return pltpu.make_async_remote_copy(src_ref=src, dst_ref=dst, send_sem=send, recv_sem=recv,
                                        device_id=(peer,), device_id_type=MESH)


def row_parts(split, phase):
    sizes = split[phase % 3]
    return tuple((sum(sizes[:r]), sizes[r]) for r in range(3))


class HalvingReduce:
    def __init__(self, place, acc, bufs, ssem, rsem):
        self.place, self.acc, self.bufs, self.ssem, self.rsem = place, acc, bufs, ssem, rsem

    def at(self, t, picks):
        return (lax.rem(t, RING),) + tuple(picks)

    def copy(self, step, t, phase, r):
        slot = lax.rem(t, RING)
        off, size = row_parts(F32_SPLIT, phase)[r]
        rows = pl.ds(off, size)
        picks = [slice(None)] * 3
        for k in range(step):
            axis = (r + k) % 3
            picks[axis] = self.place.coord[axis]
        axis = (r + step) % 3
        picks[axis] = 1 - self.place.coord[axis]
        src = self.acc.at[(slot, *picks, rows, slice(None))]
        dst = self.bufs[step].at[(slot,) + (slice(None),) * (2 - step) + (rows, slice(None))]
        return remote(src, dst, self.ssem.at[slot, 3 * step + r], self.rsem.at[slot, 3 * step + r],
                      self.place.near[axis])

    def send(self, step, t, phase):
        for r in range(3):
            self.copy(step, t, phase, r).start()

    def wait_sends(self, t, phase):
        for step in range(3):
            for r in range(3):
                self.copy(step, t, phase, r).wait_send()

    def add(self, step, t, phase):
        slot = lax.rem(t, RING)
        for r in range(3):
            self.copy(step, t, phase, r).wait_recv()
            off, size = row_parts(F32_SPLIT, phase)[r]
            rows = pl.ds(off, size)
            fixed = {(r + k) % 3 for k in range(step + 1)}
            free = [a for a in range(3) if a not in fixed]
            for n in range(2 ** len(free)):
                picks = list(self.place.coord)
                sub = []
                for pos, a in enumerate(free):
                    bit = (n >> (len(free) - 1 - pos)) & 1
                    picks[a] = bit
                    sub.append(bit)
                where = (slot, *picks, rows, slice(None))
                self.acc[where] = self.acc[where] + self.bufs[step][(slot, *sub, rows, slice(None))]

    def result(self, t, phase, r):
        slot = lax.rem(t, RING)
        self.copy(2, t, phase, r).wait_recv()
        off, size = row_parts(F32_SPLIT, phase)[r]
        rows = pl.ds(off, size)
        return off, size, (self.acc[(slot, *self.place.coord, rows, slice(None))]
                           + self.bufs[2][(slot, rows, slice(None))])


def columns(t, width=COLS):
    return pl.ds(pl.multiple_of(t * width, width), width)


def product_reduce(place, chunks, x_ref, d_ref, xt, xsend, dpart, acc, bufs, sems, finish, extra_slots, extra):
    ssem, rsem, psend, precv = sems
    rows = x_ref.shape[0]
    partner = place.partner
    greet((partner,) + place.near)

    def swap(t):
        cols = columns(t)
        return remote(d_ref.at[:, cols], dpart.at[:, cols], psend.at[t], precv.at[t], partner)

    @pl.loop(0, chunks)
    def _(t):
        swap(t).start()

    @pl.loop(0, 8)
    def _(b):
        to = pl.ds(pl.multiple_of(b * BLOCK, BLOCK), BLOCK)
        other = pl.ds(pl.multiple_of((2 * b + 1 - place.core) * BLOCK, BLOCK), BLOCK)
        xsend[to, :] = x_ref[:, other].T

    x_swap = remote(xsend, xt.at[:, pl.ds(rows, rows)], psend.at[chunks], precv.at[chunks], partner)
    x_swap.start()

    @pl.loop(0, 8)
    def _(b):
        to = pl.ds(pl.multiple_of(b * BLOCK, BLOCK), BLOCK)
        own = pl.ds(pl.multiple_of((2 * b + place.core) * BLOCK, BLOCK), BLOCK)
        xt[to, pl.ds(0, rows)] = x_ref[:, own].T

    x_swap.wait_recv()
    ring = HalvingReduce(place, acc, bufs, ssem, rsem)

    def slot_step(t, s):
        @pl.when(t < chunks)
        def _():
            @pl.when(t >= RING)
            def _():
                ring.wait_sends(t - RING, s - RING)
            swap(t).wait_recv()
            cols = columns(t)
            slot = lax.rem(t, RING)
            for half in range(2):
                feats = pl.ds(512 * half, 512)
                part = jnp.dot(xt[feats, pl.ds(0, rows)], d_ref[:, cols], preferred_element_type=jnp.float32)
                part += jnp.dot(xt[feats, pl.ds(rows, rows)], dpart[:, cols], preferred_element_type=jnp.float32)
                acc[slot, half] = part.reshape(2, 2, BLOCK, COLS)
            ring.send(0, t, s)

        for step in range(2):
            u = t - 1 - step

            @pl.when((u >= 0) & (u < chunks))
            def _():
                ring.add(step, u, s - 1 - step)
                ring.send(step + 1, u, s - 1 - step)

        @pl.when((t >= 3) & (t - 3 < chunks))
        def _():
            finish(ring, t - 3, s - 3)

        extra(t, s)

    @pl.loop(0, (chunks + 3 + extra_slots + 2) // 3)
    def _(q):
        for s in range(3):
            slot_step(3 * q + s, s)

    for t in range(chunks - RING, chunks):
        ring.wait_sends(t, t)

    @pl.loop(0, chunks)
    def _(t):
        swap(t).wait_send()
    x_swap.wait_send()


def exchange_parts(place, psum, parts, total, sems):
    asend, arecv, csend, crecv, fsend, frecv = sems
    peers = [lax.rem(place.chip + dist, 8) * 2 + place.core for dist in range(1, 8)]
    other = 1 - place.core
    land = psum.at[2]
    first = remote(psum.at[other], land, asend, arecv, place.partner)
    mine = parts.at[place.chip]
    across = [remote(mine, mine, csend.at[n], crecv.at[n], peer) for n, peer in enumerate(peers)]
    last = remote(total.at[place.core], total.at[place.core], fsend, frecv, place.partner)

    def start():
        first.start()

    def chips():
        first.wait_recv()
        parts[place.chip] = psum[place.core] + psum[2]
        for copy in across:
            copy.start()

    def finish():
        for copy in across:
            copy.wait_recv()
        value = parts[0]
        for c in range(1, 8):
            value = value + parts[c]
        total[place.core] = value
        last.start()

    def close():
        last.wait_recv()
        first.wait_send()
        for copy in across:
            copy.wait_send()
        last.wait_send()

    return peers, start, chips, finish, close


def back_kernel(inv_rows, gains, shifts, invs, dz_hbm, x2_hbm, x1_hbm, x0_hbm, n2_hbm, n1_hbm, w3_hbm, w2_hbm,
                out_ref, sums_ref, xt, xsend, xs, own, other, acc, b0, b1, b2, gp, wbuf, nbuf, psum, parts,
                ssem, rsem, psend, precv, asend, arecv, csend, crecv, fsend, frecv, lsem, wsem, nsem):
    place = Place()
    rows, width = dz_hbm.shape
    view_rows = rows // 2
    chunks = width // COLS
    jobs = 3
    peers = [lax.rem(place.chip + dist, 8) * 2 + place.core for dist in range(1, 8)]
    partner = place.partner
    ring = HalvingReduce(place, acc, (b0, b1, b2), ssem, rsem)

    def load_w(j, c, buf):
        rows_c = columns(c)
        for k, ref in enumerate((w3_hbm, w2_hbm)):
            @pl.when(j == k)
            def _():
                pltpu.make_async_copy(ref.at[rows_c, :], wbuf.at[buf], wsem.at[buf]).start()

    def load_n(j, c, buf):
        for k, ref in enumerate((n2_hbm, n1_hbm)):
            @pl.when(j == k)
            def _():
                pltpu.make_async_copy(ref.at[:, columns(c)], nbuf.at[buf], nsem.at[buf]).start()

    def wait_w(buf):
        pltpu.make_async_copy(w3_hbm.at[pl.ds(0, COLS), :], wbuf.at[buf], wsem.at[buf]).wait()

    def wait_n(buf):
        pltpu.make_async_copy(n2_hbm.at[:, pl.ds(0, COLS)], nbuf.at[buf], nsem.at[buf]).wait()

    def swap(jb, c):
        cols = columns(c)
        return remote(own.at[jb, :, cols], other.at[jb, :, cols], psend.at[jb, c], precv.at[jb, c], partner)

    def x_swap(jb):
        return remote(xsend, xt.at[jb, :, pl.ds(rows, rows)], psend.at[jb, chunks], precv.at[jb, chunks], partner)

    def load_x(ref):
        return pltpu.make_async_copy(ref, xs, lsem.at[1])

    def turn_x(jb):
        @pl.loop(0, 8)
        def _(b):
            to = pl.ds(pl.multiple_of(b * BLOCK, BLOCK), BLOCK)
            cols = pl.ds(pl.multiple_of((2 * b + 1 - place.core) * BLOCK, BLOCK), BLOCK)
            xsend[to, :] = xs[:, cols].T

        x_swap(jb).start()

        @pl.loop(0, 8)
        def _(b):
            to = pl.ds(pl.multiple_of(b * BLOCK, BLOCK), BLOCK)
            cols = pl.ds(pl.multiple_of((2 * b + place.core) * BLOCK, BLOCK), BLOCK)
            xt[jb, to, pl.ds(0, rows)] = xs[:, cols].T

    def sums_of(j):
        return exchange_parts(place, psum, parts, sums_ref.at[j], (asend, arecv, csend, crecv, fsend, frecv))[1:]

    def layer_chunk(j, jb, c, buf):
        cols = columns(c)
        wait_w(buf)
        wait_n(buf)
        for view in range(2):
            first = jnp.zeros((1, COLS), jnp.float32)
            second = jnp.zeros((1, COLS), jnp.float32)
            for part in range(2):
                at = pl.ds(view * view_rows + part * (view_rows // 2), view_rows // 2)
                grad = lax.dot_general(own[jb, at, :], wbuf[buf], (((1,), (1,)), ((), ())),
                                       preferred_element_type=jnp.float32)
                normed = nbuf[buf, at, :]
                grad = jnp.where(gains[j, :, cols] * normed + shifts[j, :, cols] > 0, grad, 0.0)
                gp[at, cols] = grad
                first += jnp.sum(grad, axis=0, keepdims=True)
                second += jnp.sum(grad * normed, axis=0, keepdims=True)
            psum[view, :, cols] = first
            psum[view, :, pl.ds(pl.multiple_of(width + c * COLS, COLS), COLS)] = second

    def norm_chunk(j, jn, c, buf):
        cols = columns(c)
        wait_n(buf)
        for view in range(2):
            at = pl.ds(view * view_rows, view_rows)
            first = sums_ref[j, view, :, cols]
            second = sums_ref[j, view, :, pl.ds(pl.multiple_of(width + c * COLS, COLS), COLS)]
            grad = invs[j, view, :, cols] * (gp[at, cols] - (first + nbuf[buf, at, :] * second) * inv_rows)
            own[jn, at, cols] = (gains[j, :, cols] * grad).astype(jnp.bfloat16)
        swap(jn, c).start()

    load_d = pltpu.make_async_copy(dz_hbm, own.at[0], lsem.at[0])
    load_d.start()
    load_x(x2_hbm).start()
    for buf in range(2):
        load_w(0, buf, buf)
        load_n(0, buf, buf)
    greet([partner] + peers)
    load_d.wait()

    @pl.loop(0, chunks)
    def _(c):
        swap(0, c).start()

    load_x(x2_hbm).wait()
    turn_x(0)

    @pl.loop(0, jobs * chunks + 3)
    def _(t):
        j = t // chunks
        n = lax.rem(t, chunks)
        jb = lax.rem(j, 2)
        jn = 1 - jb
        phase = lax.rem(t, 3)

        @pl.when(t < jobs * chunks)
        def _():
            for s in range(3):
                @pl.when((phase == s) & (t >= RING))
                def _():
                    ring.wait_sends(t - RING, s - RING)

            @pl.when(n == 0)
            def _():
                x_swap(jb).wait_recv()
            swap(jb, n).wait_recv()
            cols = columns(n)
            slot = lax.rem(t, RING)
            for half in range(2):
                feats = pl.ds(512 * half, 512)
                part = jnp.dot(xt[jb, feats, pl.ds(0, rows)], own[jb, :, cols], preferred_element_type=jnp.float32)
                part += jnp.dot(xt[jb, feats, pl.ds(rows, rows)], other[jb, :, cols],
                                preferred_element_type=jnp.float32)
                acc[slot, half] = part.reshape(2, 2, BLOCK, COLS)

        for s in range(3):
            @pl.when(phase == s)
            def _():
                @pl.when(t < jobs * chunks)
                def _():
                    ring.send(0, t, s)

                for step in range(2):
                    u = t - 1 - step

                    @pl.when((u >= 0) & (u < jobs * chunks))
                    def _():
                        ring.add(step, u, s - 1 - step)
                        ring.send(step + 1, u, s - 1 - step)

                @pl.when(t >= 3)
                def _():
                    u = t - 3
                    for r in range(3):
                        off, size, val = ring.result(u, s - 3, r)
                        out_ref[u // chunks, pl.ds(off, size), columns(lax.rem(u, chunks))] = val

        @pl.when(j < jobs - 1)
        def _():
            start, chips, finish, close = sums_of(j)

            @pl.when(n < 4)
            def _():
                for buf in range(2):
                    c = 2 * n + buf
                    layer_chunk(j, jb, c, buf)

                    @pl.when(n < 3)
                    def _():
                        load_w(j, c + 2, buf)
                        load_n(j, c + 2, buf)

                    @pl.when(n == 3)
                    def _():
                        load_n(j, buf, buf)

            @pl.when(n == 3)
            def _():
                start()

                @pl.when(j == 0)
                def _():
                    load_x(x1_hbm).start()

                @pl.when(j == 1)
                def _():
                    load_x(x0_hbm).start()

            @pl.when(n == 4)
            def _():
                chips()

            @pl.when(n == 5)
            def _():
                finish()
                load_x(x1_hbm).wait()
                x_swap(jb).wait_send()
                turn_x(jn)

            @pl.when(n == 6)
            def _():
                close()

                @pl.loop(0, chunks)
                def _(c):
                    swap(jb, c).wait_send()

            @pl.when(n >= 6)
            def _():
                @pl.loop(0, 2)
                def _(pair):
                    for buf in range(2):
                        c = (n - 6) * 4 + pair * 2 + buf
                        norm_chunk(j, jn, c, buf)

                        @pl.when(c < chunks - 2)
                        def _():
                            load_n(j, c + 2, buf)

            @pl.when((n == 7) & (j == 0))
            def _():
                for buf in range(2):
                    load_n(1, buf, buf)
                    load_w(1, buf, buf)

    for t in range(jobs * chunks - RING, jobs * chunks):
        ring.wait_sends(t, t)

    @pl.loop(0, chunks)
    def _(c):
        swap(0, c).wait_send()
    x_swap(0).wait_send()


def corr_kernel(inv_rows, lam_ref, x_ref, d_ref, g_ref, loss_ref,
                xt, xsend, dpart, acc, b0, b1, b2, ssem, rsem, psend, precv, gsend, grecv, stage):
    place = Place()
    chunks = d_ref.shape[1] // COLS
    lam = lam_ref[0, 0]
    loss_ref[...] = jnp.zeros_like(loss_ref)

    def gather(step, t, phase, r):
        off, size = row_parts(BF16_SPLIT, phase)[r]
        picks = list(place.coord)
        for k in range(step):
            picks[(r + 2 - k) % 3] = slice(None)
        axis = (r + 2 - step) % 3
        ref = g_ref.at[(*picks, place.core, pl.ds(off, size), columns(t))]
        return remote(ref, ref, gsend.at[t, 3 * step + r], grecv.at[t, 3 * step + r], place.near[axis])

    def across(t):
        ref = g_ref.at[:, :, :, place.core, :, columns(t)]
        return remote(ref, ref, gsend.at[t, 9], grecv.at[t, 9], place.partner)

    def finish(ring, t, phase):
        for r in range(3):
            off, size, val = ring.result(t, phase, r)
            corr = val * inv_rows
            row_id = place.me * BLOCK + off + lax.broadcasted_iota(jnp.int32, corr.shape, 0)
            col_id = t * COLS + lax.broadcasted_iota(jnp.int32, corr.shape, 1)
            diag = row_id == col_id
            gap = 1.0 - corr
            terms = jnp.where(diag, gap * gap, lam * corr * corr)
            loss_ref[...] += jnp.sum(terms, axis=0, keepdims=True)
            grad = jnp.where(diag, -2.0 * gap, 2.0 * lam * corr) * inv_rows
            stage[pl.ds(off, size), :] = grad
        g_ref[(*place.coord, place.core, slice(None), columns(t))] = stage[...].astype(jnp.bfloat16)
        for r in range(3):
            gather(0, t, phase, r).start()

    def extra(t, s):
        for step in range(2):
            u = t - 4 - step

            @pl.when((u >= 0) & (u < chunks))
            def _():
                for r in range(3):
                    gather(step, u, s - 4 - step, r).wait_recv()
                    gather(step + 1, u, s - 4 - step, r).start()

        @pl.when((t >= 6) & (t - 6 < chunks))
        def _():
            for r in range(3):
                gather(2, t - 6, s - 6, r).wait_recv()
            across(t - 6).start()

    product_reduce(place, chunks, x_ref, d_ref, xt, xsend, dpart, acc, (b0, b1, b2),
                   (ssem, rsem, psend, precv), finish, 3, extra)
    for t in range(chunks):
        across(t).wait()
        for step in range(3):
            for r in range(3):
                gather(step, t, t, r).wait_send()


def product_scratch(rows, width):
    chunks = width // COLS
    return [
        pltpu.VMEM((width // 2, 2 * rows), jnp.bfloat16),
        pltpu.VMEM((width // 2, rows), jnp.bfloat16),
        pltpu.VMEM((rows, width), jnp.bfloat16),
        pltpu.VMEM((RING, 2, 2, 2, BLOCK, COLS), jnp.float32),
        pltpu.VMEM((RING, 2, 2, BLOCK, COLS), jnp.float32),
        pltpu.VMEM((RING, 2, BLOCK, COLS), jnp.float32),
        pltpu.VMEM((RING, BLOCK, COLS), jnp.float32),
        pltpu.SemaphoreType.DMA((RING, 9)),
        pltpu.SemaphoreType.DMA((RING, 9)),
        pltpu.SemaphoreType.DMA((chunks + 1,)),
        pltpu.SemaphoreType.DMA((chunks + 1,)),
    ]


VM = pl.BlockSpec(memory_space=pltpu.VMEM)


def back_all(gains, shifts, invs, dz, x2, x1, x0, n2, n1, w3, w2, total_rows):
    rows, width = dz.shape
    chunks = width // COLS
    base = product_scratch(rows, width)
    hbm = pl.BlockSpec(memory_space=pltpu.HBM)
    bf16, f32 = jnp.bfloat16, jnp.float32
    dma = pltpu.SemaphoreType.DMA
    return pl.pallas_call(
        functools.partial(back_kernel, 1.0 / total_rows),
        out_shape=(jax.ShapeDtypeStruct((3, BLOCK, width), f32), jax.ShapeDtypeStruct((2, 2, 1, 2 * width), f32)),
        in_specs=[VM] * 3 + [hbm] * 8, out_specs=(VM, VM),
        scratch_shapes=[
            pltpu.VMEM((2, width // 2, 2 * rows), bf16),
            pltpu.VMEM((width // 2, rows), bf16),
            pltpu.VMEM((rows, width), bf16),
            pltpu.VMEM((2, rows, width), bf16),
            pltpu.VMEM((2, rows, width), bf16),
            *base[3:7],
            pltpu.VMEM((rows, width), f32),
            pltpu.VMEM((2, COLS, width), bf16),
            pltpu.VMEM((2, rows, COLS), f32),
            pltpu.VMEM((3, 1, 2 * width), f32),
            pltpu.VMEM((8, 1, 2 * width), f32),
            *base[7:9], dma((2, chunks + 1)), dma((2, chunks + 1)),
            dma, dma, dma((7,)), dma((7,)), dma, dma, dma((2,)), dma((2,)), dma((2,)),
        ],
        compiler_params=pltpu.CompilerParams(collective_id=1, has_side_effects=True, vmem_limit_bytes=62 << 20),
        name="back_all",
    )(gains, shifts, invs, dz, x2, x1, x0, n2, n1, w3, w2)


def corr_grad(x, d, lam, total_rows):
    rows, width = x.shape
    chunks = width // COLS
    g, loss = pl.pallas_call(
        functools.partial(corr_kernel, 1.0 / total_rows),
        out_shape=(jax.ShapeDtypeStruct((2, 2, 2, 2, BLOCK, width), jnp.bfloat16),
                   jax.ShapeDtypeStruct((1, COLS), jnp.float32)),
        in_specs=[pl.BlockSpec(memory_space=pltpu.SMEM), VM, VM], out_specs=(VM, VM),
        scratch_shapes=product_scratch(rows, width) + [pltpu.SemaphoreType.DMA((chunks, 10))] * 2
        + [pltpu.VMEM((BLOCK, COLS), jnp.float32)],
        compiler_params=pltpu.CompilerParams(collective_id=2, has_side_effects=True, vmem_limit_bytes=56 << 20),
        name="corr_grad",
    )(lam.reshape(1, 1), x, d)
    return g.reshape(width, width), loss


def stats_kernel(p_ref, out_ref, land, parts, psend, precv, csend, crecv, fsend, frecv):
    place = Place()
    peers = []
    for dist in range(1, 8):
        peers.append(lax.rem(place.chip + dist, 8) * 2 + place.core)
    greet([place.partner] + peers)
    first = remote(p_ref.at[1 - place.core], land, psend, precv, place.partner)
    first.start()
    first.wait_recv()
    parts[place.chip] = p_ref[place.core] + land[...]
    copies = []
    for n, peer in enumerate(peers):
        copies.append(remote(parts.at[place.chip], parts.at[place.chip], csend.at[n], crecv.at[n], peer))
        copies[-1].start()
    for copy in copies:
        copy.wait_recv()
    total = parts[0]
    for c in range(1, 8):
        total = total + parts[c]
    out_ref[place.core] = total
    last = remote(out_ref.at[place.core], out_ref.at[place.core], fsend, frecv, place.partner)
    last.start()
    first.wait_send()
    for copy in copies:
        copy.wait_send()
    last.wait()


def all_sum(payload, cid):
    shape = payload.shape
    return pl.pallas_call(
        stats_kernel,
        out_shape=jax.ShapeDtypeStruct(shape, jnp.float32),
        in_specs=[VM], out_specs=VM,
        scratch_shapes=[pltpu.VMEM(shape[1:], jnp.float32), pltpu.VMEM((8,) + shape[1:], jnp.float32),
                        pltpu.SemaphoreType.DMA, pltpu.SemaphoreType.DMA,
                        pltpu.SemaphoreType.DMA((7,)), pltpu.SemaphoreType.DMA((7,)),
                        pltpu.SemaphoreType.DMA, pltpu.SemaphoreType.DMA],
        compiler_params=pltpu.CompilerParams(collective_id=cid, has_side_effects=True),
        name="all_sum",
    )(payload)


def reduce_sums(first, second):
    width = first.shape[1]
    payload = jnp.stack([first, second], axis=1).reshape(2, 8, width // 4)
    total = all_sum(payload, 3).reshape(2, 2, width)
    return total[:, 0], total[:, 1]


def norm_forward(values, total_rows):
    sums, squares = reduce_sums(jnp.sum(values, axis=1), jnp.sum(values * values, axis=1))
    col_mean = sums / total_rows
    inv_std = lax.rsqrt(squares / total_rows - col_mean * col_mean + NORM_EPS)
    return (values - col_mean[:, None, :]) * inv_std[:, None, :], inv_std


def norm_backward(grad_out, normed, inv_std, total_rows):
    sums = reduce_sums(jnp.sum(grad_out, axis=1), jnp.sum(grad_out * normed, axis=1))
    grad_in = inv_std[:, None, :] * (grad_out - (sums[0][:, None, :] + normed * sums[1][:, None, :]) / total_rows)
    return grad_in, sums


def solution(mesh):
    shards = mesh.shape["data"]

    def local_step(h_a, h_b, w_one, w_two, w_three, gain_one, shift_one, gain_two, shift_two, lam_off):
        rows_dev, width = h_a.shape
        total_rows = rows_dev * shards
        feat_rows = jnp.concatenate([h_a, h_b], axis=0)
        hidden_one = jnp.dot(feat_rows, w_one, preferred_element_type=jnp.float32).reshape(2, rows_dev, -1)
        normed_one, inv_one = norm_forward(hidden_one, total_rows)
        pre_one = gain_one * normed_one + shift_one
        act_one = jax.nn.relu(pre_one).astype(jnp.bfloat16)
        hidden_two = jnp.dot(act_one, w_two, preferred_element_type=jnp.float32)
        normed_two, inv_two = norm_forward(hidden_two, total_rows)
        pre_two = gain_two * normed_two + shift_two
        act_two = jax.nn.relu(pre_two).astype(jnp.bfloat16)
        proj_out = jnp.dot(act_two, w_three, preferred_element_type=jnp.float32)
        normed_out, inv_out = norm_forward(proj_out, total_rows)
        embed_pair = normed_out.astype(jnp.bfloat16)
        grad_scaled, loss_part = corr_grad(embed_pair[0], embed_pair[1], lam_off, total_rows)
        grad_embed_a = lax.dot_general(embed_pair[1], grad_scaled, (((1,), (1,)), ((), ())),
                                       preferred_element_type=jnp.float32)
        grad_embed_b = jnp.dot(embed_pair[0], grad_scaled, preferred_element_type=jnp.float32)
        grad_embed = jnp.stack([grad_embed_a, grad_embed_b])
        grad_proj = norm_backward(grad_embed, normed_out, inv_out, total_rows)[0].astype(jnp.bfloat16)
        flat = lambda a: a.reshape(2 * rows_dev, -1)
        weights, sums = back_all(
            jnp.stack([gain_two, gain_one])[:, None], jnp.stack([shift_two, shift_one])[:, None],
            jnp.stack([inv_two, inv_one])[:, :, None],
            flat(grad_proj), flat(act_two), flat(act_one), feat_rows, flat(normed_two), flat(normed_one),
            w_three, w_two, total_rows)
        sums = jnp.sum(sums.reshape(2, 2, 2, width), axis=1)
        loss_block = jnp.pad(loss_part.reshape(1, 2, 128), ((0, 1), (0, 6), (0, 0)))
        loss_total = jnp.sum(all_sum(loss_block, 4)[0])
        return (loss_total, weights[2], weights[1], weights[0],
                sums[1, 1], sums[1, 0], sums[0, 1], sums[0, 0])

    row_spec = P("data", None)
    whole_mat = P(None, None)
    whole_vec = P(None)
    return jax.shard_map(
        local_step, mesh=mesh,
        in_specs=(row_spec, row_spec, whole_mat, whole_mat, whole_mat,
                  whole_vec, whole_vec, whole_vec, whole_vec, P()),
        out_specs=(P(), row_spec, row_spec, row_spec, whole_vec, whole_vec, whole_vec, whole_vec),
        check_vma=False)
```

```python
import functools

import jax
import jax.numpy as jnp
from jax import lax
from jax.experimental import pallas as pl
from jax.experimental.pallas import tpu as pltpu
from jax.sharding import PartitionSpec as P

NORM_EPS = 1e-5
MESH = pl.DeviceIdType.MESH
RING = 4
COLS = 256
BLOCK = 128
PAIR = range(2)
AXES = range(3)
F32_SPLIT = ((48, 40, 40), (40, 48, 40), (40, 40, 48))
BF16_SPLIT = ((48, 48, 32), (32, 48, 48), (48, 32, 48))


LAST_DIMS = (((1,), (1,)), ((), ()))


def odd(n):
    return n % 2


class Place:
    def __init__(self):
        self.me = lax.axis_index("data")
        self.core = lax.rem(self.me, 2)
        self.chip = self.me // 2
        self.coord = (self.chip // 4, lax.rem(self.chip // 2, 2), lax.rem(self.chip, 2))
        self.partner = self.me + 1 - 2 * self.core
        self.near = tuple(self.me + (1 - 2 * c) * w for c, w in zip(self.coord, (8, 4, 2)))


def greet(peers):
    barrier = pltpu.get_barrier_semaphore()
    for peer in peers:
        pl.semaphore_signal(barrier, inc=1, device_id=(peer,), device_id_type=MESH)
    pl.semaphore_wait(barrier, len(peers))


def remote(src, dst, send, recv, peer):
    return pltpu.make_async_remote_copy(src_ref=src, dst_ref=dst, send_sem=send, recv_sem=recv,
                                        device_id=(peer,), device_id_type=MESH)


def row_parts(split, phase):
    sizes = split[phase % 3]
    return tuple((sum(sizes[:r]), sizes[r]) for r in AXES)


class HalvingReduce:
    def __init__(self, place, acc, bufs, ssem, rsem):
        self.place, self.acc, self.bufs, self.ssem, self.rsem = place, acc, bufs, ssem, rsem

    def at(self, t, picks):
        return (lax.rem(t, RING),) + tuple(picks)

    def copy(self, step, t, phase, r):
        slot = lax.rem(t, RING)
        off, size = row_parts(F32_SPLIT, phase)[r]
        rows = pl.ds(off, size)
        picks = [slice(None)] * 3
        for k in range(step):
            axis = (r + k) % 3
            picks[axis] = self.place.coord[axis]
        axis = (r + step) % 3
        picks[axis] = 1 - self.place.coord[axis]
        src = self.acc.at[(slot, *picks, rows, slice(None))]
        dst = self.bufs[step].at[(slot,) + (slice(None),) * (2 - step) + (rows, slice(None))]
        return remote(src, dst, self.ssem.at[slot, 3 * step + r], self.rsem.at[slot, 3 * step + r],
                      self.place.near[axis])

    def send(self, step, t, phase):
        for r in AXES:
            self.copy(step, t, phase, r).start()

    def wait_sends(self, t, phase):
        for step in AXES:
            for r in AXES:
                self.copy(step, t, phase, r).wait_send()

    def add(self, step, t, phase):
        slot = lax.rem(t, RING)
        for r in AXES:
            self.copy(step, t, phase, r).wait_recv()
            off, size = row_parts(F32_SPLIT, phase)[r]
            rows = pl.ds(off, size)
            fixed = {(r + k) % 3 for k in range(step + 1)}
            free = [a for a in range(3) if a not in fixed]
            for n in range(2 ** len(free)):
                picks = list(self.place.coord)
                sub = []
                for pos, a in enumerate(free):
                    bit = (n >> (len(free) - 1 - pos)) & 1
                    picks[a] = bit
                    sub.append(bit)
                where = (slot, *picks, rows, slice(None))
                self.acc[where] = self.acc[where] + self.bufs[step][(slot, *sub, rows, slice(None))]

    def result(self, t, phase, r):
        slot = lax.rem(t, RING)
        self.copy(2, t, phase, r).wait_recv()
        off, size = row_parts(F32_SPLIT, phase)[r]
        rows = pl.ds(off, size)
        return off, size, (self.acc[(slot, *self.place.coord, rows, slice(None))]
                           + self.bufs[2][(slot, rows, slice(None))])


def columns(t, width=COLS):
    return pl.ds(pl.multiple_of(t * width, width), width)


def product_reduce(place, chunks, x_ref, d_ref, xt, xsend, dpart, acc, bufs, sems, finish, extra_slots, extra):
    ssem, rsem, psend, precv = sems
    rows = x_ref.shape[0]
    partner = place.partner
    greet((partner,) + place.near)

    def swap(t):
        cols = columns(t)
        return remote(d_ref.at[:, cols], dpart.at[:, cols], psend.at[t], precv.at[t], partner)

    @pl.loop(0, chunks)
    def _(t):
        swap(t).start()

    @pl.loop(0, 8)
    def _(b):
        to = pl.ds(pl.multiple_of(b * BLOCK, BLOCK), BLOCK)
        other = pl.ds(pl.multiple_of((2 * b + 1 - place.core) * BLOCK, BLOCK), BLOCK)
        xsend[to, :] = x_ref[:, other].T

    x_swap = remote(xsend, xt.at[:, pl.ds(rows, rows)], psend.at[chunks], precv.at[chunks], partner)
    x_swap.start()

    @pl.loop(0, 8)
    def _(b):
        to = pl.ds(pl.multiple_of(b * BLOCK, BLOCK), BLOCK)
        own = pl.ds(pl.multiple_of((2 * b + place.core) * BLOCK, BLOCK), BLOCK)
        xt[to, pl.ds(0, rows)] = x_ref[:, own].T

    x_swap.wait_recv()
    ring = HalvingReduce(place, acc, bufs, ssem, rsem)

    def slot_step(t, s):
        @pl.when(t < chunks)
        def _():
            @pl.when(t >= RING)
            def _():
                ring.wait_sends(t - RING, s - RING)
            swap(t).wait_recv()
            cols = columns(t)
            slot = lax.rem(t, RING)
            for half in PAIR:
                feats = pl.ds(512 * half, 512)
                part = jnp.dot(xt[feats, pl.ds(0, rows)], d_ref[:, cols], preferred_element_type=jnp.float32)
                part += jnp.dot(xt[feats, pl.ds(rows, rows)], dpart[:, cols], preferred_element_type=jnp.float32)
                acc[slot, half] = part.reshape(2, 2, BLOCK, COLS)
            ring.send(0, t, s)

        for step in PAIR:
            u = t - 1 - step

            @pl.when((u >= 0) & (u < chunks))
            def _():
                ring.add(step, u, s - 1 - step)
                ring.send(step + 1, u, s - 1 - step)

        @pl.when((t >= 3) & (t - 3 < chunks))
        def _():
            finish(ring, t - 3, s - 3)

        extra(t, s)

    @pl.loop(0, (chunks + 3 + extra_slots + 2) // 3)
    def _(q):
        for s in AXES:
            slot_step(3 * q + s, s)

    for t in range(chunks - RING, chunks):
        ring.wait_sends(t, t)

    @pl.loop(0, chunks)
    def _(t):
        swap(t).wait_send()
    x_swap.wait_send()


def exchange_parts(place, psum, parts, total, sems):
    asend, arecv, csend, crecv, fsend, frecv = sems
    peers = [lax.rem(place.chip + dist, 8) * 2 + place.core for dist in range(1, 8)]
    other = 1 - place.core
    land = psum.at[2]
    first = remote(psum.at[other], land, asend, arecv, place.partner)
    mine = parts.at[place.chip]
    across = [remote(mine, mine, csend.at[n], crecv.at[n], peer) for n, peer in enumerate(peers)]
    last = remote(total.at[place.core], total.at[place.core], fsend, frecv, place.partner)

    def start():
        first.start()

    def chips():
        first.wait_recv()
        parts[place.chip] = psum[place.core] + psum[2]
        for copy in across:
            copy.start()

    def finish():
        for copy in across:
            copy.wait_recv()
        value = parts[0]
        for c in range(1, 8):
            value = value + parts[c]
        total[place.core] = value
        last.start()

    def close():
        last.wait_recv()
        first.wait_send()
        for copy in across:
            copy.wait_send()
        last.wait_send()

    return peers, start, chips, finish, close


def forward_kernel(inv_rows, gains, shifts, ha, hb, w1, w2, w3, n1, n2, n3, x1, x2, x3, inv_ref,
                   xbuf, ubuf, wbuf, psum, parts, total, hsem, wsem, usem, xsem,
                   asend, arecv, csend, crecv, fsend, frecv):
    place = Place()
    view_rows, width = ha.shape
    chunks = width // COLS
    half = width // 2
    per = chunks // 2
    weights = (w1, w2, w3)
    normed_out = (n1, n2, n3)
    act_out = (x1, x2, x3)

    def load_w(l, c):
        cols = columns(c)
        return pltpu.make_async_copy(weights[l].at[:, cols], wbuf.at[odd(l), :, cols], wsem.at[odd(l), c])

    loads = [pltpu.make_async_copy(ref, xbuf.at[0, pl.ds(view * view_rows, view_rows), :], hsem.at[view])
             for view, ref in enumerate((ha, hb))]
    for load in loads:
        load.start()
    for l in PAIR:
        @pl.loop(0, chunks)
        def _(c):
            load_w(l, c).start()

    rings = [exchange_parts(place, psum.at[g], parts.at[g], total.at[g],
                            tuple(sem.at[g] for sem in (asend, arecv, csend, crecv, fsend, frecv)))
             for g in range(2)]
    greet([place.partner] + rings[0][0])
    for load in loads:
        load.wait()

    def products(l, lo, hi, start, stop, add, sums, at_chunk=None, action=None):
        depth = pl.ds(start, stop - start)

        @pl.loop(lo, hi)
        def _(c):
            if start == 0:
                load_w(l, c).wait()
            if action is not None:
                pl.when(c == at_chunk)(action)
            cols = columns(c)
            for view in PAIR:
                at = pl.ds(view * view_rows, view_rows)
                value = jnp.dot(xbuf[odd(l), at, depth], wbuf[odd(l), depth, cols], preferred_element_type=jnp.float32)
                if add:
                    value += ubuf[odd(l), at, cols]
                ubuf[odd(l), at, cols] = value
                if sums:
                    g = lo // per
                    local = columns(c - lo)
                    psum[g, view, :, local] = jnp.sum(value, axis=0, keepdims=True)
                    psum[g, view, :, pl.ds(pl.multiple_of(half + (c - lo) * COLS, COLS), COLS)] = jnp.sum(
                        value * value, axis=0, keepdims=True)

    def outputs(l, g):
        cols = pl.ds(g * half, half)
        return (pltpu.make_async_copy(ubuf.at[odd(l), :, cols], normed_out[l].at[:, cols], usem.at[odd(l), g]),
                pltpu.make_async_copy(xbuf.at[odd(l + 1), :, cols], act_out[l].at[:, cols], xsem.at[odd(l), g]))

    def normalise(l, g):
        @pl.loop(0, per)
        def _(k):
            cols = columns(g * per + k)
            for view in PAIR:
                at = pl.ds(view * view_rows, view_rows)
                mean = total[g, view, :, columns(k)] * inv_rows
                square = total[g, view, :, pl.ds(pl.multiple_of(half + k * COLS, COLS), COLS)] * inv_rows
                inv = lax.rsqrt(square - mean * mean + NORM_EPS)
                inv_ref[l, view, :, cols] = inv
                normed = (ubuf[odd(l), at, cols] - mean) * inv
                ubuf[odd(l), at, cols] = normed
                if l < 2:
                    act = jnp.maximum(gains[l, :, cols] * normed + shifts[l, :, cols], 0.0)
                else:
                    act = normed
                xbuf[odd(l + 1), at, cols] = act.astype(jnp.bfloat16)
        for copy in outputs(l, g):
            copy.start()

    for l in AXES:
        first, second = rings[0][1:], rings[1][1:]
        if l == 0:
            products(l, 0, per, 0, width, False, True)
        else:
            products(l, 0, per, half, width, True, True)
        first[0]()
        products(l, per, chunks, 0, width, False, True, per + 1, first[1])
        second[0]()
        if l == 0:
            @pl.loop(0, chunks)
            def _(c):
                load_w(2, c).start()
        first[2]()
        first[3]()
        if l == 2:
            for g in PAIR:
                outputs(0, g)[1].wait()
        normalise(l, 0)
        if l < 2:
            if l == 1:
                for g in PAIR:
                    outputs(0, g)[0].wait()
            products(l + 1, 0, per, 0, half, False, False, 1, second[1])
        else:
            second[1]()
        second[2]()
        second[3]()
        normalise(l, 1)

    for l in (1, 2):
        for g in PAIR:
            for copy in outputs(l, g):
                copy.wait()


def forward_all(gains, shifts, h_a, h_b, w1, w2, w3, total_rows):
    view_rows, width = h_a.shape
    rows = 2 * view_rows
    chunks = width // COLS
    hbm = pl.BlockSpec(memory_space=pltpu.HBM)
    bf16, f32 = jnp.bfloat16, jnp.float32
    dma = pltpu.SemaphoreType.DMA
    normed = jax.ShapeDtypeStruct((rows, width), f32)
    act = jax.ShapeDtypeStruct((rows, width), bf16)
    return pl.pallas_call(
        functools.partial(forward_kernel, 1.0 / total_rows),
        out_shape=(normed,) * 3 + (act,) * 3 + (jax.ShapeDtypeStruct((3, 2, 1, width), f32),),
        in_specs=[VM] * 2 + [hbm] * 5, out_specs=(hbm,) * 6 + (VM,),
        scratch_shapes=[
            pltpu.VMEM((2, rows, width), bf16),
            pltpu.VMEM((2, rows, width), f32),
            pltpu.VMEM((2, width, width), bf16),
            pltpu.VMEM((2, 3, 1, width), f32),
            pltpu.VMEM((2, 8, 1, width), f32),
            pltpu.VMEM((2, 2, 1, width), f32),
            dma((2,)), dma((2, chunks)), dma((2, 2)), dma((2, 2)),
            dma((2,)), dma((2,)), dma((2, 7)), dma((2, 7)), dma((2,)), dma((2,)),
        ],
        compiler_params=pltpu.CompilerParams(collective_id=3, has_side_effects=True, vmem_limit_bytes=60 << 20),
        name="forward_all",
    )(gains, shifts, h_a, h_b, w1, w2, w3)


def back_kernel(inv_rows, gains, shifts, invs, dz_hbm, x2_hbm, x1_hbm, ha_hbm, hb_hbm, n2_hbm, n1_hbm, w3_hbm, w2_hbm,
                out_ref, sums_ref, xt, xsend, xs, own, other, acc, b0, b1, b2, gp, wbuf, nbuf, psum, parts,
                ssem, rsem, psend, precv, asend, arecv, csend, crecv, fsend, frecv, lsem, wsem, nsem):
    place = Place()
    rows, width = dz_hbm.shape
    view_rows = rows // 2
    chunks = width // COLS
    jobs = 3
    peers = [lax.rem(place.chip + dist, 8) * 2 + place.core for dist in range(1, 8)]
    partner = place.partner
    ring = HalvingReduce(place, acc, (b0, b1, b2), ssem, rsem)

    def load_w(j, c, buf):
        rows_c = columns(c)
        for k, ref in enumerate((w3_hbm, w2_hbm)):
            @pl.when(j == k)
            def _():
                pltpu.make_async_copy(ref.at[rows_c, :], wbuf.at[buf], wsem.at[buf]).start()

    def load_n(j, c, buf):
        for k, ref in enumerate((n2_hbm, n1_hbm)):
            @pl.when(j == k)
            def _():
                pltpu.make_async_copy(ref.at[:, columns(c)], nbuf.at[buf], nsem.at[buf]).start()

    def wait_w(buf):
        pltpu.make_async_copy(w3_hbm.at[pl.ds(0, COLS), :], wbuf.at[buf], wsem.at[buf]).wait()

    def wait_n(buf):
        pltpu.make_async_copy(n2_hbm.at[:, pl.ds(0, COLS)], nbuf.at[buf], nsem.at[buf]).wait()

    def swap(jb, c):
        cols = columns(c)
        return remote(own.at[jb, :, cols], other.at[jb, :, cols], psend.at[jb, c], precv.at[jb, c], partner)

    def x_swap(jb):
        return remote(xsend, xt.at[jb, :, pl.ds(rows, rows)], psend.at[jb, chunks], precv.at[jb, chunks], partner)

    def load_x(ref):
        return pltpu.make_async_copy(ref, xs, lsem.at[1])

    def turn_x(jb):
        @pl.loop(0, 8)
        def _(b):
            to = pl.ds(pl.multiple_of(b * BLOCK, BLOCK), BLOCK)
            cols = pl.ds(pl.multiple_of((2 * b + 1 - place.core) * BLOCK, BLOCK), BLOCK)
            xsend[to, :] = xs[:, cols].T

        x_swap(jb).start()

        @pl.loop(0, 8)
        def _(b):
            to = pl.ds(pl.multiple_of(b * BLOCK, BLOCK), BLOCK)
            cols = pl.ds(pl.multiple_of((2 * b + place.core) * BLOCK, BLOCK), BLOCK)
            xt[jb, to, pl.ds(0, rows)] = xs[:, cols].T

    def sums_of(j):
        return exchange_parts(place, psum, parts, sums_ref.at[j], (asend, arecv, csend, crecv, fsend, frecv))[1:]

    def layer_chunk(j, jb, c, buf):
        cols = columns(c)
        wait_w(buf)
        wait_n(buf)
        for view in PAIR:
            first = jnp.zeros((1, COLS), jnp.float32)
            second = jnp.zeros((1, COLS), jnp.float32)
            for part in PAIR:
                at = pl.ds(view * view_rows + part * (view_rows // 2), view_rows // 2)
                grad = lax.dot_general(own[jb, at, :], wbuf[buf], LAST_DIMS,
                                       preferred_element_type=jnp.float32)
                normed = nbuf[buf, at, :]
                grad = jnp.where(gains[j, :, cols] * normed + shifts[j, :, cols] > 0, grad, 0.0)
                gp[at, cols] = grad
                first += jnp.sum(grad, axis=0, keepdims=True)
                second += jnp.sum(grad * normed, axis=0, keepdims=True)
            psum[view, :, cols] = first
            psum[view, :, pl.ds(pl.multiple_of(width + c * COLS, COLS), COLS)] = second

    def norm_chunk(j, jn, c, buf):
        cols = columns(c)
        wait_n(buf)
        for view in PAIR:
            at = pl.ds(view * view_rows, view_rows)
            first = sums_ref[j, view, :, cols]
            second = sums_ref[j, view, :, pl.ds(pl.multiple_of(width + c * COLS, COLS), COLS)]
            grad = invs[j, view, :, cols] * (gp[at, cols] - (first + nbuf[buf, at, :] * second) * inv_rows)
            own[jn, at, cols] = (gains[j, :, cols] * grad).astype(jnp.bfloat16)
        swap(jn, c).start()

    load_d = pltpu.make_async_copy(dz_hbm, own.at[0], lsem.at[0])
    load_d.start()
    load_x(x2_hbm).start()
    for buf in PAIR:
        load_w(0, buf, buf)
        load_n(0, buf, buf)
    greet([partner] + peers)
    load_d.wait()

    @pl.loop(0, chunks)
    def _(c):
        swap(0, c).start()

    load_x(x2_hbm).wait()
    turn_x(0)

    @pl.loop(0, jobs * chunks + 3)
    def _(t):
        j = t // chunks
        n = lax.rem(t, chunks)
        jb = lax.rem(j, 2)
        jn = 1 - jb
        phase = lax.rem(t, 3)

        @pl.when(t < jobs * chunks)
        def _():
            for s in AXES:
                @pl.when((phase == s) & (t >= RING))
                def _():
                    ring.wait_sends(t - RING, s - RING)

            @pl.when(n == 0)
            def _():
                x_swap(jb).wait_recv()
            swap(jb, n).wait_recv()
            cols = columns(n)
            slot = lax.rem(t, RING)
            for half in PAIR:
                feats = pl.ds(512 * half, 512)
                part = jnp.dot(xt[jb, feats, pl.ds(0, rows)], own[jb, :, cols], preferred_element_type=jnp.float32)
                part += jnp.dot(xt[jb, feats, pl.ds(rows, rows)], other[jb, :, cols],
                                preferred_element_type=jnp.float32)
                acc[slot, half] = part.reshape(2, 2, BLOCK, COLS)

        for s in AXES:
            @pl.when(phase == s)
            def _():
                @pl.when(t < jobs * chunks)
                def _():
                    ring.send(0, t, s)

                for step in PAIR:
                    u = t - 1 - step

                    @pl.when((u >= 0) & (u < jobs * chunks))
                    def _():
                        ring.add(step, u, s - 1 - step)
                        ring.send(step + 1, u, s - 1 - step)

                @pl.when(t >= 3)
                def _():
                    u = t - 3
                    for r in AXES:
                        off, size, val = ring.result(u, s - 3, r)
                        out_ref[u // chunks, pl.ds(off, size), columns(lax.rem(u, chunks))] = val

        @pl.when(j < jobs - 1)
        def _():
            start, chips, finish, close = sums_of(j)

            @pl.when(n < 4)
            def _():
                for buf in PAIR:
                    c = 2 * n + buf
                    layer_chunk(j, jb, c, buf)

                    @pl.when(n < 3)
                    def _():
                        load_w(j, c + 2, buf)
                        load_n(j, c + 2, buf)

                    @pl.when(n == 3)
                    def _():
                        load_n(j, buf, buf)

            @pl.when(n == 3)
            def _():
                start()

                @pl.when(j == 0)
                def _():
                    load_x(x1_hbm).start()

                @pl.when(j == 1)
                def _():
                    for view, ref in enumerate((ha_hbm, hb_hbm)):
                        pltpu.make_async_copy(ref, xs.at[pl.ds(view * view_rows, view_rows), :], lsem.at[1]).start()

            @pl.when(n == 4)
            def _():
                chips()

            @pl.when(n == 5)
            def _():
                finish()
                load_x(x1_hbm).wait()
                x_swap(jb).wait_send()
                turn_x(jn)

            @pl.when(n == 6)
            def _():
                close()

                @pl.loop(0, chunks)
                def _(c):
                    swap(jb, c).wait_send()

            @pl.when(n >= 6)
            def _():
                @pl.loop(0, 2)
                def _(pair):
                    for buf in PAIR:
                        c = (n - 6) * 4 + pair * 2 + buf
                        norm_chunk(j, jn, c, buf)

                        @pl.when(c < chunks - 2)
                        def _():
                            load_n(j, c + 2, buf)

            @pl.when((n == 7) & (j == 0))
            def _():
                for buf in PAIR:
                    load_n(1, buf, buf)
                    load_w(1, buf, buf)

    for t in range(jobs * chunks - RING, jobs * chunks):
        ring.wait_sends(t, t)

    @pl.loop(0, chunks)
    def _(c):
        swap(0, c).wait_send()
    x_swap(0).wait_send()


def corr_kernel(inv_rows, lam_ref, z_ref, g_ref, loss_ref,
                xt, xsend, dpart, acc, b0, b1, b2, ssem, rsem, psend, precv, gsend, grecv, stage):
    place = Place()
    view_rows = z_ref.shape[0] // 2
    x_ref, d_ref = z_ref.at[pl.ds(0, view_rows), :], z_ref.at[pl.ds(view_rows, view_rows), :]
    chunks = z_ref.shape[1] // COLS
    lam = lam_ref[0, 0]
    loss_ref[...] = jnp.zeros_like(loss_ref)

    def gather(step, t, phase, r):
        off, size = row_parts(BF16_SPLIT, phase)[r]
        picks = list(place.coord)
        for k in range(step):
            picks[(r + 2 - k) % 3] = slice(None)
        axis = (r + 2 - step) % 3
        ref = g_ref.at[(*picks, place.core, pl.ds(off, size), columns(t))]
        return remote(ref, ref, gsend.at[t, 3 * step + r], grecv.at[t, 3 * step + r], place.near[axis])

    def across(t):
        ref = g_ref.at[:, :, :, place.core, :, columns(t)]
        return remote(ref, ref, gsend.at[t, 9], grecv.at[t, 9], place.partner)

    def finish(ring, t, phase):
        for r in AXES:
            off, size, val = ring.result(t, phase, r)
            corr = val * inv_rows
            row_id = place.me * BLOCK + off + lax.broadcasted_iota(jnp.int32, corr.shape, 0)
            col_id = t * COLS + lax.broadcasted_iota(jnp.int32, corr.shape, 1)
            diag = row_id == col_id
            gap = 1.0 - corr
            terms = jnp.where(diag, gap * gap, lam * corr * corr)
            loss_ref[...] += jnp.sum(terms, axis=0, keepdims=True)
            grad = jnp.where(diag, -2.0 * gap, 2.0 * lam * corr) * inv_rows
            stage[pl.ds(off, size), :] = grad
        g_ref[(*place.coord, place.core, slice(None), columns(t))] = stage[...].astype(jnp.bfloat16)
        for r in AXES:
            gather(0, t, phase, r).start()

    def extra(t, s):
        for step in PAIR:
            u = t - 4 - step

            @pl.when((u >= 0) & (u < chunks))
            def _():
                for r in AXES:
                    gather(step, u, s - 4 - step, r).wait_recv()
                    gather(step + 1, u, s - 4 - step, r).start()

        @pl.when((t >= 6) & (t - 6 < chunks))
        def _():
            for r in AXES:
                gather(2, t - 6, s - 6, r).wait_recv()
            across(t - 6).start()

    product_reduce(place, chunks, x_ref, d_ref, xt, xsend, dpart, acc, (b0, b1, b2),
                   (ssem, rsem, psend, precv), finish, 3, extra)
    for t in range(chunks):
        across(t).wait()
        for step in AXES:
            for r in AXES:
                gather(step, t, t, r).wait_send()


def product_scratch(rows, width):
    chunks = width // COLS
    return [
        pltpu.VMEM((width // 2, 2 * rows), jnp.bfloat16),
        pltpu.VMEM((width // 2, rows), jnp.bfloat16),
        pltpu.VMEM((rows, width), jnp.bfloat16),
        pltpu.VMEM((RING, 2, 2, 2, BLOCK, COLS), jnp.float32),
        pltpu.VMEM((RING, 2, 2, BLOCK, COLS), jnp.float32),
        pltpu.VMEM((RING, 2, BLOCK, COLS), jnp.float32),
        pltpu.VMEM((RING, BLOCK, COLS), jnp.float32),
        pltpu.SemaphoreType.DMA((RING, 9)),
        pltpu.SemaphoreType.DMA((RING, 9)),
        pltpu.SemaphoreType.DMA((chunks + 1,)),
        pltpu.SemaphoreType.DMA((chunks + 1,)),
    ]


VM = pl.BlockSpec(memory_space=pltpu.VMEM)


def back_all(gains, shifts, invs, dz, x2, x1, h_a, h_b, n2, n1, w3, w2, total_rows):
    rows, width = dz.shape
    chunks = width // COLS
    base = product_scratch(rows, width)
    hbm = pl.BlockSpec(memory_space=pltpu.HBM)
    bf16, f32 = jnp.bfloat16, jnp.float32
    dma = pltpu.SemaphoreType.DMA
    return pl.pallas_call(
        functools.partial(back_kernel, 1.0 / total_rows),
        out_shape=(jax.ShapeDtypeStruct((3, BLOCK, width), f32), jax.ShapeDtypeStruct((2, 2, 1, 2 * width), f32)),
        in_specs=[VM] * 3 + [hbm] * 9, out_specs=(VM, VM),
        scratch_shapes=[
            pltpu.VMEM((2, width // 2, 2 * rows), bf16),
            pltpu.VMEM((width // 2, rows), bf16),
            pltpu.VMEM((rows, width), bf16),
            pltpu.VMEM((2, rows, width), bf16),
            pltpu.VMEM((2, rows, width), bf16),
            *base[3:7],
            pltpu.VMEM((rows, width), f32),
            pltpu.VMEM((2, COLS, width), bf16),
            pltpu.VMEM((2, rows, COLS), f32),
            pltpu.VMEM((3, 1, 2 * width), f32),
            pltpu.VMEM((8, 1, 2 * width), f32),
            *base[7:9], dma((2, chunks + 1)), dma((2, chunks + 1)),
            dma, dma, dma((7,)), dma((7,)), dma, dma, dma((2,)), dma((2,)), dma((2,)),
        ],
        compiler_params=pltpu.CompilerParams(collective_id=1, has_side_effects=True, vmem_limit_bytes=62 << 20),
        name="back_all",
    )(gains, shifts, invs, dz, x2, x1, h_a, h_b, n2, n1, w3, w2)


def corr_grad(z, lam, total_rows):
    rows, width = z.shape[0] // 2, z.shape[1]
    chunks = width // COLS
    g, loss = pl.pallas_call(
        functools.partial(corr_kernel, 1.0 / total_rows),
        out_shape=(jax.ShapeDtypeStruct((2, 2, 2, 2, BLOCK, width), jnp.bfloat16),
                   jax.ShapeDtypeStruct((1, COLS), jnp.float32)),
        in_specs=[pl.BlockSpec(memory_space=pltpu.SMEM), VM], out_specs=(VM, VM),
        scratch_shapes=product_scratch(rows, width) + [pltpu.SemaphoreType.DMA((chunks, 10))] * 2
        + [pltpu.VMEM((BLOCK, COLS), jnp.float32)],
        compiler_params=pltpu.CompilerParams(collective_id=2, has_side_effects=True, vmem_limit_bytes=56 << 20),
        name="corr_grad",
    )(lam.reshape(1, 1), z)
    return g.reshape(width, width), loss


def stats_kernel(p_ref, out_ref, land, parts, psend, precv, csend, crecv, fsend, frecv):
    place = Place()
    peers = []
    for dist in range(1, 8):
        peers.append(lax.rem(place.chip + dist, 8) * 2 + place.core)
    greet([place.partner] + peers)
    first = remote(p_ref.at[1 - place.core], land, psend, precv, place.partner)
    first.start()
    first.wait_recv()
    parts[place.chip] = p_ref[place.core] + land[...]
    copies = []
    for n, peer in enumerate(peers):
        copies.append(remote(parts.at[place.chip], parts.at[place.chip], csend.at[n], crecv.at[n], peer))
        copies[-1].start()
    for copy in copies:
        copy.wait_recv()
    total = parts[0]
    for c in range(1, 8):
        total = total + parts[c]
    out_ref[place.core] = total
    last = remote(out_ref.at[place.core], out_ref.at[place.core], fsend, frecv, place.partner)
    last.start()
    first.wait_send()
    for copy in copies:
        copy.wait_send()
    last.wait()


def all_sum(payload, cid):
    shape = payload.shape
    return pl.pallas_call(
        stats_kernel,
        out_shape=jax.ShapeDtypeStruct(shape, jnp.float32),
        in_specs=[VM], out_specs=VM,
        scratch_shapes=[pltpu.VMEM(shape[1:], jnp.float32), pltpu.VMEM((8,) + shape[1:], jnp.float32),
                        pltpu.SemaphoreType.DMA, pltpu.SemaphoreType.DMA,
                        pltpu.SemaphoreType.DMA((7,)), pltpu.SemaphoreType.DMA((7,)),
                        pltpu.SemaphoreType.DMA, pltpu.SemaphoreType.DMA],
        compiler_params=pltpu.CompilerParams(collective_id=cid, has_side_effects=True),
        name="all_sum",
    )(payload)


def reduce_sums(first, second):
    width = first.shape[1]
    payload = jnp.stack([first, second], axis=1).reshape(2, 8, width // 4)
    total = all_sum(payload, 5).reshape(2, 2, width)
    return total[:, 0], total[:, 1]


def norm_backward(grad_out, normed, inv_std, total_rows):
    sums = reduce_sums(jnp.sum(grad_out, axis=1), jnp.sum(grad_out * normed, axis=1))
    grad_in = inv_std[:, None, :] * (grad_out - (sums[0][:, None, :] + normed * sums[1][:, None, :]) / total_rows)
    return grad_in, sums


def solution(mesh):
    shards = mesh.shape["data"]

    def local_step(h_a, h_b, w_one, w_two, w_three, gain_one, shift_one, gain_two, shift_two, lam_off):
        rows_dev, width = h_a.shape
        total_rows = rows_dev * shards
        normed_one, normed_two, normed_out, act_one, act_two, embed, invs = forward_all(
            jnp.stack([gain_one, gain_two])[:, None], jnp.stack([shift_one, shift_two])[:, None],
            h_a, h_b, w_one, w_two, w_three, total_rows)
        embed_pair = embed.reshape(2, rows_dev, width)
        normed_out = normed_out.reshape(2, rows_dev, width)
        grad_scaled, loss_part = corr_grad(embed, lam_off, total_rows)
        grad_embed_a = lax.dot_general(embed_pair[1], grad_scaled, LAST_DIMS,
                                       preferred_element_type=jnp.float32)
        grad_embed_b = jnp.dot(embed_pair[0], grad_scaled, preferred_element_type=jnp.float32)
        grad_embed = jnp.stack([grad_embed_a, grad_embed_b])
        grad_proj = norm_backward(grad_embed, normed_out, invs[2, :, 0], total_rows)[0].astype(jnp.bfloat16)
        flat = lambda a: a.reshape(2 * rows_dev, -1)
        weights, sums = back_all(
            jnp.stack([gain_two, gain_one])[:, None], jnp.stack([shift_two, shift_one])[:, None],
            jnp.stack([invs[1], invs[0]]),
            flat(grad_proj), act_two, act_one, h_a, h_b, normed_two, normed_one,
            w_three, w_two, total_rows)
        sums = jnp.sum(sums.reshape(2, 2, 2, width), axis=1)
        loss_block = jnp.pad(loss_part.reshape(1, 2, 128), ((0, 1), (0, 6), (0, 0)))
        loss_total = jnp.sum(all_sum(loss_block, 4)[0])
        return (loss_total, weights[2], weights[1], weights[0],
                sums[1, 1], sums[1, 0], sums[0, 1], sums[0, 0])

    row_spec = P("data", None)
    whole_mat = P(None, None)
    whole_vec = P(None)
    return jax.shard_map(
        local_step, mesh=mesh,
        in_specs=(row_spec, row_spec, whole_mat, whole_mat, whole_mat,
                  whole_vec, whole_vec, whole_vec, whole_vec, P()),
        out_specs=(P(), row_spec, row_spec, row_spec, whole_vec, whole_vec, whole_vec, whole_vec),
        check_vma=False)
```

```python
import functools

import jax
import jax.numpy as jnp
from jax import lax
from jax.experimental import pallas as pl
from jax.experimental.pallas import tpu as pltpu
from jax.sharding import PartitionSpec as P

NORM_EPS = 1e-5
MESH = pl.DeviceIdType.MESH
RING = 4
COLS = 256
BLOCK = 128
PAIR = range(2)
AXES = range(3)
F32_SPLIT = ((48, 40, 40), (40, 48, 40), (40, 40, 48))
BF16_SPLIT = ((48, 48, 32), (32, 48, 48), (48, 32, 48))


LAST_DIMS = (((1,), (1,)), ((), ()))


def odd(n):
    return n % 2


class Place:
    def __init__(self):
        self.me = lax.axis_index("data")
        self.core = lax.rem(self.me, 2)
        self.chip = self.me // 2
        self.coord = (self.chip // 4, lax.rem(self.chip // 2, 2), lax.rem(self.chip, 2))
        self.partner = self.me + 1 - 2 * self.core
        self.near = tuple(self.me + (1 - 2 * c) * w for c, w in zip(self.coord, (8, 4, 2)))


def greet(peers):
    barrier = pltpu.get_barrier_semaphore()
    for peer in peers:
        pl.semaphore_signal(barrier, inc=1, device_id=(peer,), device_id_type=MESH)
    pl.semaphore_wait(barrier, len(peers))


def remote(src, dst, send, recv, peer):
    return pltpu.make_async_remote_copy(src_ref=src, dst_ref=dst, send_sem=send, recv_sem=recv,
                                        device_id=(peer,), device_id_type=MESH)


def row_parts(split, phase):
    sizes = split[phase % 3]
    return tuple((sum(sizes[:r]), sizes[r]) for r in AXES)


class HalvingReduce:
    def __init__(self, place, acc, bufs, ssem, rsem):
        self.place, self.acc, self.bufs, self.ssem, self.rsem = place, acc, bufs, ssem, rsem

    def at(self, t, picks):
        return (lax.rem(t, RING),) + tuple(picks)

    def copy(self, step, t, phase, r):
        slot = lax.rem(t, RING)
        off, size = row_parts(F32_SPLIT, phase)[r]
        rows = pl.ds(off, size)
        picks = [slice(None)] * 3
        for k in range(step):
            axis = (r + k) % 3
            picks[axis] = self.place.coord[axis]
        axis = (r + step) % 3
        picks[axis] = 1 - self.place.coord[axis]
        src = self.acc.at[(slot, *picks, rows, slice(None))]
        dst = self.bufs[step].at[(slot,) + (slice(None),) * (2 - step) + (rows, slice(None))]
        return remote(src, dst, self.ssem.at[slot, 3 * step + r], self.rsem.at[slot, 3 * step + r],
                      self.place.near[axis])

    def send(self, step, t, phase):
        for r in AXES:
            self.copy(step, t, phase, r).start()

    def wait_sends(self, t, phase):
        for step in AXES:
            for r in AXES:
                self.copy(step, t, phase, r).wait_send()

    def add(self, step, t, phase):
        slot = lax.rem(t, RING)
        for r in AXES:
            self.copy(step, t, phase, r).wait_recv()
            off, size = row_parts(F32_SPLIT, phase)[r]
            rows = pl.ds(off, size)
            fixed = {(r + k) % 3 for k in range(step + 1)}
            free = [a for a in range(3) if a not in fixed]
            for n in range(2 ** len(free)):
                picks = list(self.place.coord)
                sub = []
                for pos, a in enumerate(free):
                    bit = (n >> (len(free) - 1 - pos)) & 1
                    picks[a] = bit
                    sub.append(bit)
                where = (slot, *picks, rows, slice(None))
                self.acc[where] = self.acc[where] + self.bufs[step][(slot, *sub, rows, slice(None))]

    def result(self, t, phase, r):
        slot = lax.rem(t, RING)
        self.copy(2, t, phase, r).wait_recv()
        off, size = row_parts(F32_SPLIT, phase)[r]
        rows = pl.ds(off, size)
        return off, size, (self.acc[(slot, *self.place.coord, rows, slice(None))]
                           + self.bufs[2][(slot, rows, slice(None))])


def columns(t, width=COLS):
    return pl.ds(pl.multiple_of(t * width, width), width)


def exchange_parts(place, psum, parts, total, sems):
    asend, arecv, csend, crecv, fsend, frecv = sems
    peers = [lax.rem(place.chip + dist, 8) * 2 + place.core for dist in range(1, 8)]
    other = 1 - place.core
    land = psum.at[2]
    first = remote(psum.at[other], land, asend, arecv, place.partner)
    mine = parts.at[place.chip]
    across = [remote(mine, mine, csend.at[n], crecv.at[n], peer) for n, peer in enumerate(peers)]
    last = remote(total.at[place.core], total.at[place.core], fsend, frecv, place.partner)

    def start():
        first.start()

    def chips():
        first.wait_recv()
        parts[place.chip] = psum[place.core] + psum[2]
        for copy in across:
            copy.start()

    def finish():
        for copy in across:
            copy.wait_recv()
        value = parts[0]
        for c in range(1, 8):
            value = value + parts[c]
        total[place.core] = value
        last.start()

    def close():
        last.wait_recv()
        first.wait_send()
        for copy in across:
            copy.wait_send()
        last.wait_send()

    return peers, start, chips, finish, close


def forward_kernel(inv_rows, gains, shifts, ha, hb, w1, w2, w3, n1, n2, n3, x1, x2, x3, inv_ref,
                   xbuf, ubuf, wbuf, psum, parts, total, hsem, wsem, usem, xsem,
                   asend, arecv, csend, crecv, fsend, frecv):
    place = Place()
    view_rows, width = ha.shape
    chunks = width // COLS
    half = width // 2
    per = chunks // 2
    weights = (w1, w2, w3)
    normed_out = (n1, n2, n3)
    act_out = (x1, x2, x3)

    def load_w(l, c):
        cols = columns(c)
        return pltpu.make_async_copy(weights[l].at[:, cols], wbuf.at[odd(l), :, cols], wsem.at[odd(l), c])

    loads = [pltpu.make_async_copy(ref, xbuf.at[0, pl.ds(view * view_rows, view_rows), :], hsem.at[view])
             for view, ref in enumerate((ha, hb))]
    for load in loads:
        load.start()
    for l in PAIR:
        @pl.loop(0, chunks)
        def _(c):
            load_w(l, c).start()

    rings = [exchange_parts(place, psum.at[g], parts.at[g], total.at[g],
                            tuple(sem.at[g] for sem in (asend, arecv, csend, crecv, fsend, frecv)))
             for g in range(2)]
    greet([place.partner] + rings[0][0])
    for load in loads:
        load.wait()

    def products(l, lo, hi, start, stop, add, sums, at_chunk=None, action=None):
        depth = pl.ds(start, stop - start)

        @pl.loop(lo, hi)
        def _(c):
            if start == 0:
                load_w(l, c).wait()
            if action is not None:
                pl.when(c == at_chunk)(action)
            cols = columns(c)
            for view in PAIR:
                at = pl.ds(view * view_rows, view_rows)
                value = jnp.dot(xbuf[odd(l), at, depth], wbuf[odd(l), depth, cols], preferred_element_type=jnp.float32)
                if add:
                    value += ubuf[odd(l), at, cols]
                ubuf[odd(l), at, cols] = value
                if sums:
                    g = lo // per
                    local = columns(c - lo)
                    psum[g, view, :, local] = jnp.sum(value, axis=0, keepdims=True)
                    psum[g, view, :, pl.ds(pl.multiple_of(half + (c - lo) * COLS, COLS), COLS)] = jnp.sum(
                        value * value, axis=0, keepdims=True)

    def outputs(l, g):
        cols = pl.ds(g * half, half)
        return (pltpu.make_async_copy(ubuf.at[odd(l), :, cols], normed_out[l].at[:, cols], usem.at[odd(l), g]),
                pltpu.make_async_copy(xbuf.at[odd(l + 1), :, cols], act_out[l].at[:, cols], xsem.at[odd(l), g]))

    def normalise(l, g):
        @pl.loop(0, per)
        def _(k):
            cols = columns(g * per + k)
            for view in PAIR:
                at = pl.ds(view * view_rows, view_rows)
                mean = total[g, view, :, columns(k)] * inv_rows
                square = total[g, view, :, pl.ds(pl.multiple_of(half + k * COLS, COLS), COLS)] * inv_rows
                inv = lax.rsqrt(square - mean * mean + NORM_EPS)
                inv_ref[2 - l, view, :, cols] = inv
                normed = (ubuf[odd(l), at, cols] - mean) * inv
                ubuf[odd(l), at, cols] = normed
                if l < 2:
                    act = jnp.maximum(gains[l, :, cols] * normed + shifts[l, :, cols], 0.0)
                else:
                    act = normed
                xbuf[odd(l + 1), at, cols] = act.astype(jnp.bfloat16)
        for copy in outputs(l, g):
            copy.start()

    for l in AXES:
        first, second = rings[0][1:], rings[1][1:]
        if l == 0:
            products(l, 0, per, 0, width, False, True)
        else:
            products(l, 0, per, half, width, True, True)
        first[0]()
        products(l, per, chunks, 0, width, False, True, per + 1, first[1])
        second[0]()
        if l == 0:
            @pl.loop(0, chunks)
            def _(c):
                load_w(2, c).start()
        first[2]()
        first[3]()
        if l == 2:
            for g in PAIR:
                outputs(0, g)[1].wait()
        normalise(l, 0)
        if l < 2:
            if l == 1:
                for g in PAIR:
                    outputs(0, g)[0].wait()
            products(l + 1, 0, per, 0, half, False, False, 1, second[1])
        else:
            second[1]()
        second[2]()
        second[3]()
        normalise(l, 1)

    for l in (1, 2):
        for g in PAIR:
            for copy in outputs(l, g):
                copy.wait()


def forward_all(gains, shifts, h_a, h_b, w1, w2, w3, total_rows):
    view_rows, width = h_a.shape
    rows = 2 * view_rows
    chunks = width // COLS
    hbm = pl.BlockSpec(memory_space=pltpu.HBM)
    bf16, f32 = jnp.bfloat16, jnp.float32
    dma = pltpu.SemaphoreType.DMA
    normed = jax.ShapeDtypeStruct((rows, width), f32)
    act = jax.ShapeDtypeStruct((rows, width), bf16)
    return pl.pallas_call(
        functools.partial(forward_kernel, 1.0 / total_rows),
        out_shape=(normed,) * 3 + (act,) * 3 + (jax.ShapeDtypeStruct((3, 2, 1, width), f32),),
        in_specs=[VM] * 2 + [hbm] * 5, out_specs=(hbm,) * 6 + (VM,),
        scratch_shapes=[
            pltpu.VMEM((2, rows, width), bf16),
            pltpu.VMEM((2, rows, width), f32),
            pltpu.VMEM((2, width, width), bf16),
            pltpu.VMEM((2, 3, 1, width), f32),
            pltpu.VMEM((2, 8, 1, width), f32),
            pltpu.VMEM((2, 2, 1, width), f32),
            dma((2,)), dma((2, chunks)), dma((2, 2)), dma((2, 2)),
            dma((2,)), dma((2,)), dma((2, 7)), dma((2, 7)), dma((2,)), dma((2,)),
        ],
        compiler_params=pltpu.CompilerParams(collective_id=3, has_side_effects=True, vmem_limit_bytes=60 << 20),
        name="forward_all",
    )(gains, shifts, h_a, h_b, w1, w2, w3)


def back_kernel(inv_rows, lam_ref, gains, shifts, invs, z_hbm, x2_hbm, x1_hbm, ha_hbm, hb_hbm, n3_hbm, n2_hbm, n1_hbm,
                w3_hbm, w2_hbm, out_ref, vec_ref, loss_ref,
                xt, xsend, xs, own, other, acc, b0, b1, b2, gp, wbuf, nbuf, psum, parts, sums_ref, grads, stage,
                ssem, rsem, psend, precv, asend, arecv, csend, crecv, fsend, frecv, lsem, wsem, nsem, gsend, grecv):
    place = Place()
    rows, width = z_hbm.shape
    view_rows = rows // 2
    chunks = width // COLS
    jobs = 3
    peers = [lax.rem(place.chip + dist, 8) * 2 + place.core for dist in range(1, 8)]
    partner = place.partner
    ring = HalvingReduce(place, acc, (b0, b1, b2), ssem, rsem)

    def load_w(j, c, buf):
        rows_c = columns(c)
        for k, ref in enumerate((w3_hbm, w2_hbm)):
            @pl.when(j == k)
            def _():
                pltpu.make_async_copy(ref.at[rows_c, :], wbuf.at[buf], wsem.at[buf]).start()

    def load_z(c, buf):
        pltpu.make_async_copy(n3_hbm.at[:, columns(c)], nbuf.at[buf], nsem.at[buf]).start()

    def load_n(j, c, buf):
        for k, ref in enumerate((n2_hbm, n1_hbm)):
            @pl.when(j == k)
            def _():
                pltpu.make_async_copy(ref.at[:, columns(c)], nbuf.at[buf], nsem.at[buf]).start()

    def wait_w(buf):
        pltpu.make_async_copy(w3_hbm.at[pl.ds(0, COLS), :], wbuf.at[buf], wsem.at[buf]).wait()

    def wait_n(buf):
        pltpu.make_async_copy(n2_hbm.at[:, pl.ds(0, COLS)], nbuf.at[buf], nsem.at[buf]).wait()

    def swap(jb, c):
        cols = columns(c)
        return remote(own.at[jb, :, cols], other.at[jb, :, cols], psend.at[jb, c], precv.at[jb, c], partner)

    def x_swap(jb):
        return remote(xsend, xt.at[jb, :, pl.ds(rows, rows)], psend.at[jb, chunks], precv.at[jb, chunks], partner)

    def load_x(ref):
        return pltpu.make_async_copy(ref, xs, lsem.at[1])

    def turn(src, depth, copy, jb):
        def blocks(dst, parity):
            @pl.loop(0, 8)
            def _(b):
                to = pl.ds(pl.multiple_of(b * BLOCK, BLOCK), BLOCK)
                cols = pl.ds(pl.multiple_of((2 * b + parity) * BLOCK, BLOCK), BLOCK)
                dst[to, pl.ds(0, depth)] = src[pl.ds(0, depth), cols].T

        blocks(xsend, 1 - place.core)
        copy.start()
        blocks(xt.at[jb], place.core)

    def turn_x(src, jb):
        turn(src, rows, x_swap(jb), jb)

    def sums_of(i):
        return exchange_parts(place, psum, parts, sums_ref.at[i], (asend, arecv, csend, crecv, fsend, frecv))[1:]

    def wide(c):
        return pl.ds(pl.multiple_of(width + c * COLS, COLS), COLS)

    def layer_chunk(j, jb, c, buf):
        cols = columns(c)
        wait_w(buf)
        wait_n(buf)
        for view in PAIR:
            first = jnp.zeros((1, COLS), jnp.float32)
            second = jnp.zeros((1, COLS), jnp.float32)
            for part in PAIR:
                at = pl.ds(view * view_rows + part * (view_rows // 2), view_rows // 2)
                grad = lax.dot_general(own[jb, at, :], wbuf[buf], LAST_DIMS,
                                       preferred_element_type=jnp.float32)
                normed = nbuf[buf, at, :]
                grad = jnp.where(gains[1 - j, :, cols] * normed + shifts[1 - j, :, cols] > 0, grad, 0.0)
                gp[at, cols] = grad
                first += jnp.sum(grad, axis=0, keepdims=True)
                second += jnp.sum(grad * normed, axis=0, keepdims=True)
            psum[view, :, cols] = first
            psum[view, :, wide(c)] = second

    def norm_chunk(i, gain, jn, c, buf):
        cols = columns(c)
        wait_n(buf)
        for view in PAIR:
            at = pl.ds(view * view_rows, view_rows)
            first = sums_ref[i, view, :, cols]
            second = sums_ref[i, view, :, wide(c)]
            grad = invs[i, view, :, cols] * (gp[at, cols] - (first + nbuf[buf, at, :] * second) * inv_rows)
            if gain is not None:
                grad = gains[gain, :, cols] * grad
            own[jn, at, cols] = grad.astype(jnp.bfloat16)
        swap(jn, c).start()

    lam = lam_ref[0, 0]
    a_rows, b_rows = pl.ds(0, view_rows), pl.ds(view_rows, view_rows)
    last_cols = pl.ds(2 * width, COLS)
    load_z_rows = pltpu.make_async_copy(z_hbm, xs, lsem.at[0])
    load_x_two = pltpu.make_async_copy(x2_hbm, own.at[1], lsem.at[1])
    load_z_rows.start()
    load_x_two.start()
    for buf in PAIR:
        load_w(0, buf, buf)
        load_z(buf, buf)
    gp[a_rows, :] = jnp.zeros((view_rows, width), jnp.float32)
    for view in PAIR:
        psum[view, :, last_cols] = jnp.zeros((1, COLS), jnp.float32)
    greet([partner] + peers)
    load_z_rows.wait()

    def z_swap(c):
        cols = columns(c)
        return remote(xs.at[b_rows, cols], other.at[1, a_rows, cols], psend.at[1, c], precv.at[1, c], partner)

    z_turn = remote(xsend.at[:, a_rows], xt.at[1, :, b_rows], psend.at[1, chunks], precv.at[1, chunks], partner)
    z_swap(0).start()
    turn(xs, view_rows, z_turn, 1)

    @pl.loop(1, chunks)
    def _(c):
        z_swap(c).start()

    z_turn.wait_recv()

    def gather(step, t, phase, r):
        off, size = row_parts(BF16_SPLIT, phase)[r]
        picks = list(place.coord)
        for k in range(step):
            picks[(r + 2 - k) % 3] = slice(None)
        axis = (r + 2 - step) % 3
        ref = grads.at[(*picks, place.core, pl.ds(off, size), columns(t))]
        return remote(ref, ref, gsend.at[t, 3 * step + r], grecv.at[t, 3 * step + r], place.near[axis])

    def across(t):
        ref = grads.at[:, :, :, place.core, :, columns(t)]
        return remote(ref, ref, gsend.at[t, 9], grecv.at[t, 9], partner)

    def corr_block(t, phase):
        for r in AXES:
            off, size, val = ring.result(t, phase, r)
            corr = val * inv_rows
            row_id = place.me * BLOCK + off + lax.broadcasted_iota(jnp.int32, corr.shape, 0)
            col_id = t * COLS + lax.broadcasted_iota(jnp.int32, corr.shape, 1)
            diag = row_id == col_id
            gap = 1.0 - corr
            terms = jnp.where(diag, gap * gap, lam * corr * corr)
            psum[0, :, last_cols] += jnp.sum(terms, axis=0, keepdims=True)
            stage[pl.ds(off, size), :] = jnp.where(diag, -2.0 * gap, 2.0 * lam * corr) * inv_rows
        grads[(*place.coord, place.core, slice(None), columns(t))] = stage[...].astype(jnp.bfloat16)
        for r in AXES:
            gather(0, t, phase, r).start()

    def embed_chunk(c):
        cols = columns(c)
        buf = lax.rem(c, 2)
        block = grads[:, :, :, :, :, cols].reshape(width, COLS)
        grad = jnp.dot(xs[a_rows, :], block, preferred_element_type=jnp.float32)
        gp[b_rows, cols] = grad
        wait_n(buf)
        psum[1, :, cols] = jnp.sum(grad, axis=0, keepdims=True)
        psum[1, :, wide(c)] = jnp.sum(grad * nbuf[buf, b_rows, :], axis=0, keepdims=True)

        @pl.loop(0, chunks)
        def _(k):
            rows_g = grads[k // 4, lax.rem(k // 2, 2), lax.rem(k, 2), :, :, cols].reshape(COLS, COLS)
            gp[a_rows, columns(k)] += lax.dot_general(xs[b_rows, cols], rows_g, LAST_DIMS,
                                                      preferred_element_type=jnp.float32)

    @pl.loop(0, chunks + 7)
    def _(t):
        phase = lax.rem(t, 3)

        @pl.when(t < chunks)
        def _():
            for s in AXES:
                @pl.when((phase == s) & (t >= RING))
                def _():
                    ring.wait_sends(t - RING, s - RING)
            z_swap(t).wait_recv()
            cols = columns(t)
            for half in PAIR:
                feats = pl.ds(512 * half, 512)
                part = jnp.dot(xt[1, feats, a_rows], xs[b_rows, cols], preferred_element_type=jnp.float32)
                part += jnp.dot(xt[1, feats, b_rows], other[1, a_rows, cols], preferred_element_type=jnp.float32)
                acc[lax.rem(t, RING), half] = part.reshape(2, 2, BLOCK, COLS)

        for s in AXES:
            @pl.when(phase == s)
            def _():
                @pl.when(t < chunks)
                def _():
                    ring.send(0, t, s)

                for step in PAIR:
                    u = t - 1 - step

                    @pl.when((u >= 0) & (u < chunks))
                    def _():
                        ring.add(step, u, s - 1 - step)
                        ring.send(step + 1, u, s - 1 - step)

                @pl.when((t >= 3) & (t < chunks + 3))
                def _():
                    corr_block(t - 3, s - 3)

                for step in PAIR:
                    v = t - 4 - step

                    @pl.when((v >= 0) & (v < chunks))
                    def _():
                        for r in AXES:
                            gather(step, v, s - 4 - step, r).wait_recv()
                            gather(step + 1, v, s - 4 - step, r).start()

                @pl.when((t >= 6) & (t < chunks + 6))
                def _():
                    for r in AXES:
                        gather(2, t - 6, s - 6, r).wait_recv()
                    across(t - 6).start()

        @pl.when(t == 1)
        def _():
            load_x_two.wait()
            z_turn.wait_send()
            turn_x(own.at[1], 0)

        @pl.when(t >= 7)
        def _():
            c = t - 7
            across(c).wait_recv()
            embed_chunk(c)

            @pl.when(c < chunks - 2)
            def _():
                load_z(c + 2, lax.rem(c, 2))

    for buf in PAIR:
        load_z(buf, buf)

    def stream(body):
        @pl.loop(0, chunks // 2)
        def _(pair):
            for buf in PAIR:
                c = 2 * pair + buf
                body(c, buf)

                @pl.when(c < chunks - 2)
                def _():
                    load_z(c + 2, buf)

    def view_a_sums(c, buf):
        cols = columns(c)
        wait_n(buf)
        grad = gp[a_rows, cols]
        psum[0, :, cols] = jnp.sum(grad, axis=0, keepdims=True)
        psum[0, :, wide(c)] = jnp.sum(grad * nbuf[buf, a_rows, :], axis=0, keepdims=True)

    start, chips, finish, close = sums_of(0)
    stream(view_a_sums)
    start()
    for buf in PAIR:
        load_z(buf, buf)
    chips()
    for t in range(chunks - RING, chunks):
        ring.wait_sends(t, t)
    for t in range(chunks):
        across(t).wait_send()
        z_swap(t).wait_send()
        for step in AXES:
            for r in AXES:
                gather(step, t, t, r).wait_send()
    finish()
    close()
    loss_ref[...] = jnp.sum(sums_ref[0, 0, :, last_cols], axis=1, keepdims=True) + jnp.zeros((1, BLOCK), jnp.float32)
    stream(lambda c, buf: norm_chunk(0, None, 0, c, buf))
    for buf in PAIR:
        load_n(0, buf, buf)

    @pl.loop(0, jobs * chunks + 3)
    def _(t):
        j = t // chunks
        n = lax.rem(t, chunks)
        jb = lax.rem(j, 2)
        jn = 1 - jb
        phase = lax.rem(t, 3)

        @pl.when(t < jobs * chunks)
        def _():
            for s in AXES:
                @pl.when((phase == s) & (t >= RING))
                def _():
                    ring.wait_sends(t - RING, s - RING)

            @pl.when(n == 0)
            def _():
                x_swap(jb).wait_recv()
            swap(jb, n).wait_recv()
            cols = columns(n)
            slot = lax.rem(t, RING)
            for half in PAIR:
                feats = pl.ds(512 * half, 512)
                part = jnp.dot(xt[jb, feats, pl.ds(0, rows)], own[jb, :, cols], preferred_element_type=jnp.float32)
                part += jnp.dot(xt[jb, feats, pl.ds(rows, rows)], other[jb, :, cols],
                                preferred_element_type=jnp.float32)
                acc[slot, half] = part.reshape(2, 2, BLOCK, COLS)

        for s in AXES:
            @pl.when(phase == s)
            def _():
                @pl.when(t < jobs * chunks)
                def _():
                    ring.send(0, t, s)

                for step in PAIR:
                    u = t - 1 - step

                    @pl.when((u >= 0) & (u < jobs * chunks))
                    def _():
                        ring.add(step, u, s - 1 - step)
                        ring.send(step + 1, u, s - 1 - step)

                @pl.when(t >= 3)
                def _():
                    u = t - 3
                    for r in AXES:
                        off, size, val = ring.result(u, s - 3, r)
                        out_ref[u // chunks, pl.ds(off, size), columns(lax.rem(u, chunks))] = val

        @pl.when(j < jobs - 1)
        def _():
            start, chips, finish, close = sums_of(j + 1)

            @pl.when(n < 4)
            def _():
                for buf in PAIR:
                    c = 2 * n + buf
                    layer_chunk(j, jb, c, buf)

                    @pl.when(n < 3)
                    def _():
                        load_w(j, c + 2, buf)
                        load_n(j, c + 2, buf)

                    @pl.when(n == 3)
                    def _():
                        load_n(j, buf, buf)

            @pl.when(n == 3)
            def _():
                start()

                @pl.when(j == 0)
                def _():
                    load_x(x1_hbm).start()

                @pl.when(j == 1)
                def _():
                    for view, ref in enumerate((ha_hbm, hb_hbm)):
                        pltpu.make_async_copy(ref, xs.at[pl.ds(view * view_rows, view_rows), :], lsem.at[1]).start()

            @pl.when(n == 4)
            def _():
                chips()

            @pl.when(n == 5)
            def _():
                finish()
                load_x(x1_hbm).wait()
                x_swap(jb).wait_send()
                turn_x(xs, jn)

            @pl.when(n == 6)
            def _():
                close()
                vec_ref[j] = sums_ref[j + 1, 0, :, pl.ds(0, 2 * width)] + sums_ref[j + 1, 1, :, pl.ds(0, 2 * width)]

                @pl.loop(0, chunks)
                def _(c):
                    swap(jb, c).wait_send()

            @pl.when(n >= 6)
            def _():
                @pl.loop(0, 2)
                def _(pair):
                    for buf in PAIR:
                        c = (n - 6) * 4 + pair * 2 + buf
                        norm_chunk(j + 1, 1 - j, jn, c, buf)

                        @pl.when(c < chunks - 2)
                        def _():
                            load_n(j, c + 2, buf)

            @pl.when((n == 7) & (j == 0))
            def _():
                for buf in PAIR:
                    load_n(1, buf, buf)
                    load_w(1, buf, buf)

    for t in range(jobs * chunks - RING, jobs * chunks):
        ring.wait_sends(t, t)

    @pl.loop(0, chunks)
    def _(c):
        swap(0, c).wait_send()
    x_swap(0).wait_send()


VM = pl.BlockSpec(memory_space=pltpu.VMEM)


def back_all(lam, gains, shifts, invs, z, x2, x1, h_a, h_b, n3, n2, n1, w3, w2, total_rows):
    rows, width = z.shape
    chunks = width // COLS
    hbm = pl.BlockSpec(memory_space=pltpu.HBM)
    bf16, f32 = jnp.bfloat16, jnp.float32
    dma = pltpu.SemaphoreType.DMA
    wide = 2 * width + COLS
    return pl.pallas_call(
        functools.partial(back_kernel, 1.0 / total_rows),
        out_shape=(jax.ShapeDtypeStruct((3, BLOCK, width), f32), jax.ShapeDtypeStruct((2, 1, 2 * width), f32),
                   jax.ShapeDtypeStruct((1, BLOCK), f32)),
        in_specs=[pl.BlockSpec(memory_space=pltpu.SMEM)] + [VM] * 3 + [hbm] * 10, out_specs=(VM,) * 3,
        scratch_shapes=[
            pltpu.VMEM((2, width // 2, 2 * rows), bf16),
            pltpu.VMEM((width // 2, rows), bf16),
            pltpu.VMEM((rows, width), bf16),
            pltpu.VMEM((2, rows, width), bf16),
            pltpu.VMEM((2, rows, width), bf16),
            pltpu.VMEM((RING, 2, 2, 2, BLOCK, COLS), f32),
            pltpu.VMEM((RING, 2, 2, BLOCK, COLS), f32),
            pltpu.VMEM((RING, 2, BLOCK, COLS), f32),
            pltpu.VMEM((RING, BLOCK, COLS), f32),
            pltpu.VMEM((rows, width), f32),
            pltpu.VMEM((2, COLS, width), bf16),
            pltpu.VMEM((2, rows, COLS), f32),
            pltpu.VMEM((3, 1, wide), f32),
            pltpu.VMEM((8, 1, wide), f32),
            pltpu.VMEM((3, 2, 1, wide), f32),
            pltpu.VMEM((2, 2, 2, 2, BLOCK, width), bf16),
            pltpu.VMEM((BLOCK, COLS), f32),
            dma((RING, 9)), dma((RING, 9)), dma((2, chunks + 1)), dma((2, chunks + 1)),
            dma, dma, dma((7,)), dma((7,)), dma, dma, dma((2,)), dma((2,)), dma((2,)),
            dma((chunks, 10)), dma((chunks, 10)),
        ],
        compiler_params=pltpu.CompilerParams(collective_id=1, has_side_effects=True, vmem_limit_bytes=67043328),
        name="back_all",
    )(lam.reshape(1, 1), gains, shifts, invs, z, x2, x1, h_a, h_b, n3, n2, n1, w3, w2)


def solution(mesh):
    shards = mesh.shape["data"]

    def local_step(h_a, h_b, w_one, w_two, w_three, gain_one, shift_one, gain_two, shift_two, lam_off):
        rows_dev, width = h_a.shape
        total_rows = rows_dev * shards
        gains = jnp.stack([gain_one, gain_two])[:, None]
        shifts = jnp.stack([shift_one, shift_two])[:, None]
        normed_one, normed_two, normed_out, act_one, act_two, embed, invs = forward_all(
            gains, shifts, h_a, h_b, w_one, w_two, w_three, total_rows)
        weights, vectors, loss = back_all(
            lam_off, gains, shifts, invs, embed, act_two, act_one, h_a, h_b, normed_out, normed_two, normed_one,
            w_three, w_two, total_rows)
        return (loss[0, 0], weights[2], weights[1], weights[0],
                vectors[1, 0, width:], vectors[1, 0, :width], vectors[0, 0, width:], vectors[0, 0, :width])

    row_spec = P("data", None)
    whole_mat = P(None, None)
    whole_vec = P(None)
    return jax.shard_map(
        local_step, mesh=mesh,
        in_specs=(row_spec, row_spec, whole_mat, whole_mat, whole_mat,
                  whole_vec, whole_vec, whole_vec, whole_vec, P()),
        out_specs=(P(), row_spec, row_spec, row_spec, whole_vec, whole_vec, whole_vec, whole_vec),
        check_vma=False)
```

```python
import functools

import jax
import jax.numpy as jnp
from jax import lax
from jax.experimental import pallas as pl
from jax.experimental.pallas import tpu as pltpu
from jax.sharding import PartitionSpec as P

NORM_EPS = 1e-5
MESH = pl.DeviceIdType.MESH
RING = 4
COLS = 256
BLOCK = 128
PAIR = range(2)
AXES = range(3)
F32_SPLIT = ((48, 40, 40), (40, 48, 40), (40, 40, 48))
BF16_SPLIT = ((48, 48, 32), (32, 48, 48), (48, 32, 48))


LAST_DIMS = (((1,), (1,)), ((), ()))


def odd(n):
    return n % 2


class Place:
    def __init__(self):
        self.me = lax.axis_index("data")
        self.core = lax.rem(self.me, 2)
        self.chip = self.me // 2
        self.coord = (self.chip // 4, lax.rem(self.chip // 2, 2), lax.rem(self.chip, 2))
        self.partner = self.me + 1 - 2 * self.core
        self.near = tuple(self.me + (1 - 2 * c) * w for c, w in zip(self.coord, (8, 4, 2)))


def greet(peers):
    barrier = pltpu.get_barrier_semaphore()
    for peer in peers:
        pl.semaphore_signal(barrier, inc=1, device_id=(peer,), device_id_type=MESH)
    pl.semaphore_wait(barrier, len(peers))


def remote(src, dst, send, recv, peer):
    return pltpu.make_async_remote_copy(src_ref=src, dst_ref=dst, send_sem=send, recv_sem=recv,
                                        device_id=(peer,), device_id_type=MESH)


def row_parts(split, phase):
    sizes = split[phase % 3]
    return tuple((sum(sizes[:r]), sizes[r]) for r in AXES)


class HalvingReduce:
    def __init__(self, place, acc, bufs, ssem, rsem):
        self.place, self.acc, self.bufs, self.ssem, self.rsem = place, acc, bufs, ssem, rsem

    def at(self, t, picks):
        return (lax.rem(t, RING),) + tuple(picks)

    def copy(self, step, t, phase, r):
        slot = lax.rem(t, RING)
        off, size = row_parts(F32_SPLIT, phase)[r]
        rows = pl.ds(off, size)
        picks = [slice(None)] * 3
        for k in range(step):
            axis = (r + k) % 3
            picks[axis] = self.place.coord[axis]
        axis = (r + step) % 3
        picks[axis] = 1 - self.place.coord[axis]
        src = self.acc.at[(slot, *picks, rows, slice(None))]
        dst = self.bufs[step].at[(slot,) + (slice(None),) * (2 - step) + (rows, slice(None))]
        return remote(src, dst, self.ssem.at[slot, 3 * step + r], self.rsem.at[slot, 3 * step + r],
                      self.place.near[axis])

    def send(self, step, t, phase):
        for r in AXES:
            self.copy(step, t, phase, r).start()

    def wait_sends(self, t, phase):
        for step in AXES:
            for r in AXES:
                self.copy(step, t, phase, r).wait_send()

    def add(self, step, t, phase):
        slot = lax.rem(t, RING)
        for r in AXES:
            self.copy(step, t, phase, r).wait_recv()
            off, size = row_parts(F32_SPLIT, phase)[r]
            rows = pl.ds(off, size)
            fixed = {(r + k) % 3 for k in range(step + 1)}
            free = [a for a in range(3) if a not in fixed]
            for n in range(2 ** len(free)):
                picks = list(self.place.coord)
                sub = []
                for pos, a in enumerate(free):
                    bit = (n >> (len(free) - 1 - pos)) & 1
                    picks[a] = bit
                    sub.append(bit)
                where = (slot, *picks, rows, slice(None))
                self.acc[where] = self.acc[where] + self.bufs[step][(slot, *sub, rows, slice(None))]

    def result(self, t, phase, r):
        slot = lax.rem(t, RING)
        self.copy(2, t, phase, r).wait_recv()
        off, size = row_parts(F32_SPLIT, phase)[r]
        rows = pl.ds(off, size)
        return off, size, (self.acc[(slot, *self.place.coord, rows, slice(None))]
                           + self.bufs[2][(slot, rows, slice(None))])


def columns(t, width=COLS):
    return pl.ds(pl.multiple_of(t * width, width), width)


def exchange_parts(place, psum, parts, total, sems):
    asend, arecv, csend, crecv, fsend, frecv = sems
    peers = [lax.rem(place.chip + dist, 8) * 2 + place.core for dist in range(1, 8)]
    other = 1 - place.core
    land = psum.at[2]
    first = remote(psum.at[other], land, asend, arecv, place.partner)
    mine = parts.at[place.chip]
    across = [remote(mine, mine, csend.at[n], crecv.at[n], peer) for n, peer in enumerate(peers)]
    last = remote(total.at[place.core], total.at[place.core], fsend, frecv, place.partner)

    def start():
        first.start()

    def chips():
        first.wait_recv()
        parts[place.chip] = psum[place.core] + psum[2]
        for copy in across:
            copy.start()

    def finish():
        for copy in across:
            copy.wait_recv()
        value = parts[0]
        for c in range(1, 8):
            value = value + parts[c]
        total[place.core] = value
        last.start()

    def close():
        last.wait_recv()
        first.wait_send()
        for copy in across:
            copy.wait_send()
        last.wait_send()

    return peers, start, chips, finish, close


def whole_kernel(inv_rows, lam_ref, g1_ref, s1_ref, g2_ref, s2_ref, ha_hbm, hb_hbm, w1_hbm, w2_hbm, w3_hbm,
                 out_ref, vec_ref, loss_ref, n1_hbm, n2_hbm, n3_hbm,
                 xt, xsend, xs, own, other, acc, b0, b1, b2, gp, wbuf, nbuf, psum, parts, sums_ref, grads, stage,
                 gains, shifts, invs, fsum, fparts, ftotal,
                 ssem, rsem, psend, precv, asend, arecv, csend, crecv, fsend, frecv, lsem, wsem, nsem, gsend, grecv,
                 usem, vsem, easend, earecv, ecsend, ecrecv, efsend, efrecv):
    place = Place()
    view_rows, width = ha_hbm.shape
    rows = 2 * view_rows
    chunks = width // COLS
    jobs = 3
    peers = [lax.rem(place.chip + dist, 8) * 2 + place.core for dist in range(1, 8)]
    partner = place.partner
    ring = HalvingReduce(place, acc, (b0, b1, b2), ssem, rsem)

    def load_w(j, c, buf):
        rows_c = columns(lax.rem(c, chunks // 2))
        for k, ref in enumerate((w3_hbm, w2_hbm)):
            @pl.when(j == k)
            def _():
                pltpu.make_async_copy(ref.at[c // (chunks // 2), rows_c, :], wbuf.at[buf], wsem.at[buf]).start()

    def load_z(c, buf):
        pltpu.make_async_copy(n3_hbm.at[:, columns(c)], nbuf.at[buf], nsem.at[buf]).start()

    def load_n(j, c, buf):
        for k, ref in enumerate((n2_hbm, n1_hbm)):
            @pl.when(j == k)
            def _():
                pltpu.make_async_copy(ref.at[:, columns(c)], nbuf.at[buf], nsem.at[buf]).start()

    def wait_w(buf):
        pltpu.make_async_copy(w3_hbm.at[0, pl.ds(0, COLS), :], wbuf.at[buf], wsem.at[buf]).wait()

    def wait_n(buf):
        pltpu.make_async_copy(n2_hbm.at[:, pl.ds(0, COLS)], nbuf.at[buf], nsem.at[buf]).wait()

    def swap(jb, c):
        cols = columns(c)
        return remote(own.at[jb, :, cols], other.at[jb, :, cols], psend.at[jb, c], precv.at[jb, c], partner)

    def x_swap(jb):
        return remote(xsend, xt.at[jb, :, pl.ds(rows, rows)], psend.at[jb, chunks], precv.at[jb, chunks], partner)

    def load_h(dst):
        return [pltpu.make_async_copy(ref, dst.at[pl.ds(view * view_rows, view_rows), :], lsem.at[view])
                for view, ref in enumerate((ha_hbm, hb_hbm))]

    def turn(src, depth, copy, jb):
        def blocks(dst, parity):
            @pl.loop(0, 8)
            def _(b):
                to = pl.ds(pl.multiple_of(b * BLOCK, BLOCK), BLOCK)
                cols = pl.ds(pl.multiple_of((2 * b + parity) * BLOCK, BLOCK), BLOCK)
                dst[to, pl.ds(0, depth)] = src[pl.ds(0, depth), cols].T

        blocks(xsend, 1 - place.core)
        copy.start()
        blocks(xt.at[jb], place.core)

    def turn_x(src, jb):
        turn(src, rows, x_swap(jb), jb)

    def sums_of(i):
        return exchange_parts(place, psum, parts, sums_ref.at[i], (asend, arecv, csend, crecv, fsend, frecv))[1:]

    def wide(c):
        return pl.ds(pl.multiple_of(width + c * COLS, COLS), COLS)

    def layer_chunk(j, jb, c, buf):
        cols = columns(c)
        wait_w(buf)
        wait_n(buf)
        for view in PAIR:
            first = jnp.zeros((1, COLS), jnp.float32)
            second = jnp.zeros((1, COLS), jnp.float32)
            for part in PAIR:
                at = pl.ds(view * view_rows + part * (view_rows // 2), view_rows // 2)
                grad = lax.dot_general(own[jb, at, :], wbuf[buf], LAST_DIMS,
                                       preferred_element_type=jnp.float32)
                normed = nbuf[buf, at, :]
                grad = jnp.where(gains[1 - j, :, cols] * normed + shifts[1 - j, :, cols] > 0, grad, 0.0)
                gp[at, cols] = grad
                first += jnp.sum(grad, axis=0, keepdims=True)
                second += jnp.sum(grad * normed, axis=0, keepdims=True)
            psum[view, :, cols] = first
            psum[view, :, wide(c)] = second

    def norm_chunk(i, gain, jn, c, buf):
        cols = columns(c)
        wait_n(buf)
        for view in PAIR:
            at = pl.ds(view * view_rows, view_rows)
            first = sums_ref[i, view, :, cols]
            second = sums_ref[i, view, :, wide(c)]
            grad = invs[i, view, :, cols] * (gp[at, cols] - (first + nbuf[buf, at, :] * second) * inv_rows)
            if gain is not None:
                grad = gains[gain, :, cols] * grad
            own[jn, at, cols] = grad.astype(jnp.bfloat16)
        swap(jn, c).start()

    half = width // 2
    per = chunks // 2
    weights = (w1_hbm, w2_hbm, w3_hbm)
    w_slots = (xt, other, xt)
    normed_out = (n1_hbm, n2_hbm, n3_hbm)

    def view_at(view):
        return pl.ds(view * view_rows, view_rows)

    def fetch_w(l, c):
        cols = columns(c)
        return pltpu.make_async_copy(weights[l].at[:, :, cols], w_slots[l].at[:, :, cols], vsem.at[odd(l), c])

    def fetch_all(l):
        @pl.loop(0, chunks)
        def _(c):
            fetch_w(l, c).start()

    for load in load_h(own.at[0]):
        load.start()
    fetch_all(0)

    @pl.loop(0, width // BLOCK)
    def _(r):
        lanes = pl.ds(pl.multiple_of(r * BLOCK, BLOCK), BLOCK)
        for n, (g_ref, s_ref) in enumerate(((g1_ref, s1_ref), (g2_ref, s2_ref))):
            gains[n, :, lanes] = g_ref[pl.ds(r, 1), :]
            shifts[n, :, lanes] = s_ref[pl.ds(r, 1), :]

    swaps = [exchange_parts(place, fsum.at[v], fparts.at[v], ftotal.at[v],
                            tuple(sem.at[v] for sem in (easend, earecv, ecsend, ecrecv, efsend, efrecv)))[1:]
             for v in PAIR]
    greet([partner] + peers)
    for load in load_h(own.at[0]):
        load.wait()

    def local(c):
        return columns(lax.rem(c, per))

    def local_far(c):
        return pl.ds(pl.multiple_of(half + lax.rem(c, per) * COLS, COLS), COLS)

    def normed_copy(l, view, c):
        cols = columns(c)
        return pltpu.make_async_copy(gp.at[view_at(view), cols], normed_out[l].at[view_at(view), cols],
                                     usem.at[view, c])

    def products(l, view, actions):
        at = view_at(view)

        @pl.loop(0, chunks)
        def _(c):
            for when, action in actions:
                pl.when(c == when)(action)
            if view == 0:
                fetch_w(l, c).wait()
            if l:
                normed_copy(l - 1, view, c).wait()
            cols = columns(c)
            value = jnp.dot(own[odd(l), at, pl.ds(0, half)], w_slots[l][0, :, cols],
                            preferred_element_type=jnp.float32)
            value += jnp.dot(own[odd(l), at, pl.ds(half, half)], w_slots[l][1, :, cols],
                             preferred_element_type=jnp.float32)
            gp[at, cols] = value
            fsum[view, c // per, :, local(c)] = jnp.sum(value, axis=0, keepdims=True)
            fsum[view, c // per, :, local_far(c)] = jnp.sum(value * value, axis=0, keepdims=True)

    def normalise(l, view, after=None):
        at = view_at(view)

        @pl.loop(0, chunks)
        def _(c):
            cols = columns(c)
            mean = ftotal[view, c // per, :, local(c)] * inv_rows
            inv = lax.rsqrt(ftotal[view, c // per, :, local_far(c)] * inv_rows - mean * mean + NORM_EPS)
            invs[2 - l, view, :, cols] = inv
            normed = (gp[at, cols] - mean) * inv
            gp[at, cols] = normed
            normed_copy(l, view, c).start()
            act = normed
            if l < 2:
                act = jnp.maximum(gains[l, :, cols] * normed + shifts[l, :, cols], 0.0)
            act = act.astype(jnp.bfloat16)
            own[odd(l + 1), at, cols] = act
            if l == 0:
                xs[at, cols] = act
            if after is not None:
                after(c)

    a_swap, b_swap = swaps
    for l in AXES:
        products(l, 0, ((0, b_swap[1]), (chunks - 2, b_swap[2])) if l else ())
        a_swap[0]()
        if l:
            b_swap[3]()
            normalise(l - 1, 1)
        else:
            fetch_all(1)
        products(l, 1, ((0, a_swap[1]), (chunks - 2, a_swap[2])))
        b_swap[0]()
        if l == 0:
            fetch_all(2)
        a_swap[3]()
        normalise(l, 0)

    lam = lam_ref[0, 0]
    a_rows, b_rows = view_at(0), view_at(1)
    last_cols = pl.ds(2 * width, COLS)
    for view in PAIR:
        psum[view, :, last_cols] = jnp.zeros((1, COLS), jnp.float32)
    for buf in PAIR:
        load_w(0, buf, buf)

    def z_swap(c):
        cols = columns(c)
        return remote(own.at[1, b_rows, cols], other.at[1, a_rows, cols], psend.at[1, c], precv.at[1, c], partner)

    z_turn = remote(xsend.at[:, a_rows], xt.at[1, :, b_rows], psend.at[1, chunks], precv.at[1, chunks], partner)
    b_swap[1]()
    turn(own.at[1], view_rows, z_turn, 1)
    b_swap[2]()
    b_swap[3]()
    normalise(2, 1, lambda c: z_swap(c).start())
    for view in PAIR:
        @pl.loop(0, chunks)
        def _(c):
            normed_copy(2, view, c).wait()
    for buf in PAIR:
        load_z(buf, buf)
    z_turn.wait_recv()

    def gather(step, t, phase, r):
        off, size = row_parts(BF16_SPLIT, phase)[r]
        picks = list(place.coord)
        for k in range(step):
            picks[(r + 2 - k) % 3] = slice(None)
        axis = (r + 2 - step) % 3
        ref = grads.at[(*picks, place.core, pl.ds(off, size), columns(t))]
        return remote(ref, ref, gsend.at[t, 3 * step + r], grecv.at[t, 3 * step + r], place.near[axis])

    def across(t):
        ref = grads.at[:, :, :, place.core, :, columns(t)]
        return remote(ref, ref, gsend.at[t, 9], grecv.at[t, 9], partner)

    def corr_block(t, phase):
        for r in AXES:
            off, size, val = ring.result(t, phase, r)
            corr = val * inv_rows
            row_id = place.me * BLOCK + off + lax.broadcasted_iota(jnp.int32, corr.shape, 0)
            col_id = t * COLS + lax.broadcasted_iota(jnp.int32, corr.shape, 1)
            diag = row_id == col_id
            gap = 1.0 - corr
            terms = jnp.where(diag, gap * gap, lam * corr * corr)
            psum[0, :, last_cols] += jnp.sum(terms, axis=0, keepdims=True)
            stage[pl.ds(off, size), :] = jnp.where(diag, -2.0 * gap, 2.0 * lam * corr) * inv_rows
        grads[(*place.coord, place.core, slice(None), columns(t))] = stage[...].astype(jnp.bfloat16)
        for r in AXES:
            gather(0, t, phase, r).start()

    def embed_chunk(c):
        cols = columns(c)
        buf = lax.rem(c, 2)
        block = grads[:, :, :, :, :, cols].reshape(width, COLS)
        grad = jnp.dot(own[1, a_rows, :], block, preferred_element_type=jnp.float32)
        gp[b_rows, cols] = grad
        wait_n(buf)
        psum[1, :, cols] = jnp.sum(grad, axis=0, keepdims=True)
        psum[1, :, wide(c)] = jnp.sum(grad * nbuf[buf, b_rows, :], axis=0, keepdims=True)

        @pl.loop(0, chunks)
        def _(k):
            rows_g = grads[k // 4, lax.rem(k // 2, 2), lax.rem(k, 2), :, :, cols].reshape(COLS, COLS)
            more = lax.dot_general(own[1, b_rows, cols], rows_g, LAST_DIMS, preferred_element_type=jnp.float32)
            gp[a_rows, columns(k)] = jnp.where(c > 0, gp[a_rows, columns(k)], 0.0) + more

    @pl.loop(0, chunks + 7)
    def _(t):
        phase = lax.rem(t, 3)

        @pl.when(t < chunks)
        def _():
            for s in AXES:
                @pl.when((phase == s) & (t >= RING))
                def _():
                    ring.wait_sends(t - RING, s - RING)
            z_swap(t).wait_recv()
            cols = columns(t)
            for half in PAIR:
                feats = pl.ds(512 * half, 512)
                part = jnp.dot(xt[1, feats, a_rows], own[1, b_rows, cols], preferred_element_type=jnp.float32)
                part += jnp.dot(xt[1, feats, b_rows], other[1, a_rows, cols], preferred_element_type=jnp.float32)
                acc[lax.rem(t, RING), half] = part.reshape(2, 2, BLOCK, COLS)

        for s in AXES:
            @pl.when(phase == s)
            def _():
                @pl.when(t < chunks)
                def _():
                    ring.send(0, t, s)

                for step in PAIR:
                    u = t - 1 - step

                    @pl.when((u >= 0) & (u < chunks))
                    def _():
                        ring.add(step, u, s - 1 - step)
                        ring.send(step + 1, u, s - 1 - step)

                @pl.when((t >= 3) & (t < chunks + 3))
                def _():
                    corr_block(t - 3, s - 3)

                for step in PAIR:
                    v = t - 4 - step

                    @pl.when((v >= 0) & (v < chunks))
                    def _():
                        for r in AXES:
                            gather(step, v, s - 4 - step, r).wait_recv()
                            gather(step + 1, v, s - 4 - step, r).start()

                @pl.when((t >= 6) & (t < chunks + 6))
                def _():
                    for r in AXES:
                        gather(2, t - 6, s - 6, r).wait_recv()
                    across(t - 6).start()

        @pl.when(t == 1)
        def _():
            z_turn.wait_send()
            turn_x(own.at[0], 0)

        @pl.when(t >= 7)
        def _():
            c = t - 7
            across(c).wait_recv()
            embed_chunk(c)

            @pl.when(c < chunks - 2)
            def _():
                load_z(c + 2, lax.rem(c, 2))

    for buf in PAIR:
        load_z(buf, buf)

    def stream(body):
        @pl.loop(0, chunks // 2)
        def _(pair):
            for buf in PAIR:
                c = 2 * pair + buf
                body(c, buf)

                @pl.when(c < chunks - 2)
                def _():
                    load_z(c + 2, buf)

    def view_a_sums(c, buf):
        cols = columns(c)
        wait_n(buf)
        grad = gp[a_rows, cols]
        psum[0, :, cols] = jnp.sum(grad, axis=0, keepdims=True)
        psum[0, :, wide(c)] = jnp.sum(grad * nbuf[buf, a_rows, :], axis=0, keepdims=True)

    start, chips, finish, close = sums_of(0)
    stream(view_a_sums)
    start()
    for buf in PAIR:
        load_z(buf, buf)
    chips()
    for t in range(chunks - RING, chunks):
        ring.wait_sends(t, t)
    for t in range(chunks):
        across(t).wait_send()
        z_swap(t).wait_send()
        for step in AXES:
            for r in AXES:
                gather(step, t, t, r).wait_send()
    finish()
    close()
    loss_ref[...] = jnp.sum(sums_ref[0, 0, :, last_cols], axis=1, keepdims=True) + jnp.zeros((1, BLOCK), jnp.float32)

    def norm_pairs(lo, hi):
        @pl.loop(lo, hi)
        def _(pair):
            for buf in PAIR:
                c = 2 * pair + buf
                norm_chunk(0, None, 0, c, buf)

                @pl.when(c < chunks - 2)
                def _():
                    load_z(c + 2, buf)

    norm_pairs(0, 1)

    @pl.loop(0, jobs * chunks + 3)
    def _(t):
        j = t // chunks
        n = lax.rem(t, chunks)
        jb = lax.rem(j, 2)
        jn = 1 - jb
        phase = lax.rem(t, 3)

        @pl.when(t < jobs * chunks)
        def _():
            for s in AXES:
                @pl.when((phase == s) & (t >= RING))
                def _():
                    ring.wait_sends(t - RING, s - RING)

            @pl.when(n == 0)
            def _():
                x_swap(jb).wait_recv()
            swap(jb, n).wait_recv()
            cols = columns(n)
            slot = lax.rem(t, RING)
            for half in PAIR:
                feats = pl.ds(512 * half, 512)
                part = jnp.dot(xt[jb, feats, pl.ds(0, rows)], own[jb, :, cols], preferred_element_type=jnp.float32)
                part += jnp.dot(xt[jb, feats, pl.ds(rows, rows)], other[jb, :, cols],
                                preferred_element_type=jnp.float32)
                acc[slot, half] = part.reshape(2, 2, BLOCK, COLS)

        for s in AXES:
            @pl.when(phase == s)
            def _():
                @pl.when(t < jobs * chunks)
                def _():
                    ring.send(0, t, s)

                for step in PAIR:
                    u = t - 1 - step

                    @pl.when((u >= 0) & (u < jobs * chunks))
                    def _():
                        ring.add(step, u, s - 1 - step)
                        ring.send(step + 1, u, s - 1 - step)

                @pl.when(t >= 3)
                def _():
                    u = t - 3
                    for r in AXES:
                        off, size, val = ring.result(u, s - 3, r)
                        out_ref[u // chunks, pl.ds(off, size), columns(lax.rem(u, chunks))] = val

        @pl.when(t == 0)
        def _():
            norm_pairs(1, chunks // 2)
            for buf in PAIR:
                load_n(0, buf, buf)

        @pl.when(j < jobs - 1)
        def _():
            start, chips, finish, close = sums_of(j + 1)

            @pl.when(n < 4)
            def _():
                for buf in PAIR:
                    c = 2 * n + buf
                    layer_chunk(j, jb, c, buf)

                    @pl.when(n < 3)
                    def _():
                        load_w(j, c + 2, buf)
                        load_n(j, c + 2, buf)

                    @pl.when(n == 3)
                    def _():
                        load_n(j, buf, buf)

            @pl.when(n == 3)
            def _():
                start()

                @pl.when(j == 1)
                def _():
                    for load in load_h(xs):
                        load.start()

            @pl.when(n == 4)
            def _():
                chips()

            @pl.when(n == 5)
            def _():
                finish()

                @pl.when(j == 1)
                def _():
                    for load in load_h(xs):
                        load.wait()
                x_swap(jb).wait_send()
                turn_x(xs, jn)

            @pl.when(n == 6)
            def _():
                close()
                vec_ref[j] = sums_ref[j + 1, 0, :, pl.ds(0, 2 * width)] + sums_ref[j + 1, 1, :, pl.ds(0, 2 * width)]

                @pl.loop(0, chunks)
                def _(c):
                    swap(jb, c).wait_send()

            @pl.when(n >= 6)
            def _():
                @pl.loop(0, 2)
                def _(pair):
                    for buf in PAIR:
                        c = (n - 6) * 4 + pair * 2 + buf
                        norm_chunk(j + 1, 1 - j, jn, c, buf)

                        @pl.when(c < chunks - 2)
                        def _():
                            load_n(j, c + 2, buf)

            @pl.when((n == 7) & (j == 0))
            def _():
                for buf in PAIR:
                    load_n(1, buf, buf)
                    load_w(1, buf, buf)

    for t in range(jobs * chunks - RING, jobs * chunks):
        ring.wait_sends(t, t)

    @pl.loop(0, chunks)
    def _(c):
        swap(0, c).wait_send()
    x_swap(0).wait_send()


VM = pl.BlockSpec(memory_space=pltpu.VMEM)


def whole_step(lam, vectors, h_a, h_b, weights, total_rows):
    view_rows, width = h_a.shape
    rows = 2 * view_rows
    chunks = width // COLS
    hbm = pl.BlockSpec(memory_space=pltpu.HBM)
    bf16, f32 = jnp.bfloat16, jnp.float32
    dma = pltpu.SemaphoreType.DMA
    wide = 2 * width + COLS
    return pl.pallas_call(
        functools.partial(whole_kernel, 1.0 / total_rows),
        out_shape=(jax.ShapeDtypeStruct((3, BLOCK, width), f32), jax.ShapeDtypeStruct((2, 1, 2 * width), f32),
                   jax.ShapeDtypeStruct((1, BLOCK), f32)) + (jax.ShapeDtypeStruct((rows, width), f32),) * 3,
        in_specs=[pl.BlockSpec(memory_space=pltpu.SMEM)] + [VM] * 4 + [hbm] * 5, out_specs=(VM,) * 3 + (hbm,) * 3,
        scratch_shapes=[
            pltpu.VMEM((2, width // 2, 2 * rows), bf16),
            pltpu.VMEM((width // 2, rows), bf16),
            pltpu.VMEM((rows, width), bf16),
            pltpu.VMEM((2, rows, width), bf16),
            pltpu.VMEM((2, rows, width), bf16),
            pltpu.VMEM((RING, 2, 2, 2, BLOCK, COLS), f32),
            pltpu.VMEM((RING, 2, 2, BLOCK, COLS), f32),
            pltpu.VMEM((RING, 2, BLOCK, COLS), f32),
            pltpu.VMEM((RING, BLOCK, COLS), f32),
            pltpu.VMEM((rows, width), f32),
            pltpu.VMEM((2, COLS, width), bf16),
            pltpu.VMEM((2, rows, COLS), f32),
            pltpu.VMEM((3, 1, wide), f32),
            pltpu.VMEM((8, 1, wide), f32),
            pltpu.VMEM((3, 2, 1, wide), f32),
            pltpu.VMEM((2, 2, 2, 2, BLOCK, width), bf16),
            pltpu.VMEM((BLOCK, COLS), f32),
            pltpu.VMEM((2, 1, width), f32),
            pltpu.VMEM((2, 1, width), f32),
            pltpu.VMEM((3, 2, 1, width), f32),
            pltpu.VMEM((2, 3, 1, width), f32),
            pltpu.VMEM((2, 8, 1, width), f32),
            pltpu.VMEM((2, 2, 1, width), f32),
            dma((RING, 9)), dma((RING, 9)), dma((2, chunks + 1)), dma((2, chunks + 1)),
            dma, dma, dma((7,)), dma((7,)), dma, dma, dma((2,)), dma((2,)), dma((2,)),
            dma((chunks, 10)), dma((chunks, 10)),
            dma((2, chunks)), dma((2, chunks)),
            dma((2,)), dma((2,)), dma((2, 7)), dma((2, 7)), dma((2,)), dma((2,)),
        ],
        compiler_params=pltpu.CompilerParams(collective_id=1, has_side_effects=True, vmem_limit_bytes=67043328),
        name="whole_step",
    )(lam.reshape(1, 1), *(v.reshape(width // BLOCK, BLOCK) for v in vectors), h_a, h_b,
      *(w.reshape(2, width // 2, width) for w in weights))


def solution(mesh):
    shards = mesh.shape["data"]

    def local_step(h_a, h_b, w_one, w_two, w_three, gain_one, shift_one, gain_two, shift_two, lam_off):
        rows_dev, width = h_a.shape
        total_rows = rows_dev * shards
        weights, vectors, loss = whole_step(lam_off, (gain_one, shift_one, gain_two, shift_two), h_a, h_b,
                                            (w_one, w_two, w_three), total_rows)[:3]
        return (loss[0, 0], weights[2], weights[1], weights[0],
                vectors[1, 0, width:], vectors[1, 0, :width], vectors[0, 0, width:], vectors[0, 0, :width])

    row_spec = P("data", None)
    whole_mat = P(None, None)
    whole_vec = P(None)
    return jax.shard_map(
        local_step, mesh=mesh,
        in_specs=(row_spec, row_spec, whole_mat, whole_mat, whole_mat,
                  whole_vec, whole_vec, whole_vec, whole_vec, P()),
        out_specs=(P(), row_spec, row_spec, row_spec, whole_vec, whole_vec, whole_vec, whole_vec),
        check_vma=False)
```

```python
import functools

import jax
import jax.numpy as jnp
from jax import lax
from jax.experimental import pallas as pl
from jax.experimental.pallas import tpu as pltpu
from jax.sharding import PartitionSpec as P

NORM_EPS = 1e-5
MESH = pl.DeviceIdType.MESH
RING = 4
COLS = 256
STRIP = 512
BLOCK = 128
PAIR = range(2)
AXES = range(3)
F32_SPLIT = ((48, 40, 40), (40, 48, 40), (40, 40, 48))
BF16_SPLIT = ((48, 48, 32), (32, 48, 48), (48, 32, 48))


LAST_DIMS = (((1,), (1,)), ((), ()))


def odd(n):
    return n % 2


class Place:
    def __init__(self):
        self.me = lax.axis_index("data")
        self.core = lax.rem(self.me, 2)
        self.chip = self.me // 2
        self.coord = (self.chip // 4, lax.rem(self.chip // 2, 2), lax.rem(self.chip, 2))
        self.partner = self.me + 1 - 2 * self.core
        self.near = tuple(self.me + (1 - 2 * c) * w for c, w in zip(self.coord, (8, 4, 2)))


def greet(peers):
    barrier = pltpu.get_barrier_semaphore()
    for peer in peers:
        pl.semaphore_signal(barrier, inc=1, device_id=(peer,), device_id_type=MESH)
    pl.semaphore_wait(barrier, len(peers))


def remote(src, dst, send, recv, peer):
    return pltpu.make_async_remote_copy(src_ref=src, dst_ref=dst, send_sem=send, recv_sem=recv,
                                        device_id=(peer,), device_id_type=MESH)


def row_parts(split, phase):
    sizes = split[phase % 3]
    return tuple((sum(sizes[:r]), sizes[r]) for r in AXES)


class HalvingReduce:
    def __init__(self, place, acc, bufs, ssem, rsem):
        self.place, self.acc, self.bufs, self.ssem, self.rsem = place, acc, bufs, ssem, rsem

    def at(self, t, picks):
        return (lax.rem(t, RING),) + tuple(picks)

    def copy(self, step, t, phase, r):
        slot = lax.rem(t, RING)
        off, size = row_parts(F32_SPLIT, phase)[r]
        rows = pl.ds(off, size)
        picks = [slice(None)] * 3
        for k in range(step):
            axis = (r + k) % 3
            picks[axis] = self.place.coord[axis]
        axis = (r + step) % 3
        picks[axis] = 1 - self.place.coord[axis]
        src = self.acc.at[(slot, *picks, rows, slice(None))]
        dst = self.bufs[step].at[(slot,) + (slice(None),) * (2 - step) + (rows, slice(None))]
        return remote(src, dst, self.ssem.at[slot, 3 * step + r], self.rsem.at[slot, 3 * step + r],
                      self.place.near[axis])

    def send(self, step, t, phase):
        for r in AXES:
            self.copy(step, t, phase, r).start()

    def wait_sends(self, t, phase):
        for step in AXES:
            for r in AXES:
                self.copy(step, t, phase, r).wait_send()

    def add(self, step, t, phase):
        slot = lax.rem(t, RING)
        for r in AXES:
            self.copy(step, t, phase, r).wait_recv()
            off, size = row_parts(F32_SPLIT, phase)[r]
            rows = pl.ds(off, size)
            fixed = {(r + k) % 3 for k in range(step + 1)}
            free = [a for a in range(3) if a not in fixed]
            for n in range(2 ** len(free)):
                picks = list(self.place.coord)
                sub = []
                for pos, a in enumerate(free):
                    bit = (n >> (len(free) - 1 - pos)) & 1
                    picks[a] = bit
                    sub.append(bit)
                where = (slot, *picks, rows, slice(None))
                self.acc[where] = self.acc[where] + self.bufs[step][(slot, *sub, rows, slice(None))]

    def result(self, t, phase, r):
        slot = lax.rem(t, RING)
        self.copy(2, t, phase, r).wait_recv()
        off, size = row_parts(F32_SPLIT, phase)[r]
        rows = pl.ds(off, size)
        return off, size, (self.acc[(slot, *self.place.coord, rows, slice(None))]
                           + self.bufs[2][(slot, rows, slice(None))])


def columns(t, width=COLS):
    return pl.ds(pl.multiple_of(t * width, width), width)


def exchange_parts(place, psum, parts, total, sems):
    asend, arecv, csend, crecv, fsend, frecv = sems
    peers = [lax.rem(place.chip + dist, 8) * 2 + place.core for dist in range(1, 8)]
    other = 1 - place.core
    land = psum.at[2]
    first = remote(psum.at[other], land, asend, arecv, place.partner)
    mine = parts.at[place.chip]
    across = [remote(mine, mine, csend.at[n], crecv.at[n], peer) for n, peer in enumerate(peers)]
    last = remote(total.at[place.core], total.at[place.core], fsend, frecv, place.partner)

    def start():
        first.start()

    def chips():
        first.wait_recv()
        parts[place.chip] = psum[place.core] + psum[2]
        for copy in across:
            copy.start()

    def finish():
        for copy in across:
            copy.wait_recv()
        value = parts[0]
        for c in range(1, 8):
            value = value + parts[c]
        total[place.core] = value
        last.start()

    def close():
        last.wait_recv()
        first.wait_send()
        for copy in across:
            copy.wait_send()
        last.wait_send()

    return peers, start, chips, finish, close


def whole_kernel(inv_rows, lam_ref, g1_ref, s1_ref, g2_ref, s2_ref, ha_hbm, hb_hbm, w1_hbm, w2_hbm, w3_hbm,
                 out_ref, vec_ref, loss_ref, n1_hbm, n2_hbm, n3_hbm,
                 xt, xsend, xs, own, other, acc, b0, b1, b2, gp, wbuf, nbuf, psum, parts, sums_ref, grads, stage,
                 gains, shifts, means, invs, fsum, fparts, ftotal,
                 ssem, rsem, psend, precv, asend, arecv, csend, crecv, fsend, frecv, lsem, wsem, nsem, gsend, grecv,
                 usem, vsem, easend, earecv, ecsend, ecrecv, efsend, efrecv):
    place = Place()
    view_rows, width = ha_hbm.shape
    rows = 2 * view_rows
    chunks = width // COLS
    jobs = 3
    peers = [lax.rem(place.chip + dist, 8) * 2 + place.core for dist in range(1, 8)]
    partner = place.partner
    ring = HalvingReduce(place, acc, (b0, b1, b2), ssem, rsem)

    def load_w(j, c, buf):
        rows_c = columns(lax.rem(c, chunks // 2))
        for k, ref in enumerate((w3_hbm, w2_hbm)):
            @pl.when(j == k)
            def _():
                pltpu.make_async_copy(ref.at[c // (chunks // 2), rows_c, :], wbuf.at[buf], wsem.at[buf]).start()

    def load_z(c, buf):
        pltpu.make_async_copy(n3_hbm.at[:, columns(c)], nbuf.at[buf], nsem.at[buf]).start()

    def load_n(j, c, buf):
        for k, ref in enumerate((n2_hbm, n1_hbm)):
            @pl.when(j == k)
            def _():
                pltpu.make_async_copy(ref.at[:, columns(c)], nbuf.at[buf], nsem.at[buf]).start()

    def wait_w(buf):
        pltpu.make_async_copy(w3_hbm.at[0, pl.ds(0, COLS), :], wbuf.at[buf], wsem.at[buf]).wait()

    def wait_n(buf):
        pltpu.make_async_copy(n2_hbm.at[:, pl.ds(0, COLS)], nbuf.at[buf], nsem.at[buf]).wait()

    def swap(jb, c):
        cols = columns(c)
        return remote(own.at[jb, :, cols], other.at[jb, :, cols], psend.at[jb, c], precv.at[jb, c], partner)

    def x_swap(jb):
        return remote(xsend, xt.at[jb, :, pl.ds(rows, rows)], psend.at[jb, chunks], precv.at[jb, chunks], partner)

    def load_h(dst):
        return [pltpu.make_async_copy(ref, dst.at[pl.ds(view * view_rows, view_rows), :], lsem.at[view])
                for view, ref in enumerate((ha_hbm, hb_hbm))]

    def turn(src, depth, copy, jb):
        def blocks(dst, parity):
            @pl.loop(0, 8)
            def _(b):
                to = pl.ds(pl.multiple_of(b * BLOCK, BLOCK), BLOCK)
                cols = pl.ds(pl.multiple_of((2 * b + parity) * BLOCK, BLOCK), BLOCK)
                dst[to, pl.ds(0, depth)] = src[pl.ds(0, depth), cols].T

        blocks(xsend, 1 - place.core)
        copy.start()
        blocks(xt.at[jb], place.core)

    def turn_x(src, jb):
        turn(src, rows, x_swap(jb), jb)

    def sums_of(i):
        return exchange_parts(place, psum, parts, sums_ref.at[i], (asend, arecv, csend, crecv, fsend, frecv))[1:]

    def wide(c):
        return pl.ds(pl.multiple_of(width + c * COLS, COLS), COLS)

    def normed_of(i, view, buf, cols):
        at = pl.ds(view * view_rows, view_rows)
        return (nbuf[buf, at, :] - means[i, view, :, cols]) * invs[i, view, :, cols]

    def layer_chunk(j, jb, c, buf):
        cols = columns(c)
        wait_w(buf)
        wait_n(buf)
        for view in PAIR:
            at = pl.ds(view * view_rows, view_rows)
            grad = lax.dot_general(own[jb, at, :], wbuf[buf], LAST_DIMS, preferred_element_type=jnp.float32)
            normed = normed_of(j + 1, view, buf, cols)
            grad = jnp.where(gains[1 - j, :, cols] * normed + shifts[1 - j, :, cols] > 0, grad, 0.0)
            gp[at, cols] = grad
            psum[view, :, cols] = jnp.sum(grad, axis=0, keepdims=True)
            psum[view, :, wide(c)] = jnp.sum(grad * normed, axis=0, keepdims=True)

    def norm_chunk(i, gain, jn, c, buf):
        cols = columns(c)
        wait_n(buf)
        for view in PAIR:
            at = pl.ds(view * view_rows, view_rows)
            first = sums_ref[i, view, :, cols]
            second = sums_ref[i, view, :, wide(c)]
            grad = invs[i, view, :, cols] * (gp[at, cols] - (first + normed_of(i, view, buf, cols) * second) * inv_rows)
            if gain is not None:
                grad = gains[gain, :, cols] * grad
            own[jn, at, cols] = grad.astype(jnp.bfloat16)
        swap(jn, c).start()

    half = width // 2
    strips = width // STRIP
    per = strips // 2
    weights = (w1_hbm, w2_hbm, w3_hbm)
    w_slots = (xt, other, xt)
    hidden_out = (n1_hbm, n2_hbm, n3_hbm)

    def view_at(view):
        return pl.ds(view * view_rows, view_rows)

    def fetch_w(l, c):
        cols = columns(c, STRIP)
        return pltpu.make_async_copy(weights[l].at[:, :, cols], w_slots[l].at[:, :, cols], vsem.at[odd(l), c])

    def fetch_all(l, lo=0):
        @pl.loop(lo, strips)
        def _(c):
            fetch_w(l, c).start()

    load_a, load_b = load_h(own.at[0])
    load_a.start()
    fetch_w(0, 0).start()
    fetch_w(0, 1).start()

    @pl.loop(0, width // BLOCK)
    def _(r):
        lanes = pl.ds(pl.multiple_of(r * BLOCK, BLOCK), BLOCK)
        for n, (g_ref, s_ref) in enumerate(((g1_ref, s1_ref), (g2_ref, s2_ref))):
            gains[n, :, lanes] = g_ref[pl.ds(r, 1), :]
            shifts[n, :, lanes] = s_ref[pl.ds(r, 1), :]

    swaps = [exchange_parts(place, fsum.at[v], fparts.at[v], ftotal.at[v],
                            tuple(sem.at[v] for sem in (easend, earecv, ecsend, ecrecv, efsend, efrecv)))[1:]
             for v in PAIR]
    load_b.start()
    fetch_all(0, 2)
    greet([partner] + peers)
    load_a.wait()

    def local(c):
        return columns(lax.rem(c, per), STRIP)

    def local_far(c):
        return pl.ds(pl.multiple_of(half + lax.rem(c, per) * STRIP, STRIP), STRIP)

    def hidden_copy(l, view, c):
        cols = columns(c, STRIP)
        return pltpu.make_async_copy(gp.at[view_at(view), cols], hidden_out[l].at[view_at(view), cols],
                                     usem.at[view, c])

    def products(l, view, actions):
        at = view_at(view)

        @pl.loop(0, strips)
        def _(c):
            for when, action in actions:
                pl.when(c == when)(action)
            if view == 0:
                fetch_w(l, c).wait()
            if l:
                hidden_copy(l - 1, view, c).wait()
            cols = columns(c, STRIP)
            value = jnp.dot(own[odd(l), at, pl.ds(0, half)], w_slots[l][0, :, cols],
                            preferred_element_type=jnp.float32)
            value += jnp.dot(own[odd(l), at, pl.ds(half, half)], w_slots[l][1, :, cols],
                             preferred_element_type=jnp.float32)
            gp[at, cols] = value
            fsum[view, c // per, :, local(c)] = jnp.sum(value, axis=0, keepdims=True)
            fsum[view, c // per, :, local_far(c)] = jnp.sum(value * value, axis=0, keepdims=True)
            hidden_copy(l, view, c).start()

    def normalise(l, view, after=None):
        at = view_at(view)

        @pl.loop(0, chunks)
        def _(c):
            cols = columns(c)
            group, near = c // (chunks // 2), lax.rem(c, chunks // 2)
            mean = ftotal[view, group, :, columns(near)] * inv_rows
            square = ftotal[view, group, :, pl.ds(pl.multiple_of(half + near * COLS, COLS), COLS)] * inv_rows
            inv = lax.rsqrt(square - mean * mean + NORM_EPS)
            means[2 - l, view, :, cols] = mean
            invs[2 - l, view, :, cols] = inv
            act = (gp[at, cols] - mean) * inv
            if l < 2:
                act = jnp.maximum(gains[l, :, cols] * act + shifts[l, :, cols], 0.0)
            act = act.astype(jnp.bfloat16)
            own[odd(l + 1), at, cols] = act
            if l == 0:
                xs[at, cols] = act
            if after is not None:
                after(c)

    a_swap, b_swap = swaps
    for l in AXES:
        products(l, 0, ((0, b_swap[1]), (strips - 1, b_swap[2])) if l else ())
        a_swap[0]()
        if l:
            b_swap[3]()
            normalise(l - 1, 1)
        else:
            fetch_all(1)
            load_b.wait()
        products(l, 1, ((0, a_swap[1]),))
        b_swap[0]()
        a_swap[2]()
        if l == 0:
            fetch_all(2)
        a_swap[3]()
        normalise(l, 0)

    lam = lam_ref[0, 0]
    a_rows, b_rows = view_at(0), view_at(1)
    last_cols = pl.ds(2 * width, COLS)
    for view in PAIR:
        psum[view, :, last_cols] = jnp.zeros((1, COLS), jnp.float32)
    for buf in PAIR:
        load_w(0, buf, buf)

    def z_swap(c):
        cols = columns(c)
        return remote(own.at[1, b_rows, cols], other.at[1, a_rows, cols], psend.at[1, c], precv.at[1, c], partner)

    z_turn = remote(xsend.at[:, a_rows], xt.at[1, :, b_rows], psend.at[1, chunks], precv.at[1, chunks], partner)
    b_swap[1]()
    turn(own.at[1], view_rows, z_turn, 1)
    b_swap[2]()
    b_swap[3]()
    normalise(2, 1, lambda c: z_swap(c).start())
    for view in PAIR:
        @pl.loop(0, strips)
        def _(c):
            hidden_copy(2, view, c).wait()
    for buf in PAIR:
        load_z(buf, buf)
    z_turn.wait_recv()

    def gather(step, t, phase, r):
        off, size = row_parts(BF16_SPLIT, phase)[r]
        picks = list(place.coord)
        for k in range(step):
            picks[(r + 2 - k) % 3] = slice(None)
        axis = (r + 2 - step) % 3
        ref = grads.at[(*picks, place.core, pl.ds(off, size), columns(t))]
        return remote(ref, ref, gsend.at[t, 3 * step + r], grecv.at[t, 3 * step + r], place.near[axis])

    def across(t):
        ref = grads.at[:, :, :, place.core, :, columns(t)]
        return remote(ref, ref, gsend.at[t, 9], grecv.at[t, 9], partner)

    def corr_block(t, phase):
        for r in AXES:
            off, size, val = ring.result(t, phase, r)
            corr = val * inv_rows
            row_id = place.me * BLOCK + off + lax.broadcasted_iota(jnp.int32, corr.shape, 0)
            col_id = t * COLS + lax.broadcasted_iota(jnp.int32, corr.shape, 1)
            diag = row_id == col_id
            gap = 1.0 - corr
            terms = jnp.where(diag, gap * gap, lam * corr * corr)
            psum[0, :, last_cols] += jnp.sum(terms, axis=0, keepdims=True)
            stage[pl.ds(off, size), :] = jnp.where(diag, -2.0 * gap, 2.0 * lam * corr) * inv_rows
        grads[(*place.coord, place.core, slice(None), columns(t))] = stage[...].astype(jnp.bfloat16)
        for r in AXES:
            gather(0, t, phase, r).start()

    def embed_chunk(c):
        cols = columns(c)
        buf = lax.rem(c, 2)
        block = grads[:, :, :, :, :, cols].reshape(width, COLS)
        grad = jnp.dot(own[1, a_rows, :], block, preferred_element_type=jnp.float32)
        gp[b_rows, cols] = grad
        wait_n(buf)
        psum[1, :, cols] = jnp.sum(grad, axis=0, keepdims=True)
        psum[1, :, wide(c)] = jnp.sum(grad * normed_of(0, 1, buf, cols), axis=0, keepdims=True)
        load_z(lax.rem(c + 2, chunks), buf)

        @pl.loop(0, chunks)
        def _(k):
            rows_g = grads[k // 4, lax.rem(k // 2, 2), lax.rem(k, 2), :, :, cols].reshape(COLS, COLS)
            more = lax.dot_general(own[1, b_rows, cols], rows_g, LAST_DIMS, preferred_element_type=jnp.float32)
            at_k = columns(k)
            total = jnp.where(c > 0, gp[a_rows, at_k], 0.0) + more
            gp[a_rows, at_k] = total

            @pl.when(c == chunks - 1)
            def _():
                buf_k = lax.rem(k, 2)
                wait_n(buf_k)
                psum[0, :, at_k] = jnp.sum(total, axis=0, keepdims=True)
                psum[0, :, wide(k)] = jnp.sum(total * normed_of(0, 0, buf_k, at_k), axis=0, keepdims=True)
                load_z(lax.rem(k + 2, chunks), buf_k)

    @pl.loop(0, chunks + 7)
    def _(t):
        phase = lax.rem(t, 3)

        @pl.when(t < chunks)
        def _():
            for s in AXES:
                @pl.when((phase == s) & (t >= RING))
                def _():
                    ring.wait_sends(t - RING, s - RING)
            z_swap(t).wait_recv()
            cols = columns(t)
            for half in PAIR:
                feats = pl.ds(512 * half, 512)
                part = jnp.dot(xt[1, feats, a_rows], own[1, b_rows, cols], preferred_element_type=jnp.float32)
                part += jnp.dot(xt[1, feats, b_rows], other[1, a_rows, cols], preferred_element_type=jnp.float32)
                acc[lax.rem(t, RING), half] = part.reshape(2, 2, BLOCK, COLS)

        for s in AXES:
            @pl.when(phase == s)
            def _():
                @pl.when(t < chunks)
                def _():
                    ring.send(0, t, s)

                for step in PAIR:
                    u = t - 1 - step

                    @pl.when((u >= 0) & (u < chunks))
                    def _():
                        ring.add(step, u, s - 1 - step)
                        ring.send(step + 1, u, s - 1 - step)

                @pl.when((t >= 3) & (t < chunks + 3))
                def _():
                    corr_block(t - 3, s - 3)

                for step in PAIR:
                    v = t - 4 - step

                    @pl.when((v >= 0) & (v < chunks))
                    def _():
                        for r in AXES:
                            gather(step, v, s - 4 - step, r).wait_recv()
                            gather(step + 1, v, s - 4 - step, r).start()

                @pl.when((t >= 6) & (t < chunks + 6))
                def _():
                    for r in AXES:
                        gather(2, t - 6, s - 6, r).wait_recv()
                    across(t - 6).start()

        @pl.when(t == 1)
        def _():
            z_turn.wait_send()
            turn_x(own.at[0], 0)

        @pl.when(t >= 7)
        def _():
            c = t - 7
            across(c).wait_recv()
            embed_chunk(c)

    start, chips, finish, close = sums_of(0)
    start()
    chips()
    for t in range(chunks - RING, chunks):
        ring.wait_sends(t, t)
    for t in range(chunks):
        across(t).wait_send()
        z_swap(t).wait_send()
        for step in AXES:
            for r in AXES:
                gather(step, t, t, r).wait_send()
    finish()
    close()
    loss_ref[...] = jnp.sum(sums_ref[0, 0, :, last_cols], axis=1, keepdims=True) + jnp.zeros((1, BLOCK), jnp.float32)

    def norm_pairs(lo, hi):
        @pl.loop(lo, hi)
        def _(pair):
            for buf in PAIR:
                c = 2 * pair + buf
                norm_chunk(0, None, 0, c, buf)

                @pl.when(c < chunks - 2)
                def _():
                    load_z(c + 2, buf)

    norm_pairs(0, 1)

    @pl.loop(0, jobs * chunks + 3)
    def _(t):
        j = t // chunks
        n = lax.rem(t, chunks)
        jb = lax.rem(j, 2)
        jn = 1 - jb
        phase = lax.rem(t, 3)

        @pl.when(t < jobs * chunks)
        def _():
            for s in AXES:
                @pl.when((phase == s) & (t >= RING))
                def _():
                    ring.wait_sends(t - RING, s - RING)

            @pl.when(n == 0)
            def _():
                x_swap(jb).wait_recv()
            swap(jb, n).wait_recv()
            cols = columns(n)
            slot = lax.rem(t, RING)
            for half in PAIR:
                feats = pl.ds(512 * half, 512)
                part = jnp.dot(xt[jb, feats, pl.ds(0, rows)], own[jb, :, cols], preferred_element_type=jnp.float32)
                part += jnp.dot(xt[jb, feats, pl.ds(rows, rows)], other[jb, :, cols],
                                preferred_element_type=jnp.float32)
                acc[slot, half] = part.reshape(2, 2, BLOCK, COLS)

        for s in AXES:
            @pl.when(phase == s)
            def _():
                @pl.when(t < jobs * chunks)
                def _():
                    ring.send(0, t, s)

                for step in PAIR:
                    u = t - 1 - step

                    @pl.when((u >= 0) & (u < jobs * chunks))
                    def _():
                        ring.add(step, u, s - 1 - step)
                        ring.send(step + 1, u, s - 1 - step)

                @pl.when(t >= 3)
                def _():
                    u = t - 3
                    for r in AXES:
                        off, size, val = ring.result(u, s - 3, r)
                        out_ref[u // chunks, pl.ds(off, size), columns(lax.rem(u, chunks))] = val

        @pl.when(t == 0)
        def _():
            norm_pairs(1, chunks // 2)
            for buf in PAIR:
                load_n(0, buf, buf)

        @pl.when(j < jobs - 1)
        def _():
            start, chips, finish, close = sums_of(j + 1)

            @pl.when(n < 4)
            def _():
                for buf in PAIR:
                    c = 2 * n + buf
                    layer_chunk(j, jb, c, buf)

                    @pl.when(n < 3)
                    def _():
                        load_w(j, c + 2, buf)
                        load_n(j, c + 2, buf)

                    @pl.when(n == 3)
                    def _():
                        load_n(j, buf, buf)

            @pl.when(n == 3)
            def _():
                start()

                @pl.when(j == 1)
                def _():
                    for load in load_h(xs):
                        load.start()

            @pl.when(n == 4)
            def _():
                chips()

            @pl.when(n == 5)
            def _():
                finish()

                @pl.when(j == 1)
                def _():
                    for load in load_h(xs):
                        load.wait()
                x_swap(jb).wait_send()
                turn_x(xs, jn)

            @pl.when(n == 6)
            def _():
                close()
                vec_ref[j] = sums_ref[j + 1, 0, :, pl.ds(0, 2 * width)] + sums_ref[j + 1, 1, :, pl.ds(0, 2 * width)]

                @pl.loop(0, chunks)
                def _(c):
                    swap(jb, c).wait_send()

            @pl.when(n >= 6)
            def _():
                @pl.loop(0, 2)
                def _(pair):
                    for buf in PAIR:
                        c = (n - 6) * 4 + pair * 2 + buf
                        norm_chunk(j + 1, 1 - j, jn, c, buf)

                        @pl.when(c < chunks - 2)
                        def _():
                            load_n(j, c + 2, buf)

            @pl.when((n == 7) & (j == 0))
            def _():
                for buf in PAIR:
                    load_n(1, buf, buf)
                    load_w(1, buf, buf)

    for t in range(jobs * chunks - RING, jobs * chunks):
        ring.wait_sends(t, t)

    @pl.loop(0, chunks)
    def _(c):
        swap(0, c).wait_send()
    x_swap(0).wait_send()


VM = pl.BlockSpec(memory_space=pltpu.VMEM)


def whole_step(lam, vectors, h_a, h_b, weights, total_rows):
    view_rows, width = h_a.shape
    rows = 2 * view_rows
    chunks = width // COLS
    hbm = pl.BlockSpec(memory_space=pltpu.HBM)
    bf16, f32 = jnp.bfloat16, jnp.float32
    dma = pltpu.SemaphoreType.DMA
    wide = 2 * width + COLS
    return pl.pallas_call(
        functools.partial(whole_kernel, 1.0 / total_rows),
        out_shape=(jax.ShapeDtypeStruct((3, BLOCK, width), f32), jax.ShapeDtypeStruct((2, 1, 2 * width), f32),
                   jax.ShapeDtypeStruct((1, BLOCK), f32)) + (jax.ShapeDtypeStruct((rows, width), f32),) * 3,
        in_specs=[pl.BlockSpec(memory_space=pltpu.SMEM)] + [VM] * 4 + [hbm] * 5, out_specs=(VM,) * 3 + (hbm,) * 3,
        scratch_shapes=[
            pltpu.VMEM((2, width // 2, 2 * rows), bf16),
            pltpu.VMEM((width // 2, rows), bf16),
            pltpu.VMEM((rows, width), bf16),
            pltpu.VMEM((2, rows, width), bf16),
            pltpu.VMEM((2, rows, width), bf16),
            pltpu.VMEM((RING, 2, 2, 2, BLOCK, COLS), f32),
            pltpu.VMEM((RING, 2, 2, BLOCK, COLS), f32),
            pltpu.VMEM((RING, 2, BLOCK, COLS), f32),
            pltpu.VMEM((RING, BLOCK, COLS), f32),
            pltpu.VMEM((rows, width), f32),
            pltpu.VMEM((2, COLS, width), bf16),
            pltpu.VMEM((2, rows, COLS), f32),
            pltpu.VMEM((3, 1, wide), f32),
            pltpu.VMEM((8, 1, wide), f32),
            pltpu.VMEM((3, 2, 1, wide), f32),
            pltpu.VMEM((2, 2, 2, 2, BLOCK, width), bf16),
            pltpu.VMEM((BLOCK, COLS), f32),
            pltpu.VMEM((2, 1, width), f32),
            pltpu.VMEM((2, 1, width), f32),
            pltpu.VMEM((3, 2, 1, width), f32),
            pltpu.VMEM((3, 2, 1, width), f32),
            pltpu.VMEM((2, 3, 1, width), f32),
            pltpu.VMEM((2, 8, 1, width), f32),
            pltpu.VMEM((2, 2, 1, width), f32),
            dma((RING, 9)), dma((RING, 9)), dma((2, chunks + 1)), dma((2, chunks + 1)),
            dma, dma, dma((7,)), dma((7,)), dma, dma, dma((2,)), dma((2,)), dma((2,)),
            dma((chunks, 10)), dma((chunks, 10)),
            dma((2, width // STRIP)), dma((2, width // STRIP)),
            dma((2,)), dma((2,)), dma((2, 7)), dma((2, 7)), dma((2,)), dma((2,)),
        ],
        compiler_params=pltpu.CompilerParams(collective_id=1, has_side_effects=True, vmem_limit_bytes=67043328),
        name="whole_step",
    )(lam.reshape(1, 1), *(v.reshape(width // BLOCK, BLOCK) for v in vectors), h_a, h_b,
      *(w.reshape(2, width // 2, width) for w in weights))


def solution(mesh):
    shards = mesh.shape["data"]

    def local_step(h_a, h_b, w_one, w_two, w_three, gain_one, shift_one, gain_two, shift_two, lam_off):
        rows_dev, width = h_a.shape
        total_rows = rows_dev * shards
        weights, vectors, loss = whole_step(lam_off, (gain_one, shift_one, gain_two, shift_two), h_a, h_b,
                                            (w_one, w_two, w_three), total_rows)[:3]
        return (loss[0, 0], weights[2], weights[1], weights[0],
                vectors[1, 0, width:], vectors[1, 0, :width], vectors[0, 0, width:], vectors[0, 0, :width])

    row_spec = P("data", None)
    whole_mat = P(None, None)
    whole_vec = P(None)
    return jax.shard_map(
        local_step, mesh=mesh,
        in_specs=(row_spec, row_spec, whole_mat, whole_mat, whole_mat,
                  whole_vec, whole_vec, whole_vec, whole_vec, P()),
        out_specs=(P(), row_spec, row_spec, row_spec, whole_vec, whole_vec, whole_vec, whole_vec),
        check_vma=False)
```

```python
import functools

import jax
import jax.numpy as jnp
from jax import lax
from jax.experimental import pallas as pl
from jax.experimental.pallas import tpu as pltpu
from jax.sharding import PartitionSpec as P

NORM_EPS = 1e-5
MESH = pl.DeviceIdType.MESH
RING = 4
COLS = 256
STRIP = 512
BLOCK = 128
PAIR = range(2)
AXES = range(3)
F32_SPLIT = ((48, 40, 40), (40, 48, 40), (40, 40, 48))
BF16_SPLIT = ((48, 48, 32), (32, 48, 48), (48, 32, 48))


LAST_DIMS = (((1,), (1,)), ((), ()))


def odd(n):
    return n % 2


class Place:
    def __init__(self):
        self.me = lax.axis_index("data")
        self.core = lax.rem(self.me, 2)
        self.chip = self.me // 2
        self.coord = (self.chip // 4, lax.rem(self.chip // 2, 2), lax.rem(self.chip, 2))
        self.partner = self.me + 1 - 2 * self.core
        steps = [(1 - 2 * c) * w for c, w in zip(self.coord, (8, 4, 2))]
        self.near = tuple(self.me + step for step in steps)
        self.chips = [self.me + sum(steps[a] for a in flips)
                      for flips in ((0, 1, 2), (0, 1), (0, 2), (1, 2), (0,), (1,), (2,))]


def greet(peers):
    barrier = pltpu.get_barrier_semaphore()
    for peer in peers:
        pl.semaphore_signal(barrier, inc=1, device_id=(peer,), device_id_type=MESH)
    pl.semaphore_wait(barrier, len(peers))


def remote(src, dst, send, recv, peer):
    return pltpu.make_async_remote_copy(src_ref=src, dst_ref=dst, send_sem=send, recv_sem=recv,
                                        device_id=(peer,), device_id_type=MESH)


def row_parts(split, phase):
    sizes = split[phase % 3]
    return tuple((sum(sizes[:r]), sizes[r]) for r in AXES)


class HalvingReduce:
    def __init__(self, place, acc, bufs, ssem, rsem):
        self.place, self.acc, self.bufs, self.ssem, self.rsem = place, acc, bufs, ssem, rsem

    def at(self, t, picks):
        return (lax.rem(t, RING),) + tuple(picks)

    def copy(self, step, t, phase, r):
        slot = lax.rem(t, RING)
        off, size = row_parts(F32_SPLIT, phase)[r]
        rows = pl.ds(off, size)
        picks = [slice(None)] * 3
        for k in range(step):
            axis = (r + k) % 3
            picks[axis] = self.place.coord[axis]
        axis = (r + step) % 3
        picks[axis] = 1 - self.place.coord[axis]
        src = self.acc.at[(slot, *picks, rows, slice(None))]
        dst = self.bufs[step].at[(slot,) + (slice(None),) * (2 - step) + (rows, slice(None))]
        return remote(src, dst, self.ssem.at[slot, 3 * step + r], self.rsem.at[slot, 3 * step + r],
                      self.place.near[axis])

    def send(self, step, t, phase):
        for r in AXES:
            self.copy(step, t, phase, r).start()

    def wait_sends(self, t, phase):
        for step in AXES:
            for r in AXES:
                self.copy(step, t, phase, r).wait_send()

    def add(self, step, t, phase):
        slot = lax.rem(t, RING)
        for r in AXES:
            self.copy(step, t, phase, r).wait_recv()
            off, size = row_parts(F32_SPLIT, phase)[r]
            rows = pl.ds(off, size)
            fixed = {(r + k) % 3 for k in range(step + 1)}
            free = [a for a in range(3) if a not in fixed]
            for n in range(2 ** len(free)):
                picks = list(self.place.coord)
                sub = []
                for pos, a in enumerate(free):
                    bit = (n >> (len(free) - 1 - pos)) & 1
                    picks[a] = bit
                    sub.append(bit)
                where = (slot, *picks, rows, slice(None))
                self.acc[where] = self.acc[where] + self.bufs[step][(slot, *sub, rows, slice(None))]

    def result(self, t, phase, r):
        slot = lax.rem(t, RING)
        self.copy(2, t, phase, r).wait_recv()
        off, size = row_parts(F32_SPLIT, phase)[r]
        rows = pl.ds(off, size)
        return off, size, (self.acc[(slot, *self.place.coord, rows, slice(None))]
                           + self.bufs[2][(slot, rows, slice(None))])


def columns(t, width=COLS):
    return pl.ds(pl.multiple_of(t * width, width), width)


def exchange_parts(place, psum, parts, total, sems):
    asend, arecv, csend, crecv, fsend, frecv = sems
    other = 1 - place.core
    land = psum.at[2]
    first = remote(psum.at[other], land, asend, arecv, place.partner)
    mine = parts.at[place.chip]
    across = [remote(mine, mine, csend.at[n], crecv.at[n], peer) for n, peer in enumerate(place.chips)]
    last = remote(total.at[place.core], total.at[place.core], fsend, frecv, place.partner)

    def start():
        first.start()

    def chips():
        first.wait_recv()
        parts[place.chip] = psum[place.core] + psum[2]
        for copy in across:
            copy.start()

    def finish():
        for copy in across:
            copy.wait_recv()
        value = parts[0]
        for c in range(1, 8):
            value = value + parts[c]
        total[place.core] = value
        last.start()

    def close():
        last.wait_recv()
        first.wait_send()
        for copy in across:
            copy.wait_send()
        last.wait_send()

    return start, chips, finish, close


def exchange_pair(place, own, land, parts, total, sems):
    asend, arecv, csend, crecv = sems
    first = remote(own, land, asend, arecv, place.partner)
    mine = parts.at[place.chip]
    across = [remote(mine, mine, csend.at[n], crecv.at[n], peer) for n, peer in enumerate(place.chips)]

    def chips():
        first.wait_recv()
        parts[place.chip] = own[...] + land[...]
        for copy in across:
            copy.start()

    def finish():
        first.wait_send()
        for copy in across:
            copy.wait()
        value = parts[0]
        for c in range(1, 8):
            value = value + parts[c]
        total[...] = value

    return first.start, chips, finish


def whole_kernel(inv_rows, lam_ref, g1_ref, s1_ref, g2_ref, s2_ref, ha_hbm, hb_hbm, w1_hbm, w2_hbm, w3_hbm,
                 out_ref, vec_ref, loss_ref, n1_hbm, n2_hbm, n3_hbm,
                 xt, xsend, xs, own, other, acc, b0, b1, b2, gp, wbuf, nbuf, psum, parts, sums_ref, grads, stage,
                 gains, shifts, means, invs, fsum, fparts, ftotal,
                 ssem, rsem, psend, precv, asend, arecv, csend, crecv, fsend, frecv, lsem, wsem, nsem, gsend, grecv,
                 usem, vsem, easend, earecv, ecsend, ecrecv):
    place = Place()
    view_rows, width = ha_hbm.shape
    rows = 2 * view_rows
    chunks = width // COLS
    jobs = 3
    partner = place.partner
    ring = HalvingReduce(place, acc, (b0, b1, b2), ssem, rsem)

    def load_w(j, c, buf):
        rows_c = columns(lax.rem(c, chunks // 2))
        for k, ref in enumerate((w3_hbm, w2_hbm)):
            @pl.when(j == k)
            def _():
                pltpu.make_async_copy(ref.at[c // (chunks // 2), rows_c, :], wbuf.at[buf], wsem.at[buf]).start()

    def load_z(c, buf):
        pltpu.make_async_copy(n3_hbm.at[:, columns(c)], nbuf.at[buf], nsem.at[buf]).start()

    def load_n(j, c, buf):
        for k, ref in enumerate((n2_hbm, n1_hbm)):
            @pl.when(j == k)
            def _():
                pltpu.make_async_copy(ref.at[:, columns(c)], nbuf.at[buf], nsem.at[buf]).start()

    def wait_w(buf):
        pltpu.make_async_copy(w3_hbm.at[0, pl.ds(0, COLS), :], wbuf.at[buf], wsem.at[buf]).wait()

    def wait_n(buf):
        pltpu.make_async_copy(n2_hbm.at[:, pl.ds(0, COLS)], nbuf.at[buf], nsem.at[buf]).wait()

    def swap(jb, c):
        cols = columns(c)
        return remote(own.at[jb, :, cols], other.at[jb, :, cols], psend.at[jb, c], precv.at[jb, c], partner)

    def x_swap(jb):
        return remote(xsend, xt.at[jb, :, pl.ds(rows, rows)], psend.at[jb, chunks], precv.at[jb, chunks], partner)

    def load_h(dst):
        return [pltpu.make_async_copy(ref, dst.at[pl.ds(view * view_rows, view_rows), :], lsem.at[view])
                for view, ref in enumerate((ha_hbm, hb_hbm))]

    def turn(src, depth, copy, jb):
        def blocks(dst, parity):
            @pl.loop(0, 8)
            def _(b):
                to = pl.ds(pl.multiple_of(b * BLOCK, BLOCK), BLOCK)
                cols = pl.ds(pl.multiple_of((2 * b + parity) * BLOCK, BLOCK), BLOCK)
                dst[to, pl.ds(0, depth)] = src[pl.ds(0, depth), cols].T

        blocks(xsend, 1 - place.core)
        copy.start()
        blocks(xt.at[jb], place.core)

    def turn_x(src, jb):
        turn(src, rows, x_swap(jb), jb)

    def sums_of(i):
        return exchange_parts(place, psum, parts, sums_ref.at[i], (asend, arecv, csend, crecv, fsend, frecv))

    def wide(c):
        return pl.ds(pl.multiple_of(width + c * COLS, COLS), COLS)

    def normed_of(i, view, buf, cols):
        at = pl.ds(view * view_rows, view_rows)
        return (nbuf[buf, at, :] - means[i, view, :, cols]) * invs[i, view, :, cols]

    def layer_pair(j, jb, n):
        for buf in PAIR:
            wait_w(buf)
            wait_n(buf)
        for view in PAIR:
            at = pl.ds(view * view_rows, view_rows)
            both = lax.dot_general(own[jb, at, :], wbuf[...].reshape(2 * COLS, width), LAST_DIMS,
                                   preferred_element_type=jnp.float32)
            for buf in PAIR:
                c = 2 * n + buf
                cols = columns(c)
                normed = normed_of(j + 1, view, buf, cols)
                grad = jnp.where(gains[1 - j, :, cols] * normed + shifts[1 - j, :, cols] > 0,
                                 both[:, buf * COLS:(buf + 1) * COLS], 0.0)
                gp[at, cols] = grad
                psum[view, :, cols] = jnp.sum(grad, axis=0, keepdims=True)
                psum[view, :, wide(c)] = jnp.sum(grad * normed, axis=0, keepdims=True)

    def norm_chunk(i, gain, jn, c, buf):
        cols = columns(c)
        wait_n(buf)
        for view in PAIR:
            at = pl.ds(view * view_rows, view_rows)
            first = sums_ref[i, view, :, cols]
            second = sums_ref[i, view, :, wide(c)]
            grad = invs[i, view, :, cols] * (gp[at, cols] - (first + normed_of(i, view, buf, cols) * second) * inv_rows)
            if gain is not None:
                grad = gains[gain, :, cols] * grad
            own[jn, at, cols] = grad.astype(jnp.bfloat16)
        swap(jn, c).start()

    half = width // 2
    strips = width // STRIP
    weights = (w1_hbm, w2_hbm, w3_hbm)
    w_slots = (xt, other, xt)
    hidden_out = (n1_hbm, n2_hbm, n3_hbm)

    def view_at(view):
        return pl.ds(view * view_rows, view_rows)

    def fetch_w(l, c):
        cols = columns(c, STRIP)
        return pltpu.make_async_copy(weights[l].at[:, :, cols], w_slots[l].at[:, :, cols], vsem.at[odd(l), c])

    def fetch_all(l, lo=0):
        @pl.loop(lo, strips)
        def _(c):
            fetch_w(l, c).start()

    load_a, load_b = load_h(own.at[0])
    load_a.start()
    fetch_w(0, 0).start()
    fetch_w(0, 1).start()

    @pl.loop(0, width // BLOCK)
    def _(r):
        lanes = pl.ds(pl.multiple_of(r * BLOCK, BLOCK), BLOCK)
        for n, (g_ref, s_ref) in enumerate(((g1_ref, s1_ref), (g2_ref, s2_ref))):
            gains[n, :, lanes] = g_ref[pl.ds(r, 1), :]
            shifts[n, :, lanes] = s_ref[pl.ds(r, 1), :]

    swaps = [exchange_pair(place, fsum.at[v, 0], fsum.at[v, 1], fparts.at[v], ftotal.at[v],
                           tuple(sem.at[v] for sem in (easend, earecv, ecsend, ecrecv)))
             for v in PAIR]
    load_b.start()
    fetch_all(0, 2)
    greet([partner] + place.chips)
    load_a.wait()

    def far(c, size):
        return pl.ds(pl.multiple_of(width + c * size, size), size)

    def hidden_copy(l, view, c):
        cols = columns(c, STRIP)
        return pltpu.make_async_copy(gp.at[view_at(view), cols], hidden_out[l].at[view_at(view), cols],
                                     usem.at[view, c])

    def products(l, view, actions):
        at = view_at(view)

        @pl.loop(0, strips)
        def _(c):
            for when, action in actions:
                pl.when(c == when)(action)
            if view == 0:
                fetch_w(l, c).wait()
            if l:
                hidden_copy(l - 1, view, c).wait()
            cols = columns(c, STRIP)
            value = jnp.dot(own[odd(l), at, pl.ds(0, half)], w_slots[l][0, :, cols],
                            preferred_element_type=jnp.float32)
            value += jnp.dot(own[odd(l), at, pl.ds(half, half)], w_slots[l][1, :, cols],
                             preferred_element_type=jnp.float32)
            gp[at, cols] = value
            fsum[view, 0, :, cols] = jnp.sum(value, axis=0, keepdims=True)
            fsum[view, 0, :, far(c, STRIP)] = jnp.sum(value * value, axis=0, keepdims=True)
            hidden_copy(l, view, c).start()

    def normalise(l, view, after=None):
        at = view_at(view)

        @pl.loop(0, chunks)
        def _(c):
            cols = columns(c)
            mean = ftotal[view, :, cols] * inv_rows
            square = ftotal[view, :, far(c, COLS)] * inv_rows
            inv = lax.rsqrt(square - mean * mean + NORM_EPS)
            means[2 - l, view, :, cols] = mean
            invs[2 - l, view, :, cols] = inv
            act = (gp[at, cols] - mean) * inv
            if l < 2:
                act = jnp.maximum(gains[l, :, cols] * act + shifts[l, :, cols], 0.0)
            act = act.astype(jnp.bfloat16)
            own[odd(l + 1), at, cols] = act
            if l == 0:
                xs[at, cols] = act
            if after is not None:
                after(c)

    a_swap, b_swap = swaps
    for l in AXES:
        products(l, 0, ((0, b_swap[1]),) if l else ())
        a_swap[0]()
        if l:
            b_swap[2]()
            normalise(l - 1, 1)
        else:
            fetch_all(1)
            load_b.wait()
        products(l, 1, ((0, a_swap[1]),))
        b_swap[0]()
        if l == 0:
            fetch_all(2)
        a_swap[2]()
        normalise(l, 0)

    lam = lam_ref[0, 0]
    a_rows, b_rows = view_at(0), view_at(1)
    last_cols = pl.ds(2 * width, COLS)
    for view in PAIR:
        psum[view, :, last_cols] = jnp.zeros((1, COLS), jnp.float32)
    for buf in PAIR:
        load_w(0, buf, buf)

    def z_swap(c):
        cols = columns(c)
        return remote(own.at[1, b_rows, cols], other.at[1, a_rows, cols], psend.at[1, c], precv.at[1, c], partner)

    z_turn = remote(xsend.at[:, a_rows], xt.at[1, :, b_rows], psend.at[1, chunks], precv.at[1, chunks], partner)
    b_swap[1]()
    turn(own.at[1], view_rows, z_turn, 1)
    b_swap[2]()
    normalise(2, 1, lambda c: z_swap(c).start())
    for view in PAIR:
        @pl.loop(0, strips)
        def _(c):
            hidden_copy(2, view, c).wait()
    for buf in PAIR:
        load_z(buf, buf)
    z_turn.wait_recv()

    def gather(step, t, phase, r):
        off, size = row_parts(BF16_SPLIT, phase)[r]
        picks = list(place.coord)
        for k in range(step):
            picks[(r + 2 - k) % 3] = slice(None)
        axis = (r + 2 - step) % 3
        ref = grads.at[(*picks, place.core, pl.ds(off, size), columns(t))]
        return remote(ref, ref, gsend.at[t, 3 * step + r], grecv.at[t, 3 * step + r], place.near[axis])

    def across(t):
        ref = grads.at[:, :, :, place.core, :, columns(t)]
        return remote(ref, ref, gsend.at[t, 9], grecv.at[t, 9], partner)

    def corr_block(t, phase):
        for r in AXES:
            off, size, val = ring.result(t, phase, r)
            corr = val * inv_rows
            row_id = place.me * BLOCK + off + lax.broadcasted_iota(jnp.int32, corr.shape, 0)
            col_id = t * COLS + lax.broadcasted_iota(jnp.int32, corr.shape, 1)
            diag = row_id == col_id
            gap = 1.0 - corr
            terms = jnp.where(diag, gap * gap, lam * corr * corr)
            psum[0, :, last_cols] += jnp.sum(terms, axis=0, keepdims=True)
            stage[pl.ds(off, size), :] = jnp.where(diag, -2.0 * gap, 2.0 * lam * corr) * inv_rows
        grads[(*place.coord, place.core, slice(None), columns(t))] = stage[...].astype(jnp.bfloat16)
        for r in AXES:
            gather(0, t, phase, r).start()

    def embed_chunk(c):
        cols = columns(c)
        buf = lax.rem(c, 2)
        block = grads[:, :, :, :, :, cols].reshape(width, COLS)
        grad = jnp.dot(own[1, a_rows, :], block, preferred_element_type=jnp.float32)
        gp[b_rows, cols] = grad
        wait_n(buf)
        psum[1, :, cols] = jnp.sum(grad, axis=0, keepdims=True)
        psum[1, :, wide(c)] = jnp.sum(grad * normed_of(0, 1, buf, cols), axis=0, keepdims=True)
        load_z(lax.rem(c + 2, chunks), buf)

        @pl.loop(0, chunks // 2)
        def _(k):
            rows_g = grads[k // 2, lax.rem(k, 2), :, :, :, cols].reshape(STRIP, COLS)
            more = lax.dot_general(own[1, b_rows, cols], rows_g, LAST_DIMS, preferred_element_type=jnp.float32)
            at_k = columns(k, STRIP)
            gp[a_rows, at_k] = jnp.where(c > 0, gp[a_rows, at_k], 0.0) + more

            @pl.when(c == chunks - 1)
            def _():
                for buf_k in PAIR:
                    sub = 2 * k + buf_k
                    at_sub = columns(sub)
                    total = gp[a_rows, at_sub]
                    wait_n(buf_k)
                    psum[0, :, at_sub] = jnp.sum(total, axis=0, keepdims=True)
                    psum[0, :, wide(sub)] = jnp.sum(total * normed_of(0, 0, buf_k, at_sub), axis=0, keepdims=True)
                    load_z(lax.rem(sub + 2, chunks), buf_k)

    @pl.loop(0, chunks + 7)
    def _(t):
        phase = lax.rem(t, 3)

        @pl.when(t < chunks)
        def _():
            for s in AXES:
                @pl.when((phase == s) & (t >= RING))
                def _():
                    ring.wait_sends(t - RING, s - RING)
            z_swap(t).wait_recv()
            cols = columns(t)
            for half in PAIR:
                feats = pl.ds(512 * half, 512)
                part = jnp.dot(xt[1, feats, a_rows], own[1, b_rows, cols], preferred_element_type=jnp.float32)
                part += jnp.dot(xt[1, feats, b_rows], other[1, a_rows, cols], preferred_element_type=jnp.float32)
                acc[lax.rem(t, RING), half] = part.reshape(2, 2, BLOCK, COLS)

        for s in AXES:
            @pl.when(phase == s)
            def _():
                @pl.when(t < chunks)
                def _():
                    ring.send(0, t, s)

                for step in PAIR:
                    u = t - 1 - step

                    @pl.when((u >= 0) & (u < chunks))
                    def _():
                        ring.add(step, u, s - 1 - step)
                        ring.send(step + 1, u, s - 1 - step)

                @pl.when((t >= 3) & (t < chunks + 3))
                def _():
                    corr_block(t - 3, s - 3)

                for step in PAIR:
                    v = t - 4 - step

                    @pl.when((v >= 0) & (v < chunks))
                    def _():
                        for r in AXES:
                            gather(step, v, s - 4 - step, r).wait_recv()
                            gather(step + 1, v, s - 4 - step, r).start()

                @pl.when((t >= 6) & (t < chunks + 6))
                def _():
                    for r in AXES:
                        gather(2, t - 6, s - 6, r).wait_recv()
                    across(t - 6).start()

        @pl.when(t == 1)
        def _():
            z_turn.wait_send()
            turn_x(own.at[0], 0)

        @pl.when(t >= 7)
        def _():
            c = t - 7
            across(c).wait_recv()
            embed_chunk(c)

    start, chips, finish, close = sums_of(0)
    start()
    chips()
    for t in range(chunks - RING, chunks):
        ring.wait_sends(t, t)
    for t in range(chunks):
        across(t).wait_send()
        z_swap(t).wait_send()
        for step in AXES:
            for r in AXES:
                gather(step, t, t, r).wait_send()
    finish()
    close()
    loss_ref[...] = jnp.sum(sums_ref[0, 0, :, last_cols], axis=1, keepdims=True) + jnp.zeros((1, BLOCK), jnp.float32)

    def norm_pairs(lo, hi):
        @pl.loop(lo, hi)
        def _(pair):
            for buf in PAIR:
                c = 2 * pair + buf
                norm_chunk(0, None, 0, c, buf)

                @pl.when(c < chunks - 2)
                def _():
                    load_z(c + 2, buf)

    norm_pairs(0, 1)

    @pl.loop(0, jobs * chunks + 3)
    def _(t):
        j = t // chunks
        n = lax.rem(t, chunks)
        jb = lax.rem(j, 2)
        jn = 1 - jb
        phase = lax.rem(t, 3)

        @pl.when(t < jobs * chunks)
        def _():
            for s in AXES:
                @pl.when((phase == s) & (t >= RING))
                def _():
                    ring.wait_sends(t - RING, s - RING)

            @pl.when(n == 0)
            def _():
                x_swap(jb).wait_recv()
            swap(jb, n).wait_recv()
            cols = columns(n)
            slot = lax.rem(t, RING)
            for half in PAIR:
                feats = pl.ds(512 * half, 512)
                part = jnp.dot(xt[jb, feats, pl.ds(0, rows)], own[jb, :, cols], preferred_element_type=jnp.float32)
                part += jnp.dot(xt[jb, feats, pl.ds(rows, rows)], other[jb, :, cols],
                                preferred_element_type=jnp.float32)
                acc[slot, half] = part.reshape(2, 2, BLOCK, COLS)

        for s in AXES:
            @pl.when(phase == s)
            def _():
                @pl.when(t < jobs * chunks)
                def _():
                    ring.send(0, t, s)

                for step in PAIR:
                    u = t - 1 - step

                    @pl.when((u >= 0) & (u < jobs * chunks))
                    def _():
                        ring.add(step, u, s - 1 - step)
                        ring.send(step + 1, u, s - 1 - step)

                @pl.when(t >= 3)
                def _():
                    u = t - 3
                    for r in AXES:
                        off, size, val = ring.result(u, s - 3, r)
                        out_ref[u // chunks, pl.ds(off, size), columns(lax.rem(u, chunks))] = val

        @pl.when(t == 0)
        def _():
            norm_pairs(1, chunks // 2)
            for buf in PAIR:
                load_n(0, buf, buf)

        @pl.when(j < jobs - 1)
        def _():
            start, chips, finish, close = sums_of(j + 1)

            @pl.when(n < 4)
            def _():
                layer_pair(j, jb, n)
                for buf in PAIR:
                    c = 2 * n + buf

                    @pl.when(n < 3)
                    def _():
                        load_w(j, c + 2, buf)
                        load_n(j, c + 2, buf)

                    @pl.when(n == 3)
                    def _():
                        load_n(j, buf, buf)

            @pl.when(n == 3)
            def _():
                start()

                @pl.when(j == 1)
                def _():
                    for load in load_h(xs):
                        load.start()

            @pl.when(n == 4)
            def _():
                chips()

            @pl.when(n == 5)
            def _():
                finish()

                @pl.when(j == 1)
                def _():
                    for load in load_h(xs):
                        load.wait()
                x_swap(jb).wait_send()
                turn_x(xs, jn)

            @pl.when(n == 6)
            def _():
                close()
                vec_ref[j] = sums_ref[j + 1, 0, :, pl.ds(0, 2 * width)] + sums_ref[j + 1, 1, :, pl.ds(0, 2 * width)]

                @pl.loop(0, chunks)
                def _(c):
                    swap(jb, c).wait_send()

            @pl.when(n >= 6)
            def _():
                @pl.loop(0, 2)
                def _(pair):
                    for buf in PAIR:
                        c = (n - 6) * 4 + pair * 2 + buf
                        norm_chunk(j + 1, 1 - j, jn, c, buf)

                        @pl.when(c < chunks - 2)
                        def _():
                            load_n(j, c + 2, buf)

            @pl.when((n == 7) & (j == 0))
            def _():
                for buf in PAIR:
                    load_n(1, buf, buf)
                    load_w(1, buf, buf)

    for t in range(jobs * chunks - RING, jobs * chunks):
        ring.wait_sends(t, t)

    @pl.loop(0, chunks)
    def _(c):
        swap(0, c).wait_send()
    x_swap(0).wait_send()


VM = pl.BlockSpec(memory_space=pltpu.VMEM)


def whole_step(lam, vectors, h_a, h_b, weights, total_rows):
    view_rows, width = h_a.shape
    rows = 2 * view_rows
    chunks = width // COLS
    hbm = pl.BlockSpec(memory_space=pltpu.HBM)
    bf16, f32 = jnp.bfloat16, jnp.float32
    dma = pltpu.SemaphoreType.DMA
    wide = 2 * width + COLS
    return pl.pallas_call(
        functools.partial(whole_kernel, 1.0 / total_rows),
        out_shape=(jax.ShapeDtypeStruct((3, BLOCK, width), f32), jax.ShapeDtypeStruct((2, 1, 2 * width), f32),
                   jax.ShapeDtypeStruct((1, BLOCK), f32)) + (jax.ShapeDtypeStruct((rows, width), f32),) * 3,
        in_specs=[pl.BlockSpec(memory_space=pltpu.SMEM)] + [VM] * 4 + [hbm] * 5, out_specs=(VM,) * 3 + (hbm,) * 3,
        scratch_shapes=[
            pltpu.VMEM((2, width // 2, 2 * rows), bf16),
            pltpu.VMEM((width // 2, rows), bf16),
            pltpu.VMEM((rows, width), bf16),
            pltpu.VMEM((2, rows, width), bf16),
            pltpu.VMEM((2, rows, width), bf16),
            pltpu.VMEM((RING, 2, 2, 2, BLOCK, COLS), f32),
            pltpu.VMEM((RING, 2, 2, BLOCK, COLS), f32),
            pltpu.VMEM((RING, 2, BLOCK, COLS), f32),
            pltpu.VMEM((RING, BLOCK, COLS), f32),
            pltpu.VMEM((rows, width), f32),
            pltpu.VMEM((2, COLS, width), bf16),
            pltpu.VMEM((2, rows, COLS), f32),
            pltpu.VMEM((3, 1, wide), f32),
            pltpu.VMEM((8, 1, wide), f32),
            pltpu.VMEM((3, 2, 1, wide), f32),
            pltpu.VMEM((2, 2, 2, 2, BLOCK, width), bf16),
            pltpu.VMEM((BLOCK, COLS), f32),
            pltpu.VMEM((2, 1, width), f32),
            pltpu.VMEM((2, 1, width), f32),
            pltpu.VMEM((3, 2, 1, width), f32),
            pltpu.VMEM((3, 2, 1, width), f32),
            pltpu.VMEM((2, 2, 1, 2 * width), f32),
            pltpu.VMEM((2, 8, 1, 2 * width), f32),
            pltpu.VMEM((2, 1, 2 * width), f32),
            dma((RING, 9)), dma((RING, 9)), dma((2, chunks + 1)), dma((2, chunks + 1)),
            dma, dma, dma((7,)), dma((7,)), dma, dma, dma((2,)), dma((2,)), dma((2,)),
            dma((chunks, 10)), dma((chunks, 10)),
            dma((2, width // STRIP)), dma((2, width // STRIP)),
            dma((2,)), dma((2,)), dma((2, 7)), dma((2, 7)),
        ],
        compiler_params=pltpu.CompilerParams(collective_id=1, has_side_effects=True, vmem_limit_bytes=67043328),
        name="whole_step",
    )(lam.reshape(1, 1), *(v.reshape(width // BLOCK, BLOCK) for v in vectors), h_a, h_b,
      *(w.reshape(2, width // 2, width) for w in weights))


def solution(mesh):
    shards = mesh.shape["data"]

    def local_step(h_a, h_b, w_one, w_two, w_three, gain_one, shift_one, gain_two, shift_two, lam_off):
        rows_dev, width = h_a.shape
        total_rows = rows_dev * shards
        weights, vectors, loss = whole_step(lam_off, (gain_one, shift_one, gain_two, shift_two), h_a, h_b,
                                            (w_one, w_two, w_three), total_rows)[:3]
        return (loss[0, 0], weights[2], weights[1], weights[0],
                vectors[1, 0, width:], vectors[1, 0, :width], vectors[0, 0, width:], vectors[0, 0, :width])

    row_spec = P("data", None)
    whole_mat = P(None, None)
    whole_vec = P(None)
    return jax.shard_map(
        local_step, mesh=mesh,
        in_specs=(row_spec, row_spec, whole_mat, whole_mat, whole_mat,
                  whole_vec, whole_vec, whole_vec, whole_vec, P()),
        out_specs=(P(), row_spec, row_spec, row_spec, whole_vec, whole_vec, whole_vec, whole_vec),
        check_vma=False)
```

```python
import functools

import jax
import jax.numpy as jnp
from jax import lax
from jax.experimental import pallas as pl
from jax.experimental.pallas import tpu as pltpu
from jax.sharding import PartitionSpec as P

NORM_EPS = 1e-5
MESH = pl.DeviceIdType.MESH
RING = 4
COLS = 256
STRIP = 512
BLOCK = 128
PAIR = range(2)
AXES = range(3)
F32_SPLIT = ((48, 40, 40), (40, 48, 40), (40, 40, 48))
BF16_SPLIT = ((48, 48, 32), (32, 48, 48), (48, 32, 48))


LAST_DIMS = (((1,), (1,)), ((), ()))


def odd(n):
    return n % 2


class Place:
    def __init__(self):
        self.me = lax.axis_index("data")
        self.core = lax.rem(self.me, 2)
        self.chip = self.me // 2
        self.coord = (self.chip // 4, lax.rem(self.chip // 2, 2), lax.rem(self.chip, 2))
        self.partner = self.me + 1 - 2 * self.core
        steps = [(1 - 2 * c) * w for c, w in zip(self.coord, (8, 4, 2))]
        self.near = tuple(self.me + step for step in steps)
        self.chips = [self.me + sum(steps[a] for a in flips)
                      for flips in ((0, 1, 2), (0, 1), (0, 2), (1, 2), (0,), (1,), (2,))]


def greet(peers):
    barrier = pltpu.get_barrier_semaphore()
    for peer in peers:
        pl.semaphore_signal(barrier, inc=1, device_id=(peer,), device_id_type=MESH)
    pl.semaphore_wait(barrier, len(peers))


def remote(src, dst, send, recv, peer):
    return pltpu.make_async_remote_copy(src_ref=src, dst_ref=dst, send_sem=send, recv_sem=recv,
                                        device_id=(peer,), device_id_type=MESH)


def row_parts(split, phase):
    sizes = split[phase % 3]
    return tuple((sum(sizes[:r]), sizes[r]) for r in AXES)


class HalvingReduce:
    def __init__(self, place, acc, bufs, ssem, rsem):
        self.place, self.acc, self.bufs, self.ssem, self.rsem = place, acc, bufs, ssem, rsem

    def at(self, t, picks):
        return (lax.rem(t, RING),) + tuple(picks)

    def copy(self, step, t, phase, r):
        slot = lax.rem(t, RING)
        off, size = row_parts(F32_SPLIT, phase)[r]
        rows = pl.ds(off, size)
        picks = [slice(None)] * 3
        for k in range(step):
            axis = (r + k) % 3
            picks[axis] = self.place.coord[axis]
        axis = (r + step) % 3
        picks[axis] = 1 - self.place.coord[axis]
        src = self.acc.at[(slot, *picks, rows, slice(None))]
        dst = self.bufs[step].at[(slot,) + (slice(None),) * (2 - step) + (rows, slice(None))]
        return remote(src, dst, self.ssem.at[slot, 3 * step + r], self.rsem.at[slot, 3 * step + r],
                      self.place.near[axis])

    def send(self, step, t, phase):
        for r in AXES:
            self.copy(step, t, phase, r).start()

    def wait_sends(self, t, phase):
        for step in AXES:
            for r in AXES:
                self.copy(step, t, phase, r).wait_send()

    def add(self, step, t, phase):
        slot = lax.rem(t, RING)
        for r in AXES:
            self.copy(step, t, phase, r).wait_recv()
            off, size = row_parts(F32_SPLIT, phase)[r]
            rows = pl.ds(off, size)
            fixed = {(r + k) % 3 for k in range(step + 1)}
            free = [a for a in range(3) if a not in fixed]
            for n in range(2 ** len(free)):
                picks = list(self.place.coord)
                sub = []
                for pos, a in enumerate(free):
                    bit = (n >> (len(free) - 1 - pos)) & 1
                    picks[a] = bit
                    sub.append(bit)
                where = (slot, *picks, rows, slice(None))
                self.acc[where] = self.acc[where] + self.bufs[step][(slot, *sub, rows, slice(None))]

    def result(self, t, phase, r):
        slot = lax.rem(t, RING)
        self.copy(2, t, phase, r).wait_recv()
        off, size = row_parts(F32_SPLIT, phase)[r]
        rows = pl.ds(off, size)
        return off, size, (self.acc[(slot, *self.place.coord, rows, slice(None))]
                           + self.bufs[2][(slot, rows, slice(None))])


def columns(t, width=COLS):
    return pl.ds(pl.multiple_of(t * width, width), width)


def exchange_parts(place, psum, parts, total, sems):
    asend, arecv, csend, crecv, fsend, frecv = sems
    other = 1 - place.core
    land = psum.at[2]
    first = remote(psum.at[other], land, asend, arecv, place.partner)
    mine = parts.at[place.chip]
    across = [remote(mine, mine, csend.at[n], crecv.at[n], peer) for n, peer in enumerate(place.chips)]
    last = remote(total.at[place.core], total.at[place.core], fsend, frecv, place.partner)

    def start():
        first.start()

    def chips():
        first.wait_recv()
        parts[place.chip] = psum[place.core] + psum[2]
        for copy in across:
            copy.start()

    def finish():
        for copy in across:
            copy.wait_recv()
        value = parts[0]
        for c in range(1, 8):
            value = value + parts[c]
        total[place.core] = value
        last.start()

    def close():
        last.wait_recv()
        first.wait_send()
        for copy in across:
            copy.wait_send()
        last.wait_send()

    return start, chips, finish, close


def exchange_pair(place, own, land, parts, total, sems):
    asend, arecv, csend, crecv = sems
    first = remote(own, land, asend, arecv, place.partner)
    mine = parts.at[place.chip]
    across = [remote(mine, mine, csend.at[n], crecv.at[n], peer) for n, peer in enumerate(place.chips)]

    def chips():
        first.wait_recv()
        parts[place.chip] = own[...] + land[...]
        for copy in across:
            copy.start()

    def finish():
        first.wait_send()
        for copy in across:
            copy.wait()
        value = parts[0]
        for c in range(1, 8):
            value = value + parts[c]
        total[...] = value

    return first.start, chips, finish


def whole_kernel(inv_rows, lam_ref, g1_ref, s1_ref, g2_ref, s2_ref, ha_hbm, hb_hbm, w1_hbm, w2_hbm, w3_hbm,
                 out_ref, vec_ref, loss_ref, n1_hbm, n2_hbm, n3_hbm,
                 xt, xsend, xs, own, other, acc, b0, b1, b2, gp, wbuf, nbuf, psum, parts, sums_ref, grads, stage,
                 gains, shifts, means, invs, fsum, fparts, ftotal,
                 ssem, rsem, psend, precv, asend, arecv, csend, crecv, fsend, frecv, lsem, wsem, nsem, gsend, grecv,
                 usem, vsem, easend, earecv, ecsend, ecrecv):
    place = Place()
    view_rows, width = ha_hbm.shape
    rows = 2 * view_rows
    chunks = width // COLS
    jobs = 3
    partner = place.partner
    ring = HalvingReduce(place, acc, (b0, b1, b2), ssem, rsem)

    def load_w(j, c, buf):
        rows_c = columns(lax.rem(c, chunks // 2))
        for k, ref in enumerate((w3_hbm, w2_hbm)):
            @pl.when(j == k)
            def _():
                pltpu.make_async_copy(ref.at[c // (chunks // 2), rows_c, :], wbuf.at[buf], wsem.at[buf]).start()

    def load_z(c, buf):
        pltpu.make_async_copy(n3_hbm.at[:, columns(c)], nbuf.at[buf], nsem.at[buf]).start()

    def load_n(j, c, buf):
        for k, ref in enumerate((n2_hbm, n1_hbm)):
            @pl.when(j == k)
            def _():
                pltpu.make_async_copy(ref.at[:, columns(c)], nbuf.at[buf], nsem.at[buf]).start()

    def wait_w(buf):
        pltpu.make_async_copy(w3_hbm.at[0, pl.ds(0, COLS), :], wbuf.at[buf], wsem.at[buf]).wait()

    def wait_n(buf):
        pltpu.make_async_copy(n2_hbm.at[:, pl.ds(0, COLS)], nbuf.at[buf], nsem.at[buf]).wait()

    def swap(jb, c):
        cols = columns(c)
        return remote(own.at[jb, :, cols], other.at[jb, :, cols], psend.at[jb, c], precv.at[jb, c], partner)

    def x_swap(jb):
        return remote(xsend, xt.at[jb, :, pl.ds(rows, rows)], psend.at[jb, chunks], precv.at[jb, chunks], partner)

    def load_h(dst):
        return [pltpu.make_async_copy(ref, dst.at[pl.ds(view * view_rows, view_rows), :], lsem.at[view])
                for view, ref in enumerate((ha_hbm, hb_hbm))]

    def turn(src, depth, copy, jb):
        def blocks(dst, parity):
            @pl.loop(0, 8)
            def _(b):
                to = pl.ds(pl.multiple_of(b * BLOCK, BLOCK), BLOCK)
                cols = pl.ds(pl.multiple_of((2 * b + parity) * BLOCK, BLOCK), BLOCK)
                dst[to, pl.ds(0, depth)] = src[pl.ds(0, depth), cols].T

        blocks(xsend, 1 - place.core)
        copy.start()
        blocks(xt.at[jb], place.core)

    def turn_x(src, jb):
        turn(src, rows, x_swap(jb), jb)

    def sums_of(i):
        return exchange_parts(place, psum, parts, sums_ref.at[i], (asend, arecv, csend, crecv, fsend, frecv))

    def wide(c):
        return pl.ds(pl.multiple_of(width + c * COLS, COLS), COLS)

    def normed_of(i, view, buf, cols):
        at = pl.ds(view * view_rows, view_rows)
        return (nbuf[buf, at, :] - means[i, view, :, cols]) * invs[i, view, :, cols]

    def layer_pair(j, jb, n):
        for buf in PAIR:
            wait_w(buf)
            wait_n(buf)
        for view in PAIR:
            at = pl.ds(view * view_rows, view_rows)
            both = lax.dot_general(own[jb, at, :], wbuf[...].reshape(2 * COLS, width), LAST_DIMS,
                                   preferred_element_type=jnp.float32)
            for buf in PAIR:
                c = 2 * n + buf
                cols = columns(c)
                normed = normed_of(j + 1, view, buf, cols)
                grad = jnp.where(gains[1 - j, :, cols] * normed + shifts[1 - j, :, cols] > 0,
                                 both[:, buf * COLS:(buf + 1) * COLS], 0.0)
                gp[at, cols] = grad
                psum[view, :, cols] = jnp.sum(grad, axis=0, keepdims=True)
                psum[view, :, wide(c)] = jnp.sum(grad * normed, axis=0, keepdims=True)

    def norm_chunk(i, gain, jn, c, buf):
        cols = columns(c)
        wait_n(buf)
        for view in PAIR:
            at = pl.ds(view * view_rows, view_rows)
            first = sums_ref[i, view, :, cols]
            second = sums_ref[i, view, :, wide(c)]
            grad = invs[i, view, :, cols] * (gp[at, cols] - (first + normed_of(i, view, buf, cols) * second) * inv_rows)
            if gain is not None:
                grad = gains[gain, :, cols] * grad
            own[jn, at, cols] = grad.astype(jnp.bfloat16)
        swap(jn, c).start()

    half = width // 2
    strips = width // STRIP
    weights = (w1_hbm, w2_hbm, w3_hbm)
    w_slots = (xt, other, xt)
    hidden_out = (n1_hbm, n2_hbm, n3_hbm)

    def view_at(view):
        return pl.ds(view * view_rows, view_rows)

    def fetch_w(l, c):
        cols = columns(c, STRIP)
        return pltpu.make_async_copy(weights[l].at[:, :, cols], w_slots[l].at[:, :, cols], vsem.at[odd(l), c])

    def fetch_all(l, lo=0):
        @pl.loop(lo, strips)
        def _(c):
            fetch_w(l, c).start()

    load_a, load_b = load_h(own.at[0])
    load_a.start()
    fetch_w(0, 0).start()
    fetch_w(0, 1).start()

    @pl.loop(0, width // BLOCK)
    def _(r):
        lanes = pl.ds(pl.multiple_of(r * BLOCK, BLOCK), BLOCK)
        for n, (g_ref, s_ref) in enumerate(((g1_ref, s1_ref), (g2_ref, s2_ref))):
            gains[n, :, lanes] = g_ref[pl.ds(r, 1), :]
            shifts[n, :, lanes] = s_ref[pl.ds(r, 1), :]

    swaps = [exchange_pair(place, fsum.at[v, 0], fsum.at[v, 1], fparts.at[v], ftotal.at[v],
                           tuple(sem.at[v] for sem in (easend, earecv, ecsend, ecrecv)))
             for v in PAIR]
    load_b.start()
    fetch_all(0, 2)
    greet([partner] + place.chips)
    load_a.wait()

    def far(c, size):
        return pl.ds(pl.multiple_of(width + c * size, size), size)

    def hidden_copy(l, view, c):
        cols = columns(c, STRIP)
        return pltpu.make_async_copy(gp.at[view_at(view), cols], hidden_out[l].at[view_at(view), cols],
                                     usem.at[view, c])

    def products(l, view, actions):
        at = view_at(view)

        @pl.loop(0, strips)
        def _(c):
            for when, action in actions:
                pl.when(c == when)(action)
            if view == 0:
                fetch_w(l, c).wait()
            if l:
                hidden_copy(l - 1, view, c).wait()
            cols = columns(c, STRIP)
            value = jnp.dot(own[odd(l), at, pl.ds(0, half)], w_slots[l][0, :, cols],
                            preferred_element_type=jnp.float32)
            value += jnp.dot(own[odd(l), at, pl.ds(half, half)], w_slots[l][1, :, cols],
                             preferred_element_type=jnp.float32)
            gp[at, cols] = value
            fsum[view, 0, :, cols] = jnp.sum(value, axis=0, keepdims=True)
            fsum[view, 0, :, far(c, STRIP)] = jnp.sum(value * value, axis=0, keepdims=True)
            hidden_copy(l, view, c).start()

    def normalise(l, view, after=None):
        at = view_at(view)

        @pl.loop(0, chunks)
        def _(c):
            cols = columns(c)
            mean = ftotal[view, :, cols] * inv_rows
            square = ftotal[view, :, far(c, COLS)] * inv_rows
            inv = lax.rsqrt(square - mean * mean + NORM_EPS)
            means[2 - l, view, :, cols] = mean
            invs[2 - l, view, :, cols] = inv
            act = (gp[at, cols] - mean) * inv
            if l < 2:
                act = jnp.maximum(gains[l, :, cols] * act + shifts[l, :, cols], 0.0)
            act = act.astype(jnp.bfloat16)
            own[odd(l + 1), at, cols] = act
            if l == 0:
                xs[at, cols] = act
            if after is not None:
                after(c)

    a_swap, b_swap = swaps
    for l in AXES:
        products(l, 0, ((0, b_swap[1]),) if l else ())
        a_swap[0]()
        if l:
            b_swap[2]()
            normalise(l - 1, 1)
        else:
            fetch_all(1)
            load_b.wait()
        products(l, 1, ((0, a_swap[1]),))
        b_swap[0]()
        if l == 0:
            fetch_all(2)
        a_swap[2]()
        normalise(l, 0)

    lam = lam_ref[0, 0]
    a_rows, b_rows = view_at(0), view_at(1)
    last_cols = pl.ds(2 * width, COLS)
    for view in PAIR:
        psum[view, :, last_cols] = jnp.zeros((1, COLS), jnp.float32)
    for buf in PAIR:
        load_w(0, buf, buf)

    def z_swap(c):
        cols = columns(c)
        return remote(own.at[1, b_rows, cols], other.at[1, a_rows, cols], psend.at[1, c], precv.at[1, c], partner)

    z_turn = remote(xsend.at[:, a_rows], xt.at[1, :, b_rows], psend.at[1, chunks], precv.at[1, chunks], partner)
    b_swap[1]()
    turn(own.at[1], view_rows, z_turn, 1)
    b_swap[2]()
    normalise(2, 1, lambda c: z_swap(c).start())
    for view in PAIR:
        @pl.loop(0, strips)
        def _(c):
            hidden_copy(2, view, c).wait()
    for buf in PAIR:
        load_z(buf, buf)
    z_turn.wait_recv()

    def gather(step, t, phase, r):
        off, size = row_parts(BF16_SPLIT, phase)[r]
        picks = list(place.coord)
        for k in range(step):
            picks[(r + 2 - k) % 3] = slice(None)
        axis = (r + 2 - step) % 3
        ref = grads.at[(*picks, place.core, pl.ds(off, size), columns(t))]
        return remote(ref, ref, gsend.at[t, 3 * step + r], grecv.at[t, 3 * step + r], place.near[axis])

    def across(t):
        ref = grads.at[:, :, :, place.core, :, columns(t)]
        return remote(ref, ref, gsend.at[t, 9], grecv.at[t, 9], partner)

    def corr_block(t, phase):
        for r in AXES:
            off, size, val = ring.result(t, phase, r)
            corr = val * inv_rows
            row_id = place.me * BLOCK + off + lax.broadcasted_iota(jnp.int32, corr.shape, 0)
            col_id = t * COLS + lax.broadcasted_iota(jnp.int32, corr.shape, 1)
            diag = row_id == col_id
            gap = 1.0 - corr
            terms = jnp.where(diag, gap * gap, lam * corr * corr)
            psum[0, :, last_cols] += jnp.sum(terms, axis=0, keepdims=True)
            stage[pl.ds(off, size), :] = jnp.where(diag, -2.0 * gap, 2.0 * lam * corr) * inv_rows
        grads[(*place.coord, place.core, slice(None), columns(t))] = stage[...].astype(jnp.bfloat16)
        for r in AXES:
            gather(0, t, phase, r).start()

    def embed_chunk(c):
        cols = columns(c)
        buf = lax.rem(c, 2)
        block = grads[:, :, :, :, :, cols].reshape(width, COLS)
        grad = jnp.dot(own[1, a_rows, :], block, preferred_element_type=jnp.float32)
        gp[b_rows, cols] = grad
        wait_n(buf)
        psum[1, :, cols] = jnp.sum(grad, axis=0, keepdims=True)
        psum[1, :, wide(c)] = jnp.sum(grad * normed_of(0, 1, buf, cols), axis=0, keepdims=True)
        load_z(lax.rem(c + 2, chunks), buf)

        @pl.loop(0, chunks // 2)
        def _(k):
            rows_g = grads[k // 2, lax.rem(k, 2), :, :, :, cols].reshape(STRIP, COLS)
            more = lax.dot_general(own[1, b_rows, cols], rows_g, LAST_DIMS, preferred_element_type=jnp.float32)
            at_k = columns(k, STRIP)
            gp[a_rows, at_k] = jnp.where(c > 0, gp[a_rows, at_k], 0.0) + more

            @pl.when(c == chunks - 1)
            def _():
                for buf_k in PAIR:
                    sub = 2 * k + buf_k
                    at_sub = columns(sub)
                    total = gp[a_rows, at_sub]
                    wait_n(buf_k)
                    psum[0, :, at_sub] = jnp.sum(total, axis=0, keepdims=True)
                    psum[0, :, wide(sub)] = jnp.sum(total * normed_of(0, 0, buf_k, at_sub), axis=0, keepdims=True)
                    load_z(lax.rem(sub + 2, chunks), buf_k)

    def advance(stage, u, phase):
        if stage < 3:
            if stage:
                ring.add(stage - 1, u, phase)
            ring.send(stage, u, phase)
        elif stage == 3:
            corr_block(u, phase)
        else:
            for r in AXES:
                gather(stage - 4, u, phase, r).wait_recv()
                if stage < 6:
                    gather(stage - 3, u, phase, r).start()
            if stage == 6:
                across(u).start()

    def stages(t, phase, first):
        for s in AXES:
            @pl.when(phase == s)
            def _():
                for back in range(2, -1, -1) if first else range(4):
                    u = t - back

                    @pl.when((u >= 0) & (u < chunks))
                    def _():
                        advance(2 * back + first, u, s - back)

    @pl.loop(0, chunks + 3)
    def _(t):
        phase = lax.rem(t, 3)

        @pl.when(t < chunks)
        def _():
            for s in AXES:
                @pl.when((phase == s) & (t >= RING))
                def _():
                    ring.wait_sends(t - RING, s - RING)
            z_swap(t).wait_recv()
            cols = columns(t)
            part = jnp.dot(xt[1, :, a_rows], own[1, b_rows, cols], preferred_element_type=jnp.float32)
            part += jnp.dot(xt[1, :, b_rows], other[1, a_rows, cols], preferred_element_type=jnp.float32)
            acc[lax.rem(t, RING)] = part.reshape(2, 2, 2, BLOCK, COLS)

        stages(t, phase, 0)

        @pl.when(t == 1)
        def _():
            z_turn.wait_send()
            turn_x(own.at[0], 0)

        @pl.when(t >= 3)
        def _():
            across(t - 3).wait_recv()
            embed_chunk(t - 3)

        stages(t, phase, 1)

    start, chips, finish, close = sums_of(0)
    start()
    chips()
    for t in range(chunks - RING, chunks):
        ring.wait_sends(t, t)
    for t in range(chunks):
        across(t).wait_send()
        z_swap(t).wait_send()
        for step in AXES:
            for r in AXES:
                gather(step, t, t, r).wait_send()
    finish()
    close()
    loss_ref[...] = jnp.sum(sums_ref[0, 0, :, last_cols], axis=1, keepdims=True) + jnp.zeros((1, BLOCK), jnp.float32)

    def norm_pairs(lo, hi):
        @pl.loop(lo, hi)
        def _(pair):
            for buf in PAIR:
                c = 2 * pair + buf
                norm_chunk(0, None, 0, c, buf)

                @pl.when(c < chunks - 2)
                def _():
                    load_z(c + 2, buf)

    norm_pairs(0, 1)

    @pl.loop(0, jobs * chunks + 3)
    def _(t):
        j = t // chunks
        n = lax.rem(t, chunks)
        jb = lax.rem(j, 2)
        jn = 1 - jb
        phase = lax.rem(t, 3)

        @pl.when(t < jobs * chunks)
        def _():
            for s in AXES:
                @pl.when((phase == s) & (t >= RING))
                def _():
                    ring.wait_sends(t - RING, s - RING)

            @pl.when(n == 0)
            def _():
                x_swap(jb).wait_recv()
            swap(jb, n).wait_recv()
            cols = columns(n)
            slot = lax.rem(t, RING)
            part = jnp.dot(xt[jb, :, pl.ds(0, rows)], own[jb, :, cols], preferred_element_type=jnp.float32)
            part += jnp.dot(xt[jb, :, pl.ds(rows, rows)], other[jb, :, cols], preferred_element_type=jnp.float32)
            acc[slot] = part.reshape(2, 2, 2, BLOCK, COLS)

        start, chips, finish, close = sums_of(j + 1)
        pl.when((j < jobs - 1) & (n == 4))(chips)
        pl.when((j < jobs - 1) & (n == 5))(finish)

        for s in AXES:
            @pl.when(phase == s)
            def _():
                @pl.when(t < jobs * chunks)
                def _():
                    ring.send(0, t, s)

                for step in PAIR:
                    u = t - 1 - step

                    @pl.when((u >= 0) & (u < jobs * chunks))
                    def _():
                        ring.add(step, u, s - 1 - step)
                        ring.send(step + 1, u, s - 1 - step)

                @pl.when(t >= 3)
                def _():
                    u = t - 3
                    for r in AXES:
                        off, size, val = ring.result(u, s - 3, r)
                        out_ref[u // chunks, pl.ds(off, size), columns(lax.rem(u, chunks))] = val

        @pl.when(t == 0)
        def _():
            norm_pairs(1, chunks // 2)
            for buf in PAIR:
                load_n(0, buf, buf)

        @pl.when(j < jobs - 1)
        def _():
            @pl.when(n < 4)
            def _():
                layer_pair(j, jb, n)
                for buf in PAIR:
                    c = 2 * n + buf

                    @pl.when(n < 3)
                    def _():
                        load_w(j, c + 2, buf)
                        load_n(j, c + 2, buf)

                    @pl.when(n == 3)
                    def _():
                        load_n(j, buf, buf)

            @pl.when(n == 3)
            def _():
                start()

                @pl.when(j == 1)
                def _():
                    for load in load_h(xs):
                        load.start()

            @pl.when(n == 5)
            def _():
                @pl.when(j == 1)
                def _():
                    for load in load_h(xs):
                        load.wait()
                x_swap(jb).wait_send()
                turn_x(xs, jn)

            @pl.when(n == 6)
            def _():
                close()
                vec_ref[j] = sums_ref[j + 1, 0, :, pl.ds(0, 2 * width)] + sums_ref[j + 1, 1, :, pl.ds(0, 2 * width)]

                @pl.loop(0, chunks)
                def _(c):
                    swap(jb, c).wait_send()

            @pl.when(n >= 6)
            def _():
                @pl.loop(0, 2)
                def _(pair):
                    for buf in PAIR:
                        c = (n - 6) * 4 + pair * 2 + buf
                        norm_chunk(j + 1, 1 - j, jn, c, buf)

                        @pl.when(c < chunks - 2)
                        def _():
                            load_n(j, c + 2, buf)

            @pl.when((n == 7) & (j == 0))
            def _():
                for buf in PAIR:
                    load_n(1, buf, buf)
                    load_w(1, buf, buf)

    for t in range(jobs * chunks - RING, jobs * chunks):
        ring.wait_sends(t, t)

    @pl.loop(0, chunks)
    def _(c):
        swap(0, c).wait_send()
    x_swap(0).wait_send()


VM = pl.BlockSpec(memory_space=pltpu.VMEM)


def whole_step(lam, vectors, h_a, h_b, weights, total_rows):
    view_rows, width = h_a.shape
    rows = 2 * view_rows
    chunks = width // COLS
    hbm = pl.BlockSpec(memory_space=pltpu.HBM)
    bf16, f32 = jnp.bfloat16, jnp.float32
    dma = pltpu.SemaphoreType.DMA
    wide = 2 * width + COLS
    return pl.pallas_call(
        functools.partial(whole_kernel, 1.0 / total_rows),
        out_shape=(jax.ShapeDtypeStruct((3, BLOCK, width), f32), jax.ShapeDtypeStruct((2, 1, 2 * width), f32),
                   jax.ShapeDtypeStruct((1, BLOCK), f32)) + (jax.ShapeDtypeStruct((rows, width), f32),) * 3,
        in_specs=[pl.BlockSpec(memory_space=pltpu.SMEM)] + [VM] * 4 + [hbm] * 5, out_specs=(VM,) * 3 + (hbm,) * 3,
        scratch_shapes=[
            pltpu.VMEM((2, width // 2, 2 * rows), bf16),
            pltpu.VMEM((width // 2, rows), bf16),
            pltpu.VMEM((rows, width), bf16),
            pltpu.VMEM((2, rows, width), bf16),
            pltpu.VMEM((2, rows, width), bf16),
            pltpu.VMEM((RING, 2, 2, 2, BLOCK, COLS), f32),
            pltpu.VMEM((RING, 2, 2, BLOCK, COLS), f32),
            pltpu.VMEM((RING, 2, BLOCK, COLS), f32),
            pltpu.VMEM((RING, BLOCK, COLS), f32),
            pltpu.VMEM((rows, width), f32),
            pltpu.VMEM((2, COLS, width), bf16),
            pltpu.VMEM((2, rows, COLS), f32),
            pltpu.VMEM((3, 1, wide), f32),
            pltpu.VMEM((8, 1, wide), f32),
            pltpu.VMEM((3, 2, 1, wide), f32),
            pltpu.VMEM((2, 2, 2, 2, BLOCK, width), bf16),
            pltpu.VMEM((BLOCK, COLS), f32),
            pltpu.VMEM((2, 1, width), f32),
            pltpu.VMEM((2, 1, width), f32),
            pltpu.VMEM((3, 2, 1, width), f32),
            pltpu.VMEM((3, 2, 1, width), f32),
            pltpu.VMEM((2, 2, 1, 2 * width), f32),
            pltpu.VMEM((2, 8, 1, 2 * width), f32),
            pltpu.VMEM((2, 1, 2 * width), f32),
            dma((RING, 9)), dma((RING, 9)), dma((2, chunks + 1)), dma((2, chunks + 1)),
            dma, dma, dma((7,)), dma((7,)), dma, dma, dma((2,)), dma((2,)), dma((2,)),
            dma((chunks, 10)), dma((chunks, 10)),
            dma((2, width // STRIP)), dma((2, width // STRIP)),
            dma((2,)), dma((2,)), dma((2, 7)), dma((2, 7)),
        ],
        compiler_params=pltpu.CompilerParams(collective_id=1, has_side_effects=True, vmem_limit_bytes=67043328),
        name="whole_step",
    )(lam.reshape(1, 1), *(v.reshape(width // BLOCK, BLOCK) for v in vectors), h_a, h_b,
      *(w.reshape(2, width // 2, width) for w in weights))


def solution(mesh):
    shards = mesh.shape["data"]

    def local_step(h_a, h_b, w_one, w_two, w_three, gain_one, shift_one, gain_two, shift_two, lam_off):
        rows_dev, width = h_a.shape
        total_rows = rows_dev * shards
        weights, vectors, loss = whole_step(lam_off, (gain_one, shift_one, gain_two, shift_two), h_a, h_b,
                                            (w_one, w_two, w_three), total_rows)[:3]
        return (loss[0, 0], weights[2], weights[1], weights[0],
                vectors[1, 0, width:], vectors[1, 0, :width], vectors[0, 0, width:], vectors[0, 0, :width])

    row_spec = P("data", None)
    whole_mat = P(None, None)
    whole_vec = P(None)
    return jax.shard_map(
        local_step, mesh=mesh,
        in_specs=(row_spec, row_spec, whole_mat, whole_mat, whole_mat,
                  whole_vec, whole_vec, whole_vec, whole_vec, P()),
        out_specs=(P(), row_spec, row_spec, row_spec, whole_vec, whole_vec, whole_vec, whole_vec),
        check_vma=False)
```

```python
import functools

import jax
import jax.numpy as jnp
from jax import lax
from jax.experimental import pallas as pl
from jax.experimental.pallas import tpu as pltpu
from jax.sharding import PartitionSpec as P

NORM_EPS = 1e-5
MESH = pl.DeviceIdType.MESH
RING = 4
COLS = 256
STRIP = 1024
BLOCK = 128
PAIR = range(2)
AXES = range(3)
F32_SPLIT = ((48, 40, 40), (40, 48, 40), (40, 40, 48))
BF16_SPLIT = ((48, 48, 32), (32, 48, 48), (48, 32, 48))


LAST_DIMS = (((1,), (1,)), ((), ()))


def odd(n):
    return n % 2


class Place:
    def __init__(self):
        self.me = lax.axis_index("data")
        self.core = lax.rem(self.me, 2)
        self.chip = self.me // 2
        self.coord = (self.chip // 4, lax.rem(self.chip // 2, 2), lax.rem(self.chip, 2))
        self.partner = self.me + 1 - 2 * self.core
        steps = [(1 - 2 * c) * w for c, w in zip(self.coord, (8, 4, 2))]
        self.near = tuple(self.me + step for step in steps)
        self.chips = [self.me + sum(steps[a] for a in flips)
                      for flips in ((0, 1, 2), (0, 1), (0, 2), (1, 2), (0,), (1,), (2,))]


def greet(peers):
    barrier = pltpu.get_barrier_semaphore()
    for peer in peers:
        pl.semaphore_signal(barrier, inc=1, device_id=(peer,), device_id_type=MESH)
    pl.semaphore_wait(barrier, len(peers))


def remote(src, dst, send, recv, peer):
    return pltpu.make_async_remote_copy(src_ref=src, dst_ref=dst, send_sem=send, recv_sem=recv,
                                        device_id=(peer,), device_id_type=MESH)


def row_parts(split, phase):
    sizes = split[phase % 3]
    return tuple((sum(sizes[:r]), sizes[r]) for r in AXES)


class HalvingReduce:
    def __init__(self, place, acc, bufs, ssem, rsem):
        self.place, self.acc, self.bufs, self.ssem, self.rsem = place, acc, bufs, ssem, rsem

    def at(self, t, picks):
        return (lax.rem(t, RING),) + tuple(picks)

    def copy(self, step, t, phase, r):
        slot = lax.rem(t, RING)
        off, size = row_parts(F32_SPLIT, phase)[r]
        rows = pl.ds(off, size)
        picks = [slice(None)] * 3
        for k in range(step):
            axis = (r + k) % 3
            picks[axis] = self.place.coord[axis]
        axis = (r + step) % 3
        picks[axis] = 1 - self.place.coord[axis]
        src = self.acc.at[(slot, *picks, rows, slice(None))]
        dst = self.bufs[step].at[(slot,) + (slice(None),) * (2 - step) + (rows, slice(None))]
        return remote(src, dst, self.ssem.at[slot, 3 * step + r], self.rsem.at[slot, 3 * step + r],
                      self.place.near[axis])

    def send(self, step, t, phase):
        for r in AXES:
            self.copy(step, t, phase, r).start()

    def wait_sends(self, t, phase):
        for step in AXES:
            for r in AXES:
                self.copy(step, t, phase, r).wait_send()

    def add(self, step, t, phase):
        slot = lax.rem(t, RING)
        for r in AXES:
            self.copy(step, t, phase, r).wait_recv()
            off, size = row_parts(F32_SPLIT, phase)[r]
            rows = pl.ds(off, size)
            fixed = {(r + k) % 3 for k in range(step + 1)}
            free = [a for a in range(3) if a not in fixed]
            for n in range(2 ** len(free)):
                picks = list(self.place.coord)
                sub = []
                for pos, a in enumerate(free):
                    bit = (n >> (len(free) - 1 - pos)) & 1
                    picks[a] = bit
                    sub.append(bit)
                where = (slot, *picks, rows, slice(None))
                self.acc[where] = self.acc[where] + self.bufs[step][(slot, *sub, rows, slice(None))]

    def result(self, t, phase, r):
        slot = lax.rem(t, RING)
        self.copy(2, t, phase, r).wait_recv()
        off, size = row_parts(F32_SPLIT, phase)[r]
        rows = pl.ds(off, size)
        return off, size, (self.acc[(slot, *self.place.coord, rows, slice(None))]
                           + self.bufs[2][(slot, rows, slice(None))])


def columns(t, width=COLS):
    return pl.ds(pl.multiple_of(t * width, width), width)


def exchange_parts(place, psum, parts, total, sems):
    asend, arecv, csend, crecv, fsend, frecv = sems
    other = 1 - place.core
    land = psum.at[2]
    first = remote(psum.at[other], land, asend, arecv, place.partner)
    mine = parts.at[place.chip]
    across = [remote(mine, mine, csend.at[n], crecv.at[n], peer) for n, peer in enumerate(place.chips)]
    last = remote(total.at[place.core], total.at[place.core], fsend, frecv, place.partner)

    def start():
        first.start()

    def chips():
        first.wait_recv()
        parts[place.chip] = psum[place.core] + psum[2]
        for copy in across:
            copy.start()

    def finish():
        for copy in across:
            copy.wait_recv()
        value = parts[0]
        for c in range(1, 8):
            value = value + parts[c]
        total[place.core] = value
        last.start()

    def close():
        last.wait_recv()
        first.wait_send()
        for copy in across:
            copy.wait_send()
        last.wait_send()

    return start, chips, finish, close


def exchange_pair(place, own, land, parts, total, sems):
    asend, arecv, csend, crecv = sems
    first = remote(own, land, asend, arecv, place.partner)
    mine = parts.at[place.chip]
    across = [remote(mine, mine, csend.at[n], crecv.at[n], peer) for n, peer in enumerate(place.chips)]

    def chips():
        first.wait_recv()
        parts[place.chip] = own[...] + land[...]
        for copy in across:
            copy.start()

    def finish():
        first.wait_send()
        for copy in across:
            copy.wait()
        value = parts[0]
        for c in range(1, 8):
            value = value + parts[c]
        total[...] = value

    return first.start, chips, finish


def whole_kernel(inv_rows, lam_ref, g1_ref, s1_ref, g2_ref, s2_ref, ha_hbm, hb_hbm, w1_hbm, w2_hbm, w3_hbm,
                 out_ref, vec_ref, loss_ref, n1_hbm, n2_hbm, n3_hbm,
                 xt, xsend, xs, own, other, acc, b0, b1, b2, gp, wbuf, nbuf, psum, parts, sums_ref, grads, stage,
                 gains, shifts, means, invs, fsum, fparts, ftotal,
                 ssem, rsem, psend, precv, asend, arecv, csend, crecv, fsend, frecv, lsem, wsem, nsem, gsend, grecv,
                 usem, vsem, easend, earecv, ecsend, ecrecv):
    place = Place()
    view_rows, width = ha_hbm.shape
    rows = 2 * view_rows
    chunks = width // COLS
    jobs = 3
    partner = place.partner
    ring = HalvingReduce(place, acc, (b0, b1, b2), ssem, rsem)

    def load_w(j, c, buf):
        rows_c = columns(lax.rem(c, chunks // 2))
        for k, ref in enumerate((w3_hbm, w2_hbm)):
            @pl.when(j == k)
            def _():
                pltpu.make_async_copy(ref.at[c // (chunks // 2), rows_c, :], wbuf.at[buf], wsem.at[buf]).start()

    def load_z(c, buf):
        pltpu.make_async_copy(n3_hbm.at[:, columns(c)], nbuf.at[buf], nsem.at[buf]).start()

    def load_n(j, c, buf):
        for k, ref in enumerate((n2_hbm, n1_hbm)):
            @pl.when(j == k)
            def _():
                pltpu.make_async_copy(ref.at[:, columns(c)], nbuf.at[buf], nsem.at[buf]).start()

    def wait_w(buf):
        pltpu.make_async_copy(w3_hbm.at[0, pl.ds(0, COLS), :], wbuf.at[buf], wsem.at[buf]).wait()

    def wait_n(buf):
        pltpu.make_async_copy(n2_hbm.at[:, pl.ds(0, COLS)], nbuf.at[buf], nsem.at[buf]).wait()

    def swap(jb, c):
        cols = columns(c)
        return remote(own.at[jb, :, cols], other.at[jb, :, cols], psend.at[jb, c], precv.at[jb, c], partner)

    def x_swap(jb):
        return remote(xsend, xt.at[jb, :, pl.ds(rows, rows)], psend.at[jb, chunks], precv.at[jb, chunks], partner)

    def load_h(dst):
        return [pltpu.make_async_copy(ref, dst.at[pl.ds(view * view_rows, view_rows), :], lsem.at[view])
                for view, ref in enumerate((ha_hbm, hb_hbm))]

    def turn(src, depth, copy, jb):
        def blocks(dst, parity):
            @pl.loop(0, 8)
            def _(b):
                to = pl.ds(pl.multiple_of(b * BLOCK, BLOCK), BLOCK)
                cols = pl.ds(pl.multiple_of((2 * b + parity) * BLOCK, BLOCK), BLOCK)
                dst[to, pl.ds(0, depth)] = src[pl.ds(0, depth), cols].T

        blocks(xsend, 1 - place.core)
        copy.start()
        blocks(xt.at[jb], place.core)

    def turn_x(src, jb):
        turn(src, rows, x_swap(jb), jb)

    def sums_of(i):
        return exchange_parts(place, psum, parts, sums_ref.at[i], (asend, arecv, csend, crecv, fsend, frecv))

    def wide(c):
        return pl.ds(pl.multiple_of(width + c * COLS, COLS), COLS)

    def normed_of(i, view, buf, cols):
        at = pl.ds(view * view_rows, view_rows)
        return (nbuf[buf, at, :] - means[i, view, :, cols]) * invs[i, view, :, cols]

    def layer_pair(j, jb, n):
        for buf in PAIR:
            wait_w(buf)
            wait_n(buf)
        for view in PAIR:
            at = pl.ds(view * view_rows, view_rows)
            both = lax.dot_general(own[jb, at, :], wbuf[...].reshape(2 * COLS, width), LAST_DIMS,
                                   preferred_element_type=jnp.float32)
            for buf in PAIR:
                c = 2 * n + buf
                cols = columns(c)
                normed = normed_of(j + 1, view, buf, cols)
                grad = jnp.where(gains[1 - j, :, cols] * normed + shifts[1 - j, :, cols] > 0,
                                 both[:, buf * COLS:(buf + 1) * COLS], 0.0)
                gp[at, cols] = grad
                psum[view, :, cols] = jnp.sum(grad, axis=0, keepdims=True)
                psum[view, :, wide(c)] = jnp.sum(grad * normed, axis=0, keepdims=True)

    def norm_chunk(i, gain, jn, c, buf):
        cols = columns(c)
        wait_n(buf)
        for view in PAIR:
            at = pl.ds(view * view_rows, view_rows)
            first = sums_ref[i, view, :, cols]
            second = sums_ref[i, view, :, wide(c)]
            grad = invs[i, view, :, cols] * (gp[at, cols] - (first + normed_of(i, view, buf, cols) * second) * inv_rows)
            if gain is not None:
                grad = gains[gain, :, cols] * grad
            own[jn, at, cols] = grad.astype(jnp.bfloat16)
        swap(jn, c).start()

    half = width // 2
    strips = width // STRIP
    weights = (w1_hbm, w2_hbm, w3_hbm)
    w_slots = (xt, other, xt)
    hidden_out = (n1_hbm, n2_hbm, n3_hbm)

    def view_at(view):
        return pl.ds(view * view_rows, view_rows)

    def fetch_w(l, c):
        cols = columns(c, STRIP)
        return pltpu.make_async_copy(weights[l].at[:, :, cols], w_slots[l].at[:, :, cols], vsem.at[odd(l), c])

    def fetch_all(l, lo=0):
        @pl.loop(lo, strips)
        def _(c):
            fetch_w(l, c).start()

    load_a, load_b = load_h(own.at[0])
    load_a.start()
    fetch_w(0, 0).start()
    fetch_w(0, 1).start()

    @pl.loop(0, width // BLOCK)
    def _(r):
        lanes = pl.ds(pl.multiple_of(r * BLOCK, BLOCK), BLOCK)
        for n, (g_ref, s_ref) in enumerate(((g1_ref, s1_ref), (g2_ref, s2_ref))):
            gains[n, :, lanes] = g_ref[pl.ds(r, 1), :]
            shifts[n, :, lanes] = s_ref[pl.ds(r, 1), :]

    swaps = [exchange_pair(place, fsum.at[v, 0], fsum.at[v, 1], fparts.at[v], ftotal.at[v],
                           tuple(sem.at[v] for sem in (easend, earecv, ecsend, ecrecv)))
             for v in PAIR]
    load_b.start()
    fetch_all(0, 2)
    greet([partner] + place.chips)
    load_a.wait()

    def far(c, size):
        return pl.ds(pl.multiple_of(width + c * size, size), size)

    def hidden_copy(l, view, c):
        cols = columns(c, STRIP)
        return pltpu.make_async_copy(gp.at[view_at(view), cols], hidden_out[l].at[view_at(view), cols],
                                     usem.at[view, c])

    def products(l, view, actions):
        at = view_at(view)

        @pl.loop(0, strips)
        def _(c):
            for when, action in actions:
                pl.when(c == when)(action)
            if view == 0:
                fetch_w(l, c).wait()
            if l:
                hidden_copy(l - 1, view, c).wait()
            cols = columns(c, STRIP)
            value = jnp.dot(own[odd(l), at, pl.ds(0, half)], w_slots[l][0, :, cols],
                            preferred_element_type=jnp.float32)
            value += jnp.dot(own[odd(l), at, pl.ds(half, half)], w_slots[l][1, :, cols],
                             preferred_element_type=jnp.float32)
            gp[at, cols] = value
            fsum[view, 0, :, cols] = jnp.sum(value, axis=0, keepdims=True)
            fsum[view, 0, :, far(c, STRIP)] = jnp.sum(value * value, axis=0, keepdims=True)
            hidden_copy(l, view, c).start()

    def normalise(l, view, after=None):
        at = view_at(view)

        @pl.loop(0, chunks)
        def _(c):
            cols = columns(c)
            mean = ftotal[view, :, cols] * inv_rows
            square = ftotal[view, :, far(c, COLS)] * inv_rows
            inv = lax.rsqrt(square - mean * mean + NORM_EPS)
            means[2 - l, view, :, cols] = mean
            invs[2 - l, view, :, cols] = inv
            act = (gp[at, cols] - mean) * inv
            if l < 2:
                act = jnp.maximum(gains[l, :, cols] * act + shifts[l, :, cols], 0.0)
            act = act.astype(jnp.bfloat16)
            own[odd(l + 1), at, cols] = act
            if l == 0:
                xs[at, cols] = act
            if after is not None:
                after(c)

    a_swap, b_swap = swaps
    for l in AXES:
        products(l, 0, ((0, b_swap[1]),) if l else ())
        a_swap[0]()
        if l:
            b_swap[2]()
            normalise(l - 1, 1)
        else:
            fetch_all(1)
            load_b.wait()
        products(l, 1, ((0, a_swap[1]),))
        b_swap[0]()
        if l == 0:
            fetch_all(2)
        a_swap[2]()
        normalise(l, 0)

    lam = lam_ref[0, 0]
    a_rows, b_rows = view_at(0), view_at(1)
    last_cols = pl.ds(2 * width, COLS)
    for view in PAIR:
        psum[view, :, last_cols] = jnp.zeros((1, COLS), jnp.float32)
    for buf in PAIR:
        load_w(0, buf, buf)

    def z_swap(c):
        cols = columns(c)
        return remote(own.at[1, b_rows, cols], other.at[1, a_rows, cols], psend.at[1, c], precv.at[1, c], partner)

    z_turn = remote(xsend.at[:, a_rows], xt.at[1, :, b_rows], psend.at[1, chunks], precv.at[1, chunks], partner)
    b_swap[1]()
    turn(own.at[1], view_rows, z_turn, 1)
    b_swap[2]()
    normalise(2, 1, lambda c: z_swap(c).start())
    for view in PAIR:
        @pl.loop(0, strips)
        def _(c):
            hidden_copy(2, view, c).wait()
    for buf in PAIR:
        load_z(buf, buf)
    z_turn.wait_recv()

    def gather(step, t, phase, r):
        off, size = row_parts(BF16_SPLIT, phase)[r]
        picks = list(place.coord)
        for k in range(step):
            picks[(r + 2 - k) % 3] = slice(None)
        axis = (r + 2 - step) % 3
        ref = grads.at[(*picks, place.core, pl.ds(off, size), columns(t))]
        return remote(ref, ref, gsend.at[t, 3 * step + r], grecv.at[t, 3 * step + r], place.near[axis])

    def across(t):
        ref = grads.at[:, :, :, place.core, :, columns(t)]
        return remote(ref, ref, gsend.at[t, 9], grecv.at[t, 9], partner)

    def corr_block(t, phase):
        for r in AXES:
            off, size, val = ring.result(t, phase, r)
            corr = val * inv_rows
            row_id = place.me * BLOCK + off + lax.broadcasted_iota(jnp.int32, corr.shape, 0)
            col_id = t * COLS + lax.broadcasted_iota(jnp.int32, corr.shape, 1)
            diag = row_id == col_id
            gap = 1.0 - corr
            terms = jnp.where(diag, gap * gap, lam * corr * corr)
            psum[0, :, last_cols] += jnp.sum(terms, axis=0, keepdims=True)
            stage[pl.ds(off, size), :] = jnp.where(diag, -2.0 * gap, 2.0 * lam * corr) * inv_rows
        grads[(*place.coord, place.core, slice(None), columns(t))] = stage[...].astype(jnp.bfloat16)
        for r in AXES:
            gather(0, t, phase, r).start()

    def embed_chunk(c):
        cols = columns(c)
        buf = lax.rem(c, 2)
        block = grads[:, :, :, :, :, cols].reshape(width, COLS)
        grad = jnp.dot(own[1, a_rows, :], block, preferred_element_type=jnp.float32)
        gp[b_rows, cols] = grad
        wait_n(buf)
        psum[1, :, cols] = jnp.sum(grad, axis=0, keepdims=True)
        psum[1, :, wide(c)] = jnp.sum(grad * normed_of(0, 1, buf, cols), axis=0, keepdims=True)
        load_z(lax.rem(c + 2, chunks), buf)

        @pl.loop(0, chunks // 2)
        def _(k):
            rows_g = grads[k // 2, lax.rem(k, 2), :, :, :, cols].reshape(512, COLS)
            more = lax.dot_general(own[1, b_rows, cols], rows_g, LAST_DIMS, preferred_element_type=jnp.float32)
            at_k = columns(k, 512)
            gp[a_rows, at_k] = jnp.where(c > 0, gp[a_rows, at_k], 0.0) + more

            @pl.when(c == chunks - 1)
            def _():
                for buf_k in PAIR:
                    sub = 2 * k + buf_k
                    at_sub = columns(sub)
                    total = gp[a_rows, at_sub]
                    wait_n(buf_k)
                    psum[0, :, at_sub] = jnp.sum(total, axis=0, keepdims=True)
                    psum[0, :, wide(sub)] = jnp.sum(total * normed_of(0, 0, buf_k, at_sub), axis=0, keepdims=True)
                    load_z(lax.rem(sub + 2, chunks), buf_k)

    @pl.loop(0, chunks + 7)
    def _(t):
        phase = lax.rem(t, 3)

        @pl.when(t < chunks)
        def _():
            for s in AXES:
                @pl.when((phase == s) & (t >= RING))
                def _():
                    ring.wait_sends(t - RING, s - RING)
            z_swap(t).wait_recv()
            cols = columns(t)
            for half in PAIR:
                feats = pl.ds(512 * half, 512)
                part = jnp.dot(xt[1, feats, a_rows], own[1, b_rows, cols], preferred_element_type=jnp.float32)
                part += jnp.dot(xt[1, feats, b_rows], other[1, a_rows, cols], preferred_element_type=jnp.float32)
                acc[lax.rem(t, RING), half] = part.reshape(2, 2, BLOCK, COLS)

        for s in AXES:
            @pl.when(phase == s)
            def _():
                @pl.when(t < chunks)
                def _():
                    ring.send(0, t, s)

                for step in PAIR:
                    u = t - 1 - step

                    @pl.when((u >= 0) & (u < chunks))
                    def _():
                        ring.add(step, u, s - 1 - step)
                        ring.send(step + 1, u, s - 1 - step)

                @pl.when((t >= 3) & (t < chunks + 3))
                def _():
                    corr_block(t - 3, s - 3)

                for step in PAIR:
                    v = t - 4 - step

                    @pl.when((v >= 0) & (v < chunks))
                    def _():
                        for r in AXES:
                            gather(step, v, s - 4 - step, r).wait_recv()
                            gather(step + 1, v, s - 4 - step, r).start()

                @pl.when((t >= 6) & (t < chunks + 6))
                def _():
                    for r in AXES:
                        gather(2, t - 6, s - 6, r).wait_recv()
                    across(t - 6).start()

        @pl.when(t == 1)
        def _():
            z_turn.wait_send()
            turn_x(own.at[0], 0)

        @pl.when(t >= 7)
        def _():
            c = t - 7
            across(c).wait_recv()
            embed_chunk(c)

    start, chips, finish, close = sums_of(0)
    start()
    chips()
    for t in range(chunks - RING, chunks):
        ring.wait_sends(t, t)
    for t in range(chunks):
        across(t).wait_send()
        z_swap(t).wait_send()
        for step in AXES:
            for r in AXES:
                gather(step, t, t, r).wait_send()
    finish()
    close()
    loss_ref[...] = jnp.sum(sums_ref[0, 0, :, last_cols], axis=1, keepdims=True) + jnp.zeros((1, BLOCK), jnp.float32)

    def norm_pairs(lo, hi):
        @pl.loop(lo, hi)
        def _(pair):
            for buf in PAIR:
                c = 2 * pair + buf
                norm_chunk(0, None, 0, c, buf)

                @pl.when(c < chunks - 2)
                def _():
                    load_z(c + 2, buf)

    norm_pairs(0, 1)

    def layer_norms(j, jn, lo):
        @pl.loop(lo, lo + 2)
        def _(pair):
            for buf in PAIR:
                c = 2 * pair + buf
                norm_chunk(j + 1, 1 - j, jn, c, buf)

                @pl.when(c < chunks - 2)
                def _():
                    load_n(j, c + 2, buf)

    @pl.loop(0, jobs * chunks + 3)
    def _(t):
        j = t // chunks
        n = lax.rem(t, chunks)
        jb = lax.rem(j, 2)
        jn = 1 - jb
        phase = lax.rem(t, 3)

        @pl.when(t < jobs * chunks)
        def _():
            for s in AXES:
                @pl.when((phase == s) & (t >= RING))
                def _():
                    ring.wait_sends(t - RING, s - RING)

            @pl.when(n == 0)
            def _():
                x_swap(jb).wait_recv()
            swap(jb, n).wait_recv()
            cols = columns(n)
            slot = lax.rem(t, RING)
            for half in PAIR:
                feats = pl.ds(512 * half, 512)
                part = jnp.dot(xt[jb, feats, pl.ds(0, rows)], own[jb, :, cols], preferred_element_type=jnp.float32)
                part += jnp.dot(xt[jb, feats, pl.ds(rows, rows)], other[jb, :, cols],
                                preferred_element_type=jnp.float32)
                acc[slot, half] = part.reshape(2, 2, BLOCK, COLS)

        for s in AXES:
            @pl.when(phase == s)
            def _():
                @pl.when(t < jobs * chunks)
                def _():
                    ring.send(0, t, s)

                for step in PAIR:
                    u = t - 1 - step

                    @pl.when((u >= 0) & (u < jobs * chunks))
                    def _():
                        ring.add(step, u, s - 1 - step)
                        ring.send(step + 1, u, s - 1 - step)

                @pl.when(t >= 3)
                def _():
                    u = t - 3
                    for r in AXES:
                        off, size, val = ring.result(u, s - 3, r)
                        out_ref[u // chunks, pl.ds(off, size), columns(lax.rem(u, chunks))] = val

        @pl.when(t == 0)
        def _():
            norm_pairs(1, chunks // 2)
            for buf in PAIR:
                load_n(0, buf, buf)

        @pl.when((n == 0) & (j > 0) & (j < jobs))
        def _():
            layer_norms(j - 1, jb, 2)

            @pl.when(j == 1)
            def _():
                for buf in PAIR:
                    load_n(1, buf, buf)

        @pl.when(j < jobs - 1)
        def _():
            start, chips, finish, close = sums_of(j + 1)

            @pl.when((n > 0) & (n < 5))
            def _():
                layer_pair(j, jb, n - 1)
                for buf in PAIR:
                    c = 2 * n - 2 + buf

                    @pl.when(n < 4)
                    def _():
                        load_w(j, c + 2, buf)
                        load_n(j, c + 2, buf)

                    @pl.when(n == 4)
                    def _():
                        load_n(j, buf, buf)

            @pl.when(n == 4)
            def _():
                start()

                @pl.when(j == 1)
                def _():
                    for load in load_h(xs):
                        load.start()

            @pl.when(n == 5)
            def _():
                chips()

                @pl.when(j == 1)
                def _():
                    for load in load_h(xs):
                        load.wait()
                x_swap(jb).wait_send()
                turn_x(xs, jn)

            @pl.when(n == 6)
            def _():
                finish()

            @pl.when(n == 7)
            def _():
                close()
                vec_ref[j] = sums_ref[j + 1, 0, :, pl.ds(0, 2 * width)] + sums_ref[j + 1, 1, :, pl.ds(0, 2 * width)]

                @pl.loop(0, chunks)
                def _(c):
                    swap(jb, c).wait_send()

            @pl.when(n == 7)
            def _():
                layer_norms(j, jn, 0)

                @pl.when(j == 0)
                def _():
                    for buf in PAIR:
                        load_w(1, buf, buf)

    for t in range(jobs * chunks - RING, jobs * chunks):
        ring.wait_sends(t, t)

    @pl.loop(0, chunks)
    def _(c):
        swap(0, c).wait_send()
    x_swap(0).wait_send()


VM = pl.BlockSpec(memory_space=pltpu.VMEM)


def whole_step(lam, vectors, h_a, h_b, weights, total_rows):
    view_rows, width = h_a.shape
    rows = 2 * view_rows
    chunks = width // COLS
    hbm = pl.BlockSpec(memory_space=pltpu.HBM)
    bf16, f32 = jnp.bfloat16, jnp.float32
    dma = pltpu.SemaphoreType.DMA
    wide = 2 * width + COLS
    return pl.pallas_call(
        functools.partial(whole_kernel, 1.0 / total_rows),
        out_shape=(jax.ShapeDtypeStruct((3, BLOCK, width), f32), jax.ShapeDtypeStruct((2, 1, 2 * width), f32),
                   jax.ShapeDtypeStruct((1, BLOCK), f32)) + (jax.ShapeDtypeStruct((rows, width), f32),) * 3,
        in_specs=[pl.BlockSpec(memory_space=pltpu.SMEM)] + [VM] * 4 + [hbm] * 5, out_specs=(VM,) * 3 + (hbm,) * 3,
        scratch_shapes=[
            pltpu.VMEM((2, width // 2, 2 * rows), bf16),
            pltpu.VMEM((width // 2, rows), bf16),
            pltpu.VMEM((rows, width), bf16),
            pltpu.VMEM((2, rows, width), bf16),
            pltpu.VMEM((2, rows, width), bf16),
            pltpu.VMEM((RING, 2, 2, 2, BLOCK, COLS), f32),
            pltpu.VMEM((RING, 2, 2, BLOCK, COLS), f32),
            pltpu.VMEM((RING, 2, BLOCK, COLS), f32),
            pltpu.VMEM((RING, BLOCK, COLS), f32),
            pltpu.VMEM((rows, width), f32),
            pltpu.VMEM((2, COLS, width), bf16),
            pltpu.VMEM((2, rows, COLS), f32),
            pltpu.VMEM((3, 1, wide), f32),
            pltpu.VMEM((8, 1, wide), f32),
            pltpu.VMEM((3, 2, 1, wide), f32),
            pltpu.VMEM((2, 2, 2, 2, BLOCK, width), bf16),
            pltpu.VMEM((BLOCK, COLS), f32),
            pltpu.VMEM((2, 1, width), f32),
            pltpu.VMEM((2, 1, width), f32),
            pltpu.VMEM((3, 2, 1, width), f32),
            pltpu.VMEM((3, 2, 1, width), f32),
            pltpu.VMEM((2, 2, 1, 2 * width), f32),
            pltpu.VMEM((2, 8, 1, 2 * width), f32),
            pltpu.VMEM((2, 1, 2 * width), f32),
            dma((RING, 9)), dma((RING, 9)), dma((2, chunks + 1)), dma((2, chunks + 1)),
            dma, dma, dma((7,)), dma((7,)), dma, dma, dma((2,)), dma((2,)), dma((2,)),
            dma((chunks, 10)), dma((chunks, 10)),
            dma((2, width // STRIP)), dma((2, width // STRIP)),
            dma((2,)), dma((2,)), dma((2, 7)), dma((2, 7)),
        ],
        compiler_params=pltpu.CompilerParams(collective_id=1, has_side_effects=True, vmem_limit_bytes=67043328),
        name="whole_step",
    )(lam.reshape(1, 1), *(v.reshape(width // BLOCK, BLOCK) for v in vectors), h_a, h_b,
      *(w.reshape(2, width // 2, width) for w in weights))


def solution(mesh):
    shards = mesh.shape["data"]

    def local_step(h_a, h_b, w_one, w_two, w_three, gain_one, shift_one, gain_two, shift_two, lam_off):
        rows_dev, width = h_a.shape
        total_rows = rows_dev * shards
        weights, vectors, loss = whole_step(lam_off, (gain_one, shift_one, gain_two, shift_two), h_a, h_b,
                                            (w_one, w_two, w_three), total_rows)[:3]
        return (loss[0, 0], weights[2], weights[1], weights[0],
                vectors[1, 0, width:], vectors[1, 0, :width], vectors[0, 0, width:], vectors[0, 0, :width])

    row_spec = P("data", None)
    whole_mat = P(None, None)
    whole_vec = P(None)
    return jax.shard_map(
        local_step, mesh=mesh,
        in_specs=(row_spec, row_spec, whole_mat, whole_mat, whole_mat,
                  whole_vec, whole_vec, whole_vec, whole_vec, P()),
        out_specs=(P(), row_spec, row_spec, row_spec, whole_vec, whole_vec, whole_vec, whole_vec),
        check_vma=False)
```

```python
import functools

import jax
import jax.numpy as jnp
from jax import lax
from jax.experimental import pallas as pl
from jax.experimental.pallas import tpu as pltpu
from jax.sharding import PartitionSpec as P

NORM_EPS = 1e-5
MESH = pl.DeviceIdType.MESH
RING = 4
COLS = 256
STRIP = 1024
BLOCK = 128
PAIR = range(2)
AXES = range(3)
F32_SPLIT = ((48, 40, 40), (40, 48, 40), (40, 40, 48))
BF16_SPLIT = ((48, 48, 32), (32, 48, 48), (48, 32, 48))


LAST_DIMS = (((1,), (1,)), ((), ()))


def odd(n):
    return n % 2


class Place:
    def __init__(self):
        self.me = lax.axis_index("data")
        self.core = lax.rem(self.me, 2)
        self.chip = self.me // 2
        self.coord = (self.chip // 4, lax.rem(self.chip // 2, 2), lax.rem(self.chip, 2))
        self.partner = self.me + 1 - 2 * self.core
        steps = [(1 - 2 * c) * w for c, w in zip(self.coord, (8, 4, 2))]
        self.near = tuple(self.me + step for step in steps)
        self.chips = [self.me + sum(steps[a] for a in flips)
                      for flips in ((0, 1, 2), (0, 1), (0, 2), (1, 2), (0,), (1,), (2,))]


def greet(peers):
    barrier = pltpu.get_barrier_semaphore()
    for peer in peers:
        pl.semaphore_signal(barrier, inc=1, device_id=(peer,), device_id_type=MESH)
    pl.semaphore_wait(barrier, len(peers))


def remote(src, dst, send, recv, peer):
    return pltpu.make_async_remote_copy(src_ref=src, dst_ref=dst, send_sem=send, recv_sem=recv,
                                        device_id=(peer,), device_id_type=MESH)


def row_parts(split, phase):
    sizes = split[phase % 3]
    return tuple((sum(sizes[:r]), sizes[r]) for r in AXES)


class HalvingReduce:
    def __init__(self, place, acc, bufs, ssem, rsem):
        self.place, self.acc, self.bufs, self.ssem, self.rsem = place, acc, bufs, ssem, rsem

    def at(self, t, picks):
        return (lax.rem(t, RING),) + tuple(picks)

    def copy(self, step, t, phase, r):
        slot = lax.rem(t, RING)
        off, size = row_parts(F32_SPLIT, phase)[r]
        rows = pl.ds(off, size)
        picks = [slice(None)] * 3
        for k in range(step):
            axis = (r + k) % 3
            picks[axis] = self.place.coord[axis]
        axis = (r + step) % 3
        picks[axis] = 1 - self.place.coord[axis]
        src = self.acc.at[(slot, *picks, rows, slice(None))]
        dst = self.bufs[step].at[(slot,) + (slice(None),) * (2 - step) + (rows, slice(None))]
        return remote(src, dst, self.ssem.at[slot, 3 * step + r], self.rsem.at[slot, 3 * step + r],
                      self.place.near[axis])

    def send(self, step, t, phase):
        for r in AXES:
            self.copy(step, t, phase, r).start()

    def wait_sends(self, t, phase):
        for step in AXES:
            for r in AXES:
                self.copy(step, t, phase, r).wait_send()

    def add(self, step, t, phase):
        slot = lax.rem(t, RING)
        for r in AXES:
            self.copy(step, t, phase, r).wait_recv()
            off, size = row_parts(F32_SPLIT, phase)[r]
            rows = pl.ds(off, size)
            fixed = {(r + k) % 3 for k in range(step + 1)}
            free = [a for a in range(3) if a not in fixed]
            for n in range(2 ** len(free)):
                picks = list(self.place.coord)
                sub = []
                for pos, a in enumerate(free):
                    bit = (n >> (len(free) - 1 - pos)) & 1
                    picks[a] = bit
                    sub.append(bit)
                where = (slot, *picks, rows, slice(None))
                self.acc[where] = self.acc[where] + self.bufs[step][(slot, *sub, rows, slice(None))]

    def result(self, t, phase, r):
        slot = lax.rem(t, RING)
        self.copy(2, t, phase, r).wait_recv()
        off, size = row_parts(F32_SPLIT, phase)[r]
        rows = pl.ds(off, size)
        return off, size, (self.acc[(slot, *self.place.coord, rows, slice(None))]
                           + self.bufs[2][(slot, rows, slice(None))])


def columns(t, width=COLS):
    return pl.ds(pl.multiple_of(t * width, width), width)


def exchange_parts(place, psum, parts, total, sems):
    asend, arecv, csend, crecv, fsend, frecv = sems
    other = 1 - place.core
    land = psum.at[2]
    first = remote(psum.at[other], land, asend, arecv, place.partner)
    mine = parts.at[place.chip]
    across = [remote(mine, mine, csend.at[n], crecv.at[n], peer) for n, peer in enumerate(place.chips)]
    last = remote(total.at[place.core], total.at[place.core], fsend, frecv, place.partner)

    def start():
        first.start()

    def chips():
        first.wait_recv()
        parts[place.chip] = psum[place.core] + psum[2]
        for copy in across:
            copy.start()

    def finish():
        for copy in across:
            copy.wait_recv()
        value = parts[0]
        for c in range(1, 8):
            value = value + parts[c]
        total[place.core] = value
        last.start()

    def close():
        last.wait_recv()
        first.wait_send()
        for copy in across:
            copy.wait_send()
        last.wait_send()

    return start, chips, finish, close


def exchange_pair(place, own, land, parts, total, sems):
    asend, arecv, csend, crecv = sems
    first = remote(own, land, asend, arecv, place.partner)
    mine = parts.at[place.chip]
    across = [remote(mine, mine, csend.at[n], crecv.at[n], peer) for n, peer in enumerate(place.chips)]

    def chips():
        first.wait_recv()
        parts[place.chip] = own[...] + land[...]
        for copy in across:
            copy.start()

    def finish():
        first.wait_send()
        for copy in across:
            copy.wait()
        value = parts[0]
        for c in range(1, 8):
            value = value + parts[c]
        total[...] = value

    return first.start, chips, finish


def whole_kernel(inv_rows, lam_ref, g1_ref, s1_ref, g2_ref, s2_ref, ha_hbm, hb_hbm, w1_hbm, w2_hbm, w3_hbm,
                 out_ref, vec_ref, loss_ref, n1_hbm, n2_hbm, n3_hbm,
                 xt, xsend, xs, own, other, acc, b0, b1, b2, gp, wbuf, nbuf, psum, parts, sums_ref, grads, stage,
                 done, gains, shifts, means, invs, fsum, fparts, ftotal,
                 ssem, rsem, psend, precv, asend, arecv, csend, crecv, fsend, frecv, lsem, wsem, nsem, gsend, grecv,
                 usem, vsem, easend, earecv, ecsend, ecrecv, dsem):
    place = Place()
    view_rows, width = ha_hbm.shape
    rows = 2 * view_rows
    chunks = width // COLS
    jobs = 3
    partner = place.partner
    ring = HalvingReduce(place, acc, (b0, b1, b2), ssem, rsem)

    def load_w(j, c, buf):
        rows_c = columns(lax.rem(c, chunks // 2))
        for k, ref in enumerate((w3_hbm, w2_hbm)):
            @pl.when(j == k)
            def _():
                pltpu.make_async_copy(ref.at[c // (chunks // 2), rows_c, :], wbuf.at[buf], wsem.at[buf]).start()

    def load_z(c, buf):
        pltpu.make_async_copy(n3_hbm.at[:, columns(c)], nbuf.at[buf], nsem.at[buf]).start()

    def load_n(j, c, buf):
        for k, ref in enumerate((n2_hbm, n1_hbm)):
            @pl.when(j == k)
            def _():
                pltpu.make_async_copy(ref.at[:, columns(c)], nbuf.at[buf], nsem.at[buf]).start()

    def wait_w(buf):
        pltpu.make_async_copy(w3_hbm.at[0, pl.ds(0, COLS), :], wbuf.at[buf], wsem.at[buf]).wait()

    def wait_n(buf):
        pltpu.make_async_copy(n2_hbm.at[:, pl.ds(0, COLS)], nbuf.at[buf], nsem.at[buf]).wait()

    def swap(jb, c):
        cols = columns(c)
        return remote(own.at[jb, :, cols], other.at[jb, :, cols], psend.at[jb, c], precv.at[jb, c], partner)

    def x_swap(jb):
        return remote(xsend, xt.at[jb, :, pl.ds(rows, rows)], psend.at[jb, chunks], precv.at[jb, chunks], partner)

    def load_h(dst):
        return [pltpu.make_async_copy(ref, dst.at[pl.ds(view * view_rows, view_rows), :], lsem.at[view])
                for view, ref in enumerate((ha_hbm, hb_hbm))]

    def turn(src, depth, copy, jb):
        def blocks(dst, parity):
            @pl.loop(0, 8)
            def _(b):
                to = pl.ds(pl.multiple_of(b * BLOCK, BLOCK), BLOCK)
                cols = pl.ds(pl.multiple_of((2 * b + parity) * BLOCK, BLOCK), BLOCK)
                dst[to, pl.ds(0, depth)] = src[pl.ds(0, depth), cols].T

        blocks(xsend, 1 - place.core)
        copy.start()
        blocks(xt.at[jb], place.core)

    def turn_x(src, jb):
        turn(src, rows, x_swap(jb), jb)

    def sums_of(i):
        return exchange_parts(place, psum, parts, sums_ref.at[i], (asend, arecv, csend, crecv, fsend, frecv))

    def wide(c):
        return pl.ds(pl.multiple_of(width + c * COLS, COLS), COLS)

    def normed_of(i, view, buf, cols):
        at = pl.ds(view * view_rows, view_rows)
        return (nbuf[buf, at, :] - means[i, view, :, cols]) * invs[i, view, :, cols]

    def layer_pair(j, jb, n):
        for buf in PAIR:
            wait_w(buf)
            wait_n(buf)
        for view in PAIR:
            at = pl.ds(view * view_rows, view_rows)
            both = lax.dot_general(own[jb, at, :], wbuf[...].reshape(2 * COLS, width), LAST_DIMS,
                                   preferred_element_type=jnp.float32)
            for buf in PAIR:
                c = 2 * n + buf
                cols = columns(c)
                normed = normed_of(j + 1, view, buf, cols)
                grad = jnp.where(gains[1 - j, :, cols] * normed + shifts[1 - j, :, cols] > 0,
                                 both[:, buf * COLS:(buf + 1) * COLS], 0.0)
                gp[at, cols] = grad
                psum[view, :, cols] = jnp.sum(grad, axis=0, keepdims=True)
                psum[view, :, wide(c)] = jnp.sum(grad * normed, axis=0, keepdims=True)

    def norm_chunk(i, gain, jn, c, buf):
        cols = columns(c)
        wait_n(buf)
        for view in PAIR:
            at = pl.ds(view * view_rows, view_rows)
            first = sums_ref[i, view, :, cols]
            second = sums_ref[i, view, :, wide(c)]
            grad = invs[i, view, :, cols] * (gp[at, cols] - (first + normed_of(i, view, buf, cols) * second) * inv_rows)
            if gain is not None:
                grad = gains[gain, :, cols] * grad
            own[jn, at, cols] = grad.astype(jnp.bfloat16)
        swap(jn, c).start()

    half = width // 2
    strips = width // STRIP
    weights = (w1_hbm, w2_hbm, w3_hbm)
    w_slots = (xt, other, xt)
    hidden_out = (n1_hbm, n2_hbm, n3_hbm)

    def view_at(view):
        return pl.ds(view * view_rows, view_rows)

    def fetch_w(l, c):
        cols = columns(c, STRIP)
        return pltpu.make_async_copy(weights[l].at[:, :, cols], w_slots[l].at[:, :, cols], vsem.at[odd(l), c])

    def fetch_all(l, lo=0):
        @pl.loop(lo, strips)
        def _(c):
            fetch_w(l, c).start()

    load_a, load_b = load_h(own.at[0])
    load_a.start()
    fetch_w(0, 0).start()
    fetch_w(0, 1).start()

    @pl.loop(0, width // BLOCK)
    def _(r):
        lanes = pl.ds(pl.multiple_of(r * BLOCK, BLOCK), BLOCK)
        for n, (g_ref, s_ref) in enumerate(((g1_ref, s1_ref), (g2_ref, s2_ref))):
            gains[n, :, lanes] = g_ref[pl.ds(r, 1), :]
            shifts[n, :, lanes] = s_ref[pl.ds(r, 1), :]

    swaps = [exchange_pair(place, fsum.at[v, 0], fsum.at[v, 1], fparts.at[v], ftotal.at[v],
                           tuple(sem.at[v] for sem in (easend, earecv, ecsend, ecrecv)))
             for v in PAIR]
    load_b.start()
    fetch_all(0, 2)
    greet([partner] + place.chips)
    load_a.wait()

    def far(c, size):
        return pl.ds(pl.multiple_of(width + c * size, size), size)

    def hidden_copy(l, view, c):
        cols = columns(c, STRIP)
        return pltpu.make_async_copy(gp.at[view_at(view), cols], hidden_out[l].at[view_at(view), cols],
                                     usem.at[view, c])

    def products(l, view, actions):
        at = view_at(view)

        @pl.loop(0, strips)
        def _(c):
            for when, action in actions:
                pl.when(c == when)(action)
            if view == 0:
                fetch_w(l, c).wait()
            if l:
                hidden_copy(l - 1, view, c).wait()
            cols = columns(c, STRIP)
            value = jnp.dot(own[odd(l), at, pl.ds(0, half)], w_slots[l][0, :, cols],
                            preferred_element_type=jnp.float32)
            value += jnp.dot(own[odd(l), at, pl.ds(half, half)], w_slots[l][1, :, cols],
                             preferred_element_type=jnp.float32)
            gp[at, cols] = value
            fsum[view, 0, :, cols] = jnp.sum(value, axis=0, keepdims=True)
            fsum[view, 0, :, far(c, STRIP)] = jnp.sum(value * value, axis=0, keepdims=True)
            hidden_copy(l, view, c).start()

    def normalise(l, view, after=None):
        at = view_at(view)

        @pl.loop(0, chunks)
        def _(c):
            cols = columns(c)
            mean = ftotal[view, :, cols] * inv_rows
            square = ftotal[view, :, far(c, COLS)] * inv_rows
            inv = lax.rsqrt(square - mean * mean + NORM_EPS)
            means[2 - l, view, :, cols] = mean
            invs[2 - l, view, :, cols] = inv
            act = (gp[at, cols] - mean) * inv
            if l < 2:
                act = jnp.maximum(gains[l, :, cols] * act + shifts[l, :, cols], 0.0)
            act = act.astype(jnp.bfloat16)
            own[odd(l + 1), at, cols] = act
            if l == 0:
                xs[at, cols] = act
            if after is not None:
                after(c)

    a_swap, b_swap = swaps
    for l in AXES:
        products(l, 0, ((0, b_swap[1]),) if l else ())
        a_swap[0]()
        if l:
            b_swap[2]()
            normalise(l - 1, 1)
        else:
            fetch_all(1)
            load_b.wait()
        products(l, 1, ((0, a_swap[1]),))
        b_swap[0]()
        if l == 0:
            fetch_all(2)
        a_swap[2]()
        normalise(l, 0)

    lam = lam_ref[0, 0]
    a_rows, b_rows = view_at(0), view_at(1)
    last_cols = pl.ds(2 * width, COLS)
    for view in PAIR:
        psum[view, :, last_cols] = jnp.zeros((1, COLS), jnp.float32)
    for buf in PAIR:
        load_w(0, buf, buf)

    def z_swap(c):
        cols = columns(c)
        return remote(own.at[1, b_rows, cols], other.at[1, a_rows, cols], psend.at[1, c], precv.at[1, c], partner)

    z_turn = remote(xsend.at[:, a_rows], xt.at[1, :, b_rows], psend.at[1, chunks], precv.at[1, chunks], partner)
    b_swap[1]()
    turn(own.at[1], view_rows, z_turn, 1)
    b_swap[2]()
    normalise(2, 1, lambda c: z_swap(c).start())
    for view in PAIR:
        @pl.loop(0, strips)
        def _(c):
            hidden_copy(2, view, c).wait()
    for buf in PAIR:
        load_z(buf, buf)
    z_turn.wait_recv()

    def gather(step, t, phase, r):
        off, size = row_parts(BF16_SPLIT, phase)[r]
        picks = list(place.coord)
        for k in range(step):
            picks[(r + 2 - k) % 3] = slice(None)
        axis = (r + 2 - step) % 3
        ref = grads.at[(*picks, place.core, pl.ds(off, size), columns(t))]
        return remote(ref, ref, gsend.at[t, 3 * step + r], grecv.at[t, 3 * step + r], place.near[axis])

    def across(t):
        ref = grads.at[:, :, :, place.core, :, columns(t)]
        return remote(ref, ref, gsend.at[t, 9], grecv.at[t, 9], partner)

    def corr_block(t, phase):
        for r in AXES:
            off, size, val = ring.result(t, phase, r)
            corr = val * inv_rows
            row_id = place.me * BLOCK + off + lax.broadcasted_iota(jnp.int32, corr.shape, 0)
            col_id = t * COLS + lax.broadcasted_iota(jnp.int32, corr.shape, 1)
            diag = row_id == col_id
            gap = 1.0 - corr
            terms = jnp.where(diag, gap * gap, lam * corr * corr)
            psum[0, :, last_cols] += jnp.sum(terms, axis=0, keepdims=True)
            stage[pl.ds(off, size), :] = jnp.where(diag, -2.0 * gap, 2.0 * lam * corr) * inv_rows
        grads[(*place.coord, place.core, slice(None), columns(t))] = stage[...].astype(jnp.bfloat16)
        for r in AXES:
            gather(0, t, phase, r).start()

    def embed_chunk(c):
        cols = columns(c)
        buf = lax.rem(c, 2)
        block = grads[:, :, :, :, :, cols].reshape(width, COLS)
        grad = jnp.dot(own[1, a_rows, :], block, preferred_element_type=jnp.float32)
        gp[b_rows, cols] = grad
        wait_n(buf)
        psum[1, :, cols] = jnp.sum(grad, axis=0, keepdims=True)
        psum[1, :, wide(c)] = jnp.sum(grad * normed_of(0, 1, buf, cols), axis=0, keepdims=True)
        load_z(lax.rem(c + 2, chunks), buf)

        @pl.loop(0, 2)
        def _(k):
            rows_g = grads[k, :, :, :, :, cols].reshape(1024, COLS)
            more = lax.dot_general(own[1, b_rows, cols], rows_g, LAST_DIMS, preferred_element_type=jnp.float32)
            at_k = columns(k, 1024)
            gp[a_rows, at_k] = jnp.where(c > 0, gp[a_rows, at_k], 0.0) + more

            @pl.when(c == chunks - 1)
            def _():
                for q in range(4):
                    buf_k = q % 2
                    sub = 4 * k + q
                    at_sub = columns(sub)
                    total = gp[a_rows, at_sub]
                    wait_n(buf_k)
                    psum[0, :, at_sub] = jnp.sum(total, axis=0, keepdims=True)
                    psum[0, :, wide(sub)] = jnp.sum(total * normed_of(0, 0, buf_k, at_sub), axis=0, keepdims=True)
                    load_z(lax.rem(sub + 2, chunks), buf_k)

    @pl.loop(0, chunks + 7)
    def _(t):
        phase = lax.rem(t, 3)

        @pl.when(t < chunks)
        def _():
            for s in AXES:
                @pl.when((phase == s) & (t >= RING))
                def _():
                    ring.wait_sends(t - RING, s - RING)
            z_swap(t).wait_recv()
            cols = columns(t)
            for half in PAIR:
                feats = pl.ds(512 * half, 512)
                part = jnp.dot(xt[1, feats, a_rows], own[1, b_rows, cols], preferred_element_type=jnp.float32)
                part += jnp.dot(xt[1, feats, b_rows], other[1, a_rows, cols], preferred_element_type=jnp.float32)
                acc[lax.rem(t, RING), half] = part.reshape(2, 2, BLOCK, COLS)

        for s in AXES:
            @pl.when(phase == s)
            def _():
                @pl.when(t < chunks)
                def _():
                    ring.send(0, t, s)

                for step in PAIR:
                    u = t - 1 - step

                    @pl.when((u >= 0) & (u < chunks))
                    def _():
                        ring.add(step, u, s - 1 - step)
                        ring.send(step + 1, u, s - 1 - step)

                @pl.when((t >= 3) & (t < chunks + 3))
                def _():
                    corr_block(t - 3, s - 3)

                for step in PAIR:
                    v = t - 4 - step

                    @pl.when((v >= 0) & (v < chunks))
                    def _():
                        for r in AXES:
                            gather(step, v, s - 4 - step, r).wait_recv()
                            gather(step + 1, v, s - 4 - step, r).start()

                @pl.when((t >= 6) & (t < chunks + 6))
                def _():
                    for r in AXES:
                        gather(2, t - 6, s - 6, r).wait_recv()
                    across(t - 6).start()

        @pl.when(t == 1)
        def _():
            z_turn.wait_send()
            turn_x(own.at[0], 0)

        @pl.when(t >= 7)
        def _():
            c = t - 7
            across(c).wait_recv()
            embed_chunk(c)

    start, chips, finish, close = sums_of(0)
    start()
    chips()
    for t in range(chunks - RING, chunks):
        ring.wait_sends(t, t)
    for t in range(chunks):
        across(t).wait_send()
        z_swap(t).wait_send()
        for step in AXES:
            for r in AXES:
                gather(step, t, t, r).wait_send()
    finish()
    close()
    loss_ref[...] = jnp.sum(sums_ref[0, 0, :, last_cols], axis=1, keepdims=True) + jnp.zeros((1, BLOCK), jnp.float32)

    def norm_pairs(lo, hi):
        @pl.loop(lo, hi)
        def _(pair):
            for buf in PAIR:
                c = 2 * pair + buf
                norm_chunk(0, None, 0, c, buf)

                @pl.when(c < chunks - 2)
                def _():
                    load_z(c + 2, buf)

    norm_pairs(0, 1)

    def result_copy(u):
        return pltpu.make_async_copy(done.at[lax.rem(u, 2)], out_ref.at[u // chunks, :, columns(lax.rem(u, chunks))],
                                     dsem.at[lax.rem(u, 2)])

    def layer_norms(j, jn, lo):
        @pl.loop(lo, lo + 2)
        def _(pair):
            for buf in PAIR:
                c = 2 * pair + buf
                norm_chunk(j + 1, 1 - j, jn, c, buf)

                @pl.when(c < chunks - 2)
                def _():
                    load_n(j, c + 2, buf)

    @pl.loop(0, jobs * chunks + 3)
    def _(t):
        j = t // chunks
        n = lax.rem(t, chunks)
        jb = lax.rem(j, 2)
        jn = 1 - jb
        phase = lax.rem(t, 3)

        @pl.when(t < jobs * chunks)
        def _():
            for s in AXES:
                @pl.when((phase == s) & (t >= RING))
                def _():
                    ring.wait_sends(t - RING, s - RING)

            @pl.when(n == 0)
            def _():
                x_swap(jb).wait_recv()
            swap(jb, n).wait_recv()
            cols = columns(n)
            slot = lax.rem(t, RING)
            for half in PAIR:
                feats = pl.ds(512 * half, 512)
                part = jnp.dot(xt[jb, feats, pl.ds(0, rows)], own[jb, :, cols], preferred_element_type=jnp.float32)
                part += jnp.dot(xt[jb, feats, pl.ds(rows, rows)], other[jb, :, cols],
                                preferred_element_type=jnp.float32)
                acc[slot, half] = part.reshape(2, 2, BLOCK, COLS)

        for s in AXES:
            @pl.when(phase == s)
            def _():
                @pl.when(t < jobs * chunks)
                def _():
                    ring.send(0, t, s)

                for step in PAIR:
                    u = t - 1 - step

                    @pl.when((u >= 0) & (u < jobs * chunks))
                    def _():
                        ring.add(step, u, s - 1 - step)
                        ring.send(step + 1, u, s - 1 - step)

                @pl.when(t >= 3)
                def _():
                    u = t - 3
                    pl.when(t >= 5)(result_copy(u).wait)
                    for r in AXES:
                        off, size, val = ring.result(u, s - 3, r)
                        done[lax.rem(u, 2), pl.ds(off, size), :] = val
                    result_copy(u).start()

        @pl.when(t == 0)
        def _():
            norm_pairs(1, chunks // 2)
            for buf in PAIR:
                load_n(0, buf, buf)

        @pl.when((n == 0) & (j > 0) & (j < jobs))
        def _():
            layer_norms(j - 1, jb, 2)

            @pl.when(j == 1)
            def _():
                for buf in PAIR:
                    load_n(1, buf, buf)

        @pl.when(j < jobs - 1)
        def _():
            start, chips, finish, close = sums_of(j + 1)

            @pl.when((n > 0) & (n < 5))
            def _():
                layer_pair(j, jb, n - 1)
                for buf in PAIR:
                    c = 2 * n - 2 + buf

                    @pl.when(n < 4)
                    def _():
                        load_w(j, c + 2, buf)
                        load_n(j, c + 2, buf)

                    @pl.when(n == 4)
                    def _():
                        load_n(j, buf, buf)

            @pl.when(n == 4)
            def _():
                start()

                @pl.when(j == 1)
                def _():
                    for load in load_h(xs):
                        load.start()

            @pl.when(n == 5)
            def _():
                chips()

                @pl.when(j == 1)
                def _():
                    for load in load_h(xs):
                        load.wait()
                x_swap(jb).wait_send()
                turn_x(xs, jn)

            @pl.when(n == 6)
            def _():
                finish()

            @pl.when(n == 7)
            def _():
                close()
                vec_ref[j] = sums_ref[j + 1, 0, :, pl.ds(0, 2 * width)] + sums_ref[j + 1, 1, :, pl.ds(0, 2 * width)]

                @pl.loop(0, chunks)
                def _(c):
                    swap(jb, c).wait_send()

            @pl.when(n == 7)
            def _():
                layer_norms(j, jn, 0)

                @pl.when(j == 0)
                def _():
                    for buf in PAIR:
                        load_w(1, buf, buf)

    for u in PAIR:
        result_copy(u).wait()
    for t in range(jobs * chunks - RING, jobs * chunks):
        ring.wait_sends(t, t)

    @pl.loop(0, chunks)
    def _(c):
        swap(0, c).wait_send()
    x_swap(0).wait_send()


VM = pl.BlockSpec(memory_space=pltpu.VMEM)


def whole_step(lam, vectors, h_a, h_b, weights, total_rows):
    view_rows, width = h_a.shape
    rows = 2 * view_rows
    chunks = width // COLS
    hbm = pl.BlockSpec(memory_space=pltpu.HBM)
    bf16, f32 = jnp.bfloat16, jnp.float32
    dma = pltpu.SemaphoreType.DMA
    wide = 2 * width + COLS
    return pl.pallas_call(
        functools.partial(whole_kernel, 1.0 / total_rows),
        out_shape=(jax.ShapeDtypeStruct((3, BLOCK, width), f32), jax.ShapeDtypeStruct((2, 1, 2 * width), f32),
                   jax.ShapeDtypeStruct((1, BLOCK), f32)) + (jax.ShapeDtypeStruct((rows, width), f32),) * 3,
        in_specs=[pl.BlockSpec(memory_space=pltpu.SMEM)] + [VM] * 4 + [hbm] * 5, out_specs=(hbm,) + (VM,) * 2 + (hbm,) * 3,
        scratch_shapes=[
            pltpu.VMEM((2, width // 2, 2 * rows), bf16),
            pltpu.VMEM((width // 2, rows), bf16),
            pltpu.VMEM((rows, width), bf16),
            pltpu.VMEM((2, rows, width), bf16),
            pltpu.VMEM((2, rows, width), bf16),
            pltpu.VMEM((RING, 2, 2, 2, BLOCK, COLS), f32),
            pltpu.VMEM((RING, 2, 2, BLOCK, COLS), f32),
            pltpu.VMEM((RING, 2, BLOCK, COLS), f32),
            pltpu.VMEM((RING, BLOCK, COLS), f32),
            pltpu.VMEM((rows, width), f32),
            pltpu.VMEM((2, COLS, width), bf16),
            pltpu.VMEM((2, rows, COLS), f32),
            pltpu.VMEM((3, 1, wide), f32),
            pltpu.VMEM((8, 1, wide), f32),
            pltpu.VMEM((3, 2, 1, wide), f32),
            pltpu.VMEM((2, 2, 2, 2, BLOCK, width), bf16),
            pltpu.VMEM((BLOCK, COLS), f32),
            pltpu.VMEM((2, BLOCK, COLS), f32),
            pltpu.VMEM((2, 1, width), f32),
            pltpu.VMEM((2, 1, width), f32),
            pltpu.VMEM((3, 2, 1, width), f32),
            pltpu.VMEM((3, 2, 1, width), f32),
            pltpu.VMEM((2, 2, 1, 2 * width), f32),
            pltpu.VMEM((2, 8, 1, 2 * width), f32),
            pltpu.VMEM((2, 1, 2 * width), f32),
            dma((RING, 9)), dma((RING, 9)), dma((2, chunks + 1)), dma((2, chunks + 1)),
            dma, dma, dma((7,)), dma((7,)), dma, dma, dma((2,)), dma((2,)), dma((2,)),
            dma((chunks, 10)), dma((chunks, 10)),
            dma((2, width // STRIP)), dma((2, width // STRIP)),
            dma((2,)), dma((2,)), dma((2, 7)), dma((2, 7)), dma((2,)),
        ],
        compiler_params=pltpu.CompilerParams(collective_id=1, has_side_effects=True, vmem_limit_bytes=67043328),
        name="whole_step",
    )(lam.reshape(1, 1), *(v.reshape(width // BLOCK, BLOCK) for v in vectors), h_a, h_b,
      *(w.reshape(2, width // 2, width) for w in weights))


def solution(mesh):
    shards = mesh.shape["data"]

    def local_step(h_a, h_b, w_one, w_two, w_three, gain_one, shift_one, gain_two, shift_two, lam_off):
        rows_dev, width = h_a.shape
        total_rows = rows_dev * shards
        weights, vectors, loss = whole_step(lam_off, (gain_one, shift_one, gain_two, shift_two), h_a, h_b,
                                            (w_one, w_two, w_three), total_rows)[:3]
        return (loss[0, 0], weights[2], weights[1], weights[0],
                vectors[1, 0, width:], vectors[1, 0, :width], vectors[0, 0, width:], vectors[0, 0, :width])

    row_spec = P("data", None)
    whole_mat = P(None, None)
    whole_vec = P(None)
    return jax.shard_map(
        local_step, mesh=mesh,
        in_specs=(row_spec, row_spec, whole_mat, whole_mat, whole_mat,
                  whole_vec, whole_vec, whole_vec, whole_vec, P()),
        out_specs=(P(), row_spec, row_spec, row_spec, whole_vec, whole_vec, whole_vec, whole_vec),
        check_vma=False)
```

```python
import functools

import jax
import jax.numpy as jnp
from jax import lax
from jax.experimental import pallas as pl
from jax.experimental.pallas import tpu as pltpu
from jax.sharding import PartitionSpec as P

NORM_EPS = 1e-5
MESH = pl.DeviceIdType.MESH
RING = 4
COLS = 256
STRIP = 1024
BLOCK = 128
PAIR = range(2)
AXES = range(3)
F32_SPLIT = ((48, 40, 40), (40, 48, 40), (40, 40, 48))
BF16_SPLIT = ((48, 48, 32), (32, 48, 48), (48, 32, 48))


LAST_DIMS = (((1,), (1,)), ((), ()))


def odd(n):
    return n % 2


class Place:
    def __init__(self):
        self.me = lax.axis_index("data")
        self.core = lax.rem(self.me, 2)
        self.chip = self.me // 2
        self.coord = (self.chip // 4, lax.rem(self.chip // 2, 2), lax.rem(self.chip, 2))
        self.partner = self.me + 1 - 2 * self.core
        steps = [(1 - 2 * c) * w for c, w in zip(self.coord, (8, 4, 2))]
        self.near = tuple(self.me + step for step in steps)
        self.chips = [self.me + sum(steps[a] for a in flips)
                      for flips in ((0, 1, 2), (0, 1), (0, 2), (1, 2), (0,), (1,), (2,))]


def greet(peers):
    barrier = pltpu.get_barrier_semaphore()
    for peer in peers:
        pl.semaphore_signal(barrier, inc=1, device_id=(peer,), device_id_type=MESH)
    pl.semaphore_wait(barrier, len(peers))


def remote(src, dst, send, recv, peer):
    return pltpu.make_async_remote_copy(src_ref=src, dst_ref=dst, send_sem=send, recv_sem=recv,
                                        device_id=(peer,), device_id_type=MESH)


def row_parts(split, phase):
    sizes = split[phase % 3]
    return tuple((sum(sizes[:r]), sizes[r]) for r in AXES)


class HalvingReduce:
    def __init__(self, place, acc, bufs, ssem, rsem):
        self.place, self.acc, self.bufs, self.ssem, self.rsem = place, acc, bufs, ssem, rsem

    def at(self, t, picks):
        return (lax.rem(t, RING),) + tuple(picks)

    def copy(self, step, t, phase, r):
        slot = lax.rem(t, RING)
        off, size = row_parts(F32_SPLIT, phase)[r]
        rows = pl.ds(off, size)
        picks = [slice(None)] * 3
        for k in range(step):
            axis = (r + k) % 3
            picks[axis] = self.place.coord[axis]
        axis = (r + step) % 3
        picks[axis] = 1 - self.place.coord[axis]
        src = self.acc.at[(slot, *picks, rows, slice(None))]
        dst = self.bufs[step].at[(slot,) + (slice(None),) * (2 - step) + (rows, slice(None))]
        return remote(src, dst, self.ssem.at[slot, 3 * step + r], self.rsem.at[slot, 3 * step + r],
                      self.place.near[axis])

    def send(self, step, t, phase):
        for r in AXES:
            self.copy(step, t, phase, r).start()

    def wait_sends(self, t, phase):
        for step in AXES:
            for r in AXES:
                self.copy(step, t, phase, r).wait_send()

    def add(self, step, t, phase):
        slot = lax.rem(t, RING)
        for r in AXES:
            self.copy(step, t, phase, r).wait_recv()
            off, size = row_parts(F32_SPLIT, phase)[r]
            rows = pl.ds(off, size)
            fixed = {(r + k) % 3 for k in range(step + 1)}
            free = [a for a in range(3) if a not in fixed]
            for n in range(2 ** len(free)):
                picks = list(self.place.coord)
                sub = []
                for pos, a in enumerate(free):
                    bit = (n >> (len(free) - 1 - pos)) & 1
                    picks[a] = bit
                    sub.append(bit)
                where = (slot, *picks, rows, slice(None))
                self.acc[where] = self.acc[where] + self.bufs[step][(slot, *sub, rows, slice(None))]

    def result(self, t, phase, r):
        slot = lax.rem(t, RING)
        self.copy(2, t, phase, r).wait_recv()
        off, size = row_parts(F32_SPLIT, phase)[r]
        rows = pl.ds(off, size)
        return off, size, (self.acc[(slot, *self.place.coord, rows, slice(None))]
                           + self.bufs[2][(slot, rows, slice(None))])


def columns(t, width=COLS):
    return pl.ds(pl.multiple_of(t * width, width), width)


def exchange_parts(place, psum, parts, total, sems):
    asend, arecv, csend, crecv, fsend, frecv = sems
    other = 1 - place.core
    land = psum.at[2]
    first = remote(psum.at[other], land, asend, arecv, place.partner)
    mine = parts.at[place.chip]
    across = [remote(mine, mine, csend.at[n], crecv.at[n], peer) for n, peer in enumerate(place.chips)]
    last = remote(total.at[place.core], total.at[place.core], fsend, frecv, place.partner)

    def start():
        first.start()

    def chips():
        first.wait_recv()
        parts[place.chip] = psum[place.core] + psum[2]
        for copy in across:
            copy.start()

    def finish():
        for copy in across:
            copy.wait_recv()
        value = parts[0]
        for c in range(1, 8):
            value = value + parts[c]
        total[place.core] = value
        last.start()

    def close():
        last.wait_recv()
        first.wait_send()
        for copy in across:
            copy.wait_send()
        last.wait_send()

    return start, chips, finish, close


def exchange_pair(place, own, land, parts, total, sems):
    asend, arecv, csend, crecv = sems
    first = remote(own, land, asend, arecv, place.partner)
    mine = parts.at[place.chip]
    across = [remote(mine, mine, csend.at[n], crecv.at[n], peer) for n, peer in enumerate(place.chips)]

    def chips():
        first.wait_recv()
        parts[place.chip] = own[...] + land[...]
        for copy in across:
            copy.start()

    def finish():
        first.wait_send()
        for copy in across:
            copy.wait()
        value = parts[0]
        for c in range(1, 8):
            value = value + parts[c]
        total[...] = value

    return first.start, chips, finish


def whole_kernel(inv_rows, lam_ref, g1_ref, s1_ref, g2_ref, s2_ref, ha_hbm, hb_hbm, w1_hbm, w2_hbm, w3_hbm,
                 out_ref, vec_ref, loss_ref, n1_hbm, n2_hbm, n3_hbm,
                 xt, xsend, xs, own, other, acc, b0, b1, b2, gp, wbuf, nbuf, psum, parts, sums_ref, grads, stage,
                 done, gains, shifts, means, invs, fsum, fparts, ftotal,
                 ssem, rsem, psend, precv, asend, arecv, csend, crecv, fsend, frecv, lsem, wsem, nsem, gsend, grecv,
                 usem, vsem, easend, earecv, ecsend, ecrecv, dsem):
    place = Place()
    view_rows, width = ha_hbm.shape
    rows = 2 * view_rows
    chunks = width // COLS
    jobs = 3
    partner = place.partner
    ring = HalvingReduce(place, acc, (b0, b1, b2), ssem, rsem)

    def load_w(j, c, buf):
        rows_c = columns(lax.rem(c, chunks // 2))
        for k, ref in enumerate((w3_hbm, w2_hbm)):
            @pl.when(j == k)
            def _():
                pltpu.make_async_copy(ref.at[c // (chunks // 2), rows_c, :], wbuf.at[buf], wsem.at[buf]).start()

    def load_z(c, buf):
        pltpu.make_async_copy(n3_hbm.at[:, columns(c)], nbuf.at[buf], nsem.at[buf]).start()

    def load_n(j, c, buf):
        for k, ref in enumerate((n2_hbm, n1_hbm)):
            @pl.when(j == k)
            def _():
                pltpu.make_async_copy(ref.at[:, columns(c)], nbuf.at[buf], nsem.at[buf]).start()

    def wait_w(buf):
        pltpu.make_async_copy(w3_hbm.at[0, pl.ds(0, COLS), :], wbuf.at[buf], wsem.at[buf]).wait()

    def wait_n(buf):
        pltpu.make_async_copy(n2_hbm.at[:, pl.ds(0, COLS)], nbuf.at[buf], nsem.at[buf]).wait()

    def swap(jb, c):
        cols = columns(c)
        return remote(own.at[jb, :, cols], other.at[jb, :, cols], psend.at[jb, c], precv.at[jb, c], partner)

    def x_swap(jb):
        return remote(xsend, xt.at[jb, :, pl.ds(rows, rows)], psend.at[jb, chunks], precv.at[jb, chunks], partner)

    def load_h(dst):
        return [pltpu.make_async_copy(ref, dst.at[pl.ds(view * view_rows, view_rows), :], lsem.at[view])
                for view, ref in enumerate((ha_hbm, hb_hbm))]

    def turn(src, depth, copy, jb):
        def blocks(dst, parity):
            @pl.loop(0, 8)
            def _(b):
                to = pl.ds(pl.multiple_of(b * BLOCK, BLOCK), BLOCK)
                cols = pl.ds(pl.multiple_of((2 * b + parity) * BLOCK, BLOCK), BLOCK)
                dst[to, pl.ds(0, depth)] = src[pl.ds(0, depth), cols].T

        blocks(xsend, 1 - place.core)
        copy.start()
        blocks(xt.at[jb], place.core)

    def turn_x(src, jb):
        turn(src, rows, x_swap(jb), jb)

    def sums_of(i):
        return exchange_parts(place, psum, parts, sums_ref.at[i], (asend, arecv, csend, crecv, fsend, frecv))

    def wide(c):
        return pl.ds(pl.multiple_of(width + c * COLS, COLS), COLS)

    def normed_of(i, view, buf, cols):
        at = pl.ds(view * view_rows, view_rows)
        return (nbuf[buf, at, :] - means[i, view, :, cols]) * invs[i, view, :, cols]

    def layer_pair(j, jb, n):
        for buf in PAIR:
            wait_w(buf)
            wait_n(buf)
        for view in PAIR:
            at = pl.ds(view * view_rows, view_rows)
            both = lax.dot_general(own[jb, at, :], wbuf[...].reshape(2 * COLS, width), LAST_DIMS,
                                   preferred_element_type=jnp.float32)
            for buf in PAIR:
                c = 2 * n + buf
                cols = columns(c)
                normed = normed_of(j + 1, view, buf, cols)
                grad = jnp.where(gains[1 - j, :, cols] * normed + shifts[1 - j, :, cols] > 0,
                                 both[:, buf * COLS:(buf + 1) * COLS], 0.0)
                gp[at, cols] = grad
                psum[view, :, cols] = jnp.sum(grad, axis=0, keepdims=True)
                psum[view, :, wide(c)] = jnp.sum(grad * normed, axis=0, keepdims=True)

    def norm_chunk(i, gain, jn, c, buf):
        cols = columns(c)
        wait_n(buf)
        for view in PAIR:
            at = pl.ds(view * view_rows, view_rows)
            first = sums_ref[i, view, :, cols]
            second = sums_ref[i, view, :, wide(c)]
            grad = invs[i, view, :, cols] * (gp[at, cols] - (first + normed_of(i, view, buf, cols) * second) * inv_rows)
            if gain is not None:
                grad = gains[gain, :, cols] * grad
            own[jn, at, cols] = grad.astype(jnp.bfloat16)
        swap(jn, c).start()

    half = width // 2
    strips = width // STRIP
    weights = (w1_hbm, w2_hbm, w3_hbm)
    w_slots = (xt, other, xt)
    hidden_out = (n1_hbm, n2_hbm, n3_hbm)

    def view_at(view):
        return pl.ds(view * view_rows, view_rows)

    def fetch_w(l, c):
        cols = columns(c, STRIP)
        return pltpu.make_async_copy(weights[l].at[:, :, cols], w_slots[l].at[:, :, cols], vsem.at[odd(l), c])

    def fetch_all(l, lo=0):
        @pl.loop(lo, strips)
        def _(c):
            fetch_w(l, c).start()

    load_a, load_b = load_h(own.at[0])
    load_a.start()
    fetch_w(0, 0).start()

    @pl.loop(0, width // BLOCK)
    def _(r):
        lanes = pl.ds(pl.multiple_of(r * BLOCK, BLOCK), BLOCK)
        for n, (g_ref, s_ref) in enumerate(((g1_ref, s1_ref), (g2_ref, s2_ref))):
            gains[n, :, lanes] = g_ref[pl.ds(r, 1), :]
            shifts[n, :, lanes] = s_ref[pl.ds(r, 1), :]

    swaps = [exchange_pair(place, fsum.at[v, 0], fsum.at[v, 1], fparts.at[v], ftotal.at[v],
                           tuple(sem.at[v] for sem in (easend, earecv, ecsend, ecrecv)))
             for v in PAIR]
    greet([partner] + place.chips)
    load_b.start()
    fetch_all(0, 1)
    load_a.wait()

    def far(c, size):
        return pl.ds(pl.multiple_of(width + c * size, size), size)

    def hidden_copy(l, view, c):
        cols = columns(c, STRIP)
        return pltpu.make_async_copy(gp.at[view_at(view), cols], hidden_out[l].at[view_at(view), cols],
                                     usem.at[view, c])

    def products(l, view, actions):
        at = view_at(view)

        @pl.loop(0, strips)
        def _(c):
            for when, action in actions:
                pl.when(c == when)(action)
            if view == 0:
                fetch_w(l, c).wait()
            if l:
                hidden_copy(l - 1, view, c).wait()
            cols = columns(c, STRIP)
            value = jnp.dot(own[odd(l), at, pl.ds(0, half)], w_slots[l][0, :, cols],
                            preferred_element_type=jnp.float32)
            value += jnp.dot(own[odd(l), at, pl.ds(half, half)], w_slots[l][1, :, cols],
                             preferred_element_type=jnp.float32)
            gp[at, cols] = value
            fsum[view, 0, :, cols] = jnp.sum(value, axis=0, keepdims=True)
            fsum[view, 0, :, far(c, STRIP)] = jnp.sum(value * value, axis=0, keepdims=True)
            hidden_copy(l, view, c).start()

    def normalise(l, view, after=None):
        at = view_at(view)

        @pl.loop(0, chunks)
        def _(c):
            cols = columns(c)
            mean = ftotal[view, :, cols] * inv_rows
            square = ftotal[view, :, far(c, COLS)] * inv_rows
            inv = lax.rsqrt(square - mean * mean + NORM_EPS)
            means[2 - l, view, :, cols] = mean
            invs[2 - l, view, :, cols] = inv
            act = (gp[at, cols] - mean) * inv
            if l < 2:
                act = jnp.maximum(gains[l, :, cols] * act + shifts[l, :, cols], 0.0)
            act = act.astype(jnp.bfloat16)
            own[odd(l + 1), at, cols] = act
            if l == 0:
                xs[at, cols] = act
            if after is not None:
                after(c)

    a_swap, b_swap = swaps
    for l in AXES:
        products(l, 0, ((0, b_swap[1]),) if l else ())
        a_swap[0]()
        if l:
            b_swap[2]()
            normalise(l - 1, 1)
        else:
            fetch_all(1)
            load_b.wait()
        products(l, 1, ((0, a_swap[1]),))
        b_swap[0]()
        if l == 0:
            fetch_all(2)
        a_swap[2]()
        normalise(l, 0)

    lam = lam_ref[0, 0]
    a_rows, b_rows = view_at(0), view_at(1)
    last_cols = pl.ds(2 * width, COLS)
    for view in PAIR:
        psum[view, :, last_cols] = jnp.zeros((1, COLS), jnp.float32)
    for buf in PAIR:
        load_w(0, buf, buf)

    def z_swap(c):
        cols = columns(c)
        return remote(own.at[1, b_rows, cols], other.at[1, a_rows, cols], psend.at[1, c], precv.at[1, c], partner)

    z_turn = remote(xsend.at[:, a_rows], xt.at[1, :, b_rows], psend.at[1, chunks], precv.at[1, chunks], partner)
    b_swap[1]()
    turn(own.at[1], view_rows, z_turn, 1)
    b_swap[2]()
    normalise(2, 1, lambda c: z_swap(c).start())
    for view in PAIR:
        @pl.loop(0, strips)
        def _(c):
            hidden_copy(2, view, c).wait()
    for buf in PAIR:
        load_z(buf, buf)
    z_turn.wait_recv()

    def gather(step, t, phase, r):
        off, size = row_parts(BF16_SPLIT, phase)[r]
        picks = list(place.coord)
        for k in range(step):
            picks[(r + 2 - k) % 3] = slice(None)
        axis = (r + 2 - step) % 3
        ref = grads.at[(*picks, place.core, pl.ds(off, size), columns(t))]
        return remote(ref, ref, gsend.at[t, 3 * step + r], grecv.at[t, 3 * step + r], place.near[axis])

    def across(t):
        ref = grads.at[:, :, :, place.core, :, columns(t)]
        return remote(ref, ref, gsend.at[t, 9], grecv.at[t, 9], partner)

    def corr_block(t, phase):
        for r in AXES:
            off, size, val = ring.result(t, phase, r)
            corr = val * inv_rows
            row_id = place.me * BLOCK + off + lax.broadcasted_iota(jnp.int32, corr.shape, 0)
            col_id = t * COLS + lax.broadcasted_iota(jnp.int32, corr.shape, 1)
            diag = row_id == col_id
            gap = 1.0 - corr
            terms = jnp.where(diag, gap * gap, lam * corr * corr)
            psum[0, :, last_cols] += jnp.sum(terms, axis=0, keepdims=True)
            stage[pl.ds(off, size), :] = jnp.where(diag, -2.0 * gap, 2.0 * lam * corr) * inv_rows
        grads[(*place.coord, place.core, slice(None), columns(t))] = stage[...].astype(jnp.bfloat16)
        for r in AXES:
            gather(0, t, phase, r).start()

    def embed_chunk(c):
        cols = columns(c)
        buf = lax.rem(c, 2)
        block = grads[:, :, :, :, :, cols].reshape(width, COLS)
        grad = jnp.dot(own[1, a_rows, :], block, preferred_element_type=jnp.float32)
        gp[b_rows, cols] = grad
        wait_n(buf)
        psum[1, :, cols] = jnp.sum(grad, axis=0, keepdims=True)
        psum[1, :, wide(c)] = jnp.sum(grad * normed_of(0, 1, buf, cols), axis=0, keepdims=True)
        load_z(lax.rem(c + 2, chunks), buf)

        @pl.loop(0, 2)
        def _(k):
            rows_g = grads[k, :, :, :, :, cols].reshape(1024, COLS)
            more = lax.dot_general(own[1, b_rows, cols], rows_g, LAST_DIMS, preferred_element_type=jnp.float32)
            at_k = columns(k, 1024)
            gp[a_rows, at_k] = jnp.where(c > 0, gp[a_rows, at_k], 0.0) + more

            @pl.when(c == chunks - 1)
            def _():
                for q in range(4):
                    buf_k = q % 2
                    sub = 4 * k + q
                    at_sub = columns(sub)
                    total = gp[a_rows, at_sub]
                    wait_n(buf_k)
                    psum[0, :, at_sub] = jnp.sum(total, axis=0, keepdims=True)
                    psum[0, :, wide(sub)] = jnp.sum(total * normed_of(0, 0, buf_k, at_sub), axis=0, keepdims=True)
                    load_z(lax.rem(sub + 2, chunks), buf_k)

    @pl.loop(0, chunks + 7)
    def _(t):
        phase = lax.rem(t, 3)

        @pl.when(t < chunks)
        def _():
            for s in AXES:
                @pl.when((phase == s) & (t >= RING))
                def _():
                    ring.wait_sends(t - RING, s - RING)
            z_swap(t).wait_recv()
            cols = columns(t)
            for half in PAIR:
                feats = pl.ds(512 * half, 512)
                part = jnp.dot(xt[1, feats, a_rows], own[1, b_rows, cols], preferred_element_type=jnp.float32)
                part += jnp.dot(xt[1, feats, b_rows], other[1, a_rows, cols], preferred_element_type=jnp.float32)
                acc[lax.rem(t, RING), half] = part.reshape(2, 2, BLOCK, COLS)

        for s in AXES:
            @pl.when(phase == s)
            def _():
                @pl.when(t < chunks)
                def _():
                    ring.send(0, t, s)

                for step in PAIR:
                    u = t - 1 - step

                    @pl.when((u >= 0) & (u < chunks))
                    def _():
                        ring.add(step, u, s - 1 - step)
                        ring.send(step + 1, u, s - 1 - step)

                @pl.when((t >= 3) & (t < chunks + 3))
                def _():
                    corr_block(t - 3, s - 3)

                for step in PAIR:
                    v = t - 4 - step

                    @pl.when((v >= 0) & (v < chunks))
                    def _():
                        for r in AXES:
                            gather(step, v, s - 4 - step, r).wait_recv()
                            gather(step + 1, v, s - 4 - step, r).start()

                @pl.when((t >= 6) & (t < chunks + 6))
                def _():
                    for r in AXES:
                        gather(2, t - 6, s - 6, r).wait_recv()
                    across(t - 6).start()

        @pl.when(t == 1)
        def _():
            z_turn.wait_send()
            turn_x(own.at[0], 0)

        @pl.when(t >= 7)
        def _():
            c = t - 7
            across(c).wait_recv()
            embed_chunk(c)

    start, chips, finish, close = sums_of(0)
    start()
    chips()
    for t in range(chunks - RING, chunks):
        ring.wait_sends(t, t)
    for t in range(chunks):
        across(t).wait_send()
        z_swap(t).wait_send()
        for step in AXES:
            for r in AXES:
                gather(step, t, t, r).wait_send()
    finish()
    close()
    loss_ref[...] = jnp.sum(sums_ref[0, 0, :, last_cols], axis=1, keepdims=True) + jnp.zeros((1, BLOCK), jnp.float32)

    def norm_pairs(lo, hi):
        @pl.loop(lo, hi)
        def _(pair):
            for buf in PAIR:
                c = 2 * pair + buf
                norm_chunk(0, None, 0, c, buf)

                @pl.when(c < chunks - 2)
                def _():
                    load_z(c + 2, buf)

    norm_pairs(0, 1)

    def result_copy(u):
        return pltpu.make_async_copy(done.at[lax.rem(u, 2)], out_ref.at[u // chunks, :, columns(lax.rem(u, chunks))],
                                     dsem.at[lax.rem(u, 2)])

    def layer_norms(j, jn, lo):
        @pl.loop(lo, lo + 2)
        def _(pair):
            for buf in PAIR:
                c = 2 * pair + buf
                norm_chunk(j + 1, 1 - j, jn, c, buf)

                @pl.when(c < chunks - 2)
                def _():
                    load_n(j, c + 2, buf)

    @pl.loop(0, jobs * chunks + 3)
    def _(t):
        j = t // chunks
        n = lax.rem(t, chunks)
        jb = lax.rem(j, 2)
        jn = 1 - jb
        phase = lax.rem(t, 3)

        @pl.when(t < jobs * chunks)
        def _():
            for s in AXES:
                @pl.when((phase == s) & (t >= RING))
                def _():
                    ring.wait_sends(t - RING, s - RING)

            @pl.when(n == 0)
            def _():
                x_swap(jb).wait_recv()
            swap(jb, n).wait_recv()
            cols = columns(n)
            slot = lax.rem(t, RING)
            for half in PAIR:
                feats = pl.ds(512 * half, 512)
                part = jnp.dot(xt[jb, feats, pl.ds(0, rows)], own[jb, :, cols], preferred_element_type=jnp.float32)
                part += jnp.dot(xt[jb, feats, pl.ds(rows, rows)], other[jb, :, cols],
                                preferred_element_type=jnp.float32)
                acc[slot, half] = part.reshape(2, 2, BLOCK, COLS)

        for s in AXES:
            @pl.when(phase == s)
            def _():
                @pl.when(t < jobs * chunks)
                def _():
                    ring.send(0, t, s)

                for step in PAIR:
                    u = t - 1 - step

                    @pl.when((u >= 0) & (u < jobs * chunks))
                    def _():
                        ring.add(step, u, s - 1 - step)
                        ring.send(step + 1, u, s - 1 - step)

                @pl.when(t >= 3)
                def _():
                    u = t - 3
                    pl.when(t >= 5)(result_copy(u).wait)
                    for r in AXES:
                        off, size, val = ring.result(u, s - 3, r)
                        done[lax.rem(u, 2), pl.ds(off, size), :] = val
                    result_copy(u).start()

        @pl.when(t == 0)
        def _():
            norm_pairs(1, chunks // 2)
            for buf in PAIR:
                load_n(0, buf, buf)

        @pl.when((n == 0) & (j > 0) & (j < jobs))
        def _():
            layer_norms(j - 1, jb, 2)

            @pl.when(j == 1)
            def _():
                for buf in PAIR:
                    load_n(1, buf, buf)

        @pl.when(j < jobs - 1)
        def _():
            start, chips, finish, close = sums_of(j + 1)

            @pl.when((n > 0) & (n < 5))
            def _():
                layer_pair(j, jb, n - 1)
                for buf in PAIR:
                    c = 2 * n - 2 + buf

                    @pl.when(n < 4)
                    def _():
                        load_w(j, c + 2, buf)
                        load_n(j, c + 2, buf)

                    @pl.when(n == 4)
                    def _():
                        load_n(j, buf, buf)

            @pl.when(n == 4)
            def _():
                start()

                @pl.when(j == 1)
                def _():
                    for load in load_h(xs):
                        load.start()

            @pl.when(n == 5)
            def _():
                chips()

                @pl.when(j == 1)
                def _():
                    for load in load_h(xs):
                        load.wait()
                x_swap(jb).wait_send()
                turn_x(xs, jn)

            @pl.when(n == 6)
            def _():
                finish()

            @pl.when(n == 7)
            def _():
                close()
                vec_ref[j] = sums_ref[j + 1, 0, :, pl.ds(0, 2 * width)] + sums_ref[j + 1, 1, :, pl.ds(0, 2 * width)]

                @pl.loop(0, chunks)
                def _(c):
                    swap(jb, c).wait_send()

            @pl.when(n == 7)
            def _():
                layer_norms(j, jn, 0)

                @pl.when(j == 0)
                def _():
                    for buf in PAIR:
                        load_w(1, buf, buf)

    for u in PAIR:
        result_copy(u).wait()
    for t in range(jobs * chunks - RING, jobs * chunks):
        ring.wait_sends(t, t)

    @pl.loop(0, chunks)
    def _(c):
        swap(0, c).wait_send()
    x_swap(0).wait_send()


VM = pl.BlockSpec(memory_space=pltpu.VMEM)


def whole_step(lam, vectors, h_a, h_b, weights, total_rows):
    view_rows, width = h_a.shape
    rows = 2 * view_rows
    chunks = width // COLS
    hbm = pl.BlockSpec(memory_space=pltpu.HBM)
    bf16, f32 = jnp.bfloat16, jnp.float32
    dma = pltpu.SemaphoreType.DMA
    wide = 2 * width + COLS
    return pl.pallas_call(
        functools.partial(whole_kernel, 1.0 / total_rows),
        out_shape=(jax.ShapeDtypeStruct((3, BLOCK, width), f32), jax.ShapeDtypeStruct((2, 1, 2 * width), f32),
                   jax.ShapeDtypeStruct((1, BLOCK), f32)) + (jax.ShapeDtypeStruct((rows, width), f32),) * 3,
        in_specs=[pl.BlockSpec(memory_space=pltpu.SMEM)] + [VM] * 4 + [hbm] * 5, out_specs=(hbm,) + (VM,) * 2 + (hbm,) * 3,
        scratch_shapes=[
            pltpu.VMEM((2, width // 2, 2 * rows), bf16),
            pltpu.VMEM((width // 2, rows), bf16),
            pltpu.VMEM((rows, width), bf16),
            pltpu.VMEM((2, rows, width), bf16),
            pltpu.VMEM((2, rows, width), bf16),
            pltpu.VMEM((RING, 2, 2, 2, BLOCK, COLS), f32),
            pltpu.VMEM((RING, 2, 2, BLOCK, COLS), f32),
            pltpu.VMEM((RING, 2, BLOCK, COLS), f32),
            pltpu.VMEM((RING, BLOCK, COLS), f32),
            pltpu.VMEM((rows, width), f32),
            pltpu.VMEM((2, COLS, width), bf16),
            pltpu.VMEM((2, rows, COLS), f32),
            pltpu.VMEM((3, 1, wide), f32),
            pltpu.VMEM((8, 1, wide), f32),
            pltpu.VMEM((3, 2, 1, wide), f32),
            pltpu.VMEM((2, 2, 2, 2, BLOCK, width), bf16),
            pltpu.VMEM((BLOCK, COLS), f32),
            pltpu.VMEM((2, BLOCK, COLS), f32),
            pltpu.VMEM((2, 1, width), f32),
            pltpu.VMEM((2, 1, width), f32),
            pltpu.VMEM((3, 2, 1, width), f32),
            pltpu.VMEM((3, 2, 1, width), f32),
            pltpu.VMEM((2, 2, 1, 2 * width), f32),
            pltpu.VMEM((2, 8, 1, 2 * width), f32),
            pltpu.VMEM((2, 1, 2 * width), f32),
            dma((RING, 9)), dma((RING, 9)), dma((2, chunks + 1)), dma((2, chunks + 1)),
            dma, dma, dma((7,)), dma((7,)), dma, dma, dma((2,)), dma((2,)), dma((2,)),
            dma((chunks, 10)), dma((chunks, 10)),
            dma((2, width // STRIP)), dma((2, width // STRIP)),
            dma((2,)), dma((2,)), dma((2, 7)), dma((2, 7)), dma((2,)),
        ],
        compiler_params=pltpu.CompilerParams(collective_id=1, has_side_effects=True, vmem_limit_bytes=67043328),
        name="whole_step",
    )(lam.reshape(1, 1), *(v.reshape(width // BLOCK, BLOCK) for v in vectors), h_a, h_b,
      *(w.reshape(2, width // 2, width) for w in weights))


def solution(mesh):
    shards = mesh.shape["data"]

    def local_step(h_a, h_b, w_one, w_two, w_three, gain_one, shift_one, gain_two, shift_two, lam_off):
        rows_dev, width = h_a.shape
        total_rows = rows_dev * shards
        weights, vectors, loss = whole_step(lam_off, (gain_one, shift_one, gain_two, shift_two), h_a, h_b,
                                            (w_one, w_two, w_three), total_rows)[:3]
        return (loss[0, 0], weights[2], weights[1], weights[0],
                vectors[1, 0, width:], vectors[1, 0, :width], vectors[0, 0, width:], vectors[0, 0, :width])

    row_spec = P("data", None)
    whole_mat = P(None, None)
    whole_vec = P(None)
    return jax.shard_map(
        local_step, mesh=mesh,
        in_specs=(row_spec, row_spec, whole_mat, whole_mat, whole_mat,
                  whole_vec, whole_vec, whole_vec, whole_vec, P()),
        out_specs=(P(), row_spec, row_spec, row_spec, whole_vec, whole_vec, whole_vec, whole_vec),
        check_vma=False)
```
